32 devices in a mesh: col: 8 (over z, y), row: 4 (over x, core).
Axes of the slice: x: 2, y: 2, z: 4, core: 2. Of those that a mesh axis runs over, the one named last changes fastest.
Arguments:
- inter_mask: int32 [65536, 4096], P('row', 'col')
- emb_user: bfloat16 [65536, 64], P(('row', 'col'))
- emb_item: bfloat16 [4096, 64], P(('col', 'row'))
- triples: int32 [128, 3], replicated
Outputs:
- output 1: bfloat16 [65536, 64], P(('row', 'col'))
- output 2: bfloat16 [4096, 64], P(('col', 'row'))
- output 3: float32 [], replicated
All inputs are finite; a program needn't handle non-finite values.
Results may differ from the reference program's by a relative error of at most 0.00519882.
Values are sent between devices in bfloat16 or wider.
A program may use at most 1 GiB of HBM per device.

```python
import jax
import jax.numpy as jnp
from jax import lax

USERS = 65536
ITEMS = 4096
DIM = 64
LAYERS = 3
TRIPLES = 128
USER_DEGREE = 3


def draw_triples(trip_key):
    key_user, key_pos, key_neg = jax.random.split(trip_key, 3)
    row_pos = jnp.arange(TRIPLES)
    user_ids = jax.random.randint(key_user, (TRIPLES,), 0, USERS)
    pos_ids = jax.random.randint(key_pos, (TRIPLES,), 0, ITEMS)
    neg_ids = jax.random.randint(key_neg, (TRIPLES,), 0, ITEMS)
    user_ids = jnp.where(row_pos == 0, USERS - 1, jnp.where(row_pos == 1, 0, user_ids))
    pos_ids = jnp.where(row_pos == 0, ITEMS - 1, jnp.where(row_pos == 1, 0, pos_ids))
    neg_ids = jnp.where(row_pos == 0, 0, jnp.where(row_pos == 1, ITEMS - 1, neg_ids))
    return jnp.stack([user_ids, pos_ids, neg_ids], axis=1).astype(jnp.int32)


def setup_inputs(seed: int = 0) -> dict:
    base_key = jax.random.key(seed)
    key_mask, key_user, key_item, key_trip = jax.random.split(base_key, 4)
    raw_draw = jax.random.randint(key_mask, (USERS, ITEMS), 0, ITEMS)
    inter_mask = (raw_draw < USER_DEGREE).astype(jnp.int32)
    emb_user = jax.random.normal(key_user, (USERS, DIM), jnp.float32).astype(jnp.bfloat16)
    emb_item = jax.random.normal(key_item, (ITEMS, DIM), jnp.float32).astype(jnp.bfloat16)
    return {"inter_mask": inter_mask, "emb_user": emb_user, "emb_item": emb_item, "triples": draw_triples(key_trip)}


def reference(inter_mask, emb_user, emb_item, triples):
    deg_user = jnp.maximum(jnp.sum(inter_mask, axis=1), 1)
    deg_item = jnp.maximum(jnp.sum(inter_mask, axis=0), 1)
    scale_user = lax.rsqrt(deg_user.astype(jnp.float32))
    scale_item = lax.rsqrt(deg_item.astype(jnp.float32))
    norm_adj = (inter_mask.astype(jnp.float32) * scale_user[:, None] * scale_item[None, :]).astype(jnp.bfloat16)
    layer_user = emb_user
    layer_item = emb_item
    total_user = emb_user.astype(jnp.float32)
    total_item = emb_item.astype(jnp.float32)
    for layer_idx in range(LAYERS):
        next_user = jnp.dot(norm_adj, layer_item, preferred_element_type=jnp.float32).astype(jnp.bfloat16)
        next_item = lax.dot_general(norm_adj, layer_user, (((0,), (0,)), ((), ())), preferred_element_type=jnp.float32).astype(jnp.bfloat16)
        total_user = total_user + next_user.astype(jnp.float32)
        total_item = total_item + next_item.astype(jnp.float32)
        layer_user = next_user
        layer_item = next_item
    out_user = (total_user / (LAYERS + 1)).astype(jnp.bfloat16)
    out_item = (total_item / (LAYERS + 1)).astype(jnp.bfloat16)
    user_vec = jnp.take(out_user, triples[:, 0], axis=0).astype(jnp.float32)
    pos_vec = jnp.take(out_item, triples[:, 1], axis=0).astype(jnp.float32)
    neg_vec = jnp.take(out_item, triples[:, 2], axis=0).astype(jnp.float32)
    margin = jnp.sum(user_vec * pos_vec, axis=1) - jnp.sum(user_vec * neg_vec, axis=1)
    bpr_loss = jnp.mean(jax.nn.softplus(-margin))
    return out_user, out_item, bpr_loss
```

```python
import functools

import jax
import jax.numpy as jnp
from jax import lax
from jax.experimental import pallas as pl
from jax.experimental.pallas import tpu as pltpu
from jax.sharding import PartitionSpec as P

LAYERS = 3
RING = 8
ROWS = 4
STREAMS = 4
DIM = 64
BLK = 512
MASK_BUFS = 8
MESH = pl.DeviceIdType.MESH
BF16 = jnp.bfloat16
F32 = jnp.float32
ORDER = (0, 2, 1, 3)


def sign(j):
    return 1 if j < 2 else -1


def col_of(p):
    p = lax.rem(p + 2 * RING, RING)
    y = lax.div(p, 4)
    z = p + y * (7 - 2 * p)
    return 2 * z + y


def dot_t(lhs, rhs):
    return lax.dot_general(lhs, rhs, (((1,), (1,)), ((), ())), preferred_element_type=F32)


def dot_n(lhs, rhs):
    return lax.dot_general(lhs, rhs, (((1,), (0,)), ((), ())), preferred_element_type=F32)


def kernel(mask_hbm, euT, eiT, trip, outu, outi, loss,
           adj, mbuf, msem,
           panel0, panel1, panel2, ei_all, item_acc, item_send, item_recv,
           slots, first,
           colsum, deg_part, deg_recv, scale_u, itemdeg, itemdeg_recv, scale_v,
           onehot_a, pk, pk_recv, picks, terms, terms2,
           ag_ss, ag_rs, rs_ss, rs_rs,
           row_ss, row_rs, col_ss, col_rs):
    c = lax.axis_index("col")
    r = lax.axis_index("row")
    z, y = lax.div(c, 2), lax.rem(c, 2)
    pos = z + y * (7 - 2 * z)
    right, left = col_of(pos + 1), col_of(pos - 1)
    row_peers = [lax.rem(r + d, ROWS) for d in range(1, ROWS)]
    col_peers = [lax.rem(c + d, RING) for d in range(1, RING)]
    panels = (panel0, panel1, panel2)

    def mask_copy(i):
        slot = lax.rem(i, MASK_BUFS)
        return pltpu.make_async_copy(mask_hbm.at[pl.ds(i * BLK, BLK), :], mbuf.at[slot], msem.at[slot])

    for i in range(MASK_BUFS):
        mask_copy(i).start()

    barrier = pltpu.get_barrier_semaphore()
    for rr in row_peers:
        pl.semaphore_signal(barrier, inc=1, device_id=(c, rr), device_id_type=MESH)
    for cc in col_peers:
        pl.semaphore_signal(barrier, inc=1, device_id=(cc, r), device_id_type=MESH)

    for j in range(STREAMS):
        panel0[c, j] = euT[:, j * BLK:(j + 1) * BLK]
    ei_all[0, r] = eiT[...]
    colsum[...] = jnp.zeros_like(colsum)
    pl.semaphore_wait(barrier, (ROWS - 1) + (RING - 1))

    def ring_dev(j):
        return (right if sign(j) > 0 else left, r)

    def ag_copy(k, j, s):
        q = col_of(pos - sign(j) * s)
        ref = panels[k].at[q, j]
        return pltpu.make_async_remote_copy(src_ref=ref, dst_ref=ref, send_sem=ag_ss.at[k, j, s],
                                            recv_sem=ag_rs.at[k, j, s], device_id=ring_dev(j), device_id_type=MESH)

    def ag_step(k, j, s, last=False):
        ag_copy(k, j, s).wait_recv()
        if not last:
            ag_copy(k, j, s + 1).start()

    def rs_copy(k, j, s, src=None):
        src = slots.at[k, j, s] if src is None else src
        return pltpu.make_async_remote_copy(src_ref=src, dst_ref=slots.at[k, j, s], send_sem=rs_ss.at[k, j, s],
                                            recv_sem=rs_rs.at[k, j, s], device_id=ring_dev(j), device_id_type=MESH)

    def row_send(u, src, dst):
        for rr in row_peers:
            pltpu.make_async_remote_copy(src_ref=src(rr), dst_ref=dst, send_sem=row_ss.at[u, rr],
                                         recv_sem=row_rs.at[u, r], device_id=(c, rr), device_id_type=MESH).start()

    def row_wait(u, src, dst):
        for rr in row_peers:
            cp = pltpu.make_async_remote_copy(src_ref=src(rr), dst_ref=dst(rr), send_sem=row_ss.at[u, rr],
                                              recv_sem=row_rs.at[u, rr], device_id=(c, rr), device_id_type=MESH)
            cp.wait_recv()
            cp.wait_send()

    def col_send(u, src, dst):
        for cc in col_peers:
            pltpu.make_async_remote_copy(src_ref=src(cc), dst_ref=dst, send_sem=col_ss.at[u, cc],
                                         recv_sem=col_rs.at[u, c], device_id=(cc, r), device_id_type=MESH).start()

    def col_wait(u, src, dst):
        for cc in col_peers:
            cp = pltpu.make_async_remote_copy(src_ref=src(cc), dst_ref=dst(cc), send_sem=col_ss.at[u, cc],
                                              recv_sem=col_rs.at[u, cc], device_id=(cc, r), device_id_type=MESH)
            cp.wait_recv()
            cp.wait_send()

    for j in ORDER:
        ag_copy(0, j, 0).start()
    row_send(0, lambda rr: ei_all.at[0, r], ei_all.at[0, r])

    ones = jnp.ones((16, BLK), BF16)

    def mask_block(i, carry):
        slot = lax.rem(i, MASK_BUFS)
        mask_copy(i).wait()
        acc = jnp.zeros((8, BLK), F32)
        for t in range(4):
            m = mbuf[slot, t * 128:(t + 1) * 128, :].astype(F32)
            acc = acc + jnp.sum(m.reshape(16, 8, BLK), axis=0)
            adj[i, t * 128:(t + 1) * 128, :] = m.astype(BF16)
        colsum[...] += acc
        deg_part[i] = dot_t(ones, adj[i])[0:1, :]

        @pl.when(i + MASK_BUFS < 4 * RING)
        def _():
            mask_copy(i + MASK_BUFS).start()
        return carry

    for s in range(4):
        lax.fori_loop(8 * s, 8 * s + 8, mask_block, 0)
        if s < 3:
            for j in ORDER:
                ag_step(0, j, s)

    shard = lambda ref, cc: ref.at[pl.ds(cc * STREAMS, STREAMS)]
    itemdeg[...] = jnp.sum(colsum[...], axis=0, keepdims=True)
    col_send(0, lambda cc: shard(deg_part, cc), deg_recv.at[c])
    row_send(1, lambda rr: itemdeg, itemdeg_recv.at[r])
    itemdeg_recv[r] = itemdeg[...]
    deg_recv[c] = deg_part[pl.ds(c * STREAMS, STREAMS)]
    for j in ORDER:
        ag_step(0, j, 3)
    row_wait(1, lambda rr: itemdeg, lambda rr: itemdeg_recv.at[rr])
    dv = itemdeg_recv[0] + itemdeg_recv[1] + itemdeg_recv[2] + itemdeg_recv[3]
    scale_v[...] = lax.rsqrt(jnp.maximum(dv, 1.0))
    col_wait(0, lambda cc: shard(deg_part, cc), lambda cc: deg_recv.at[cc])
    du = deg_recv[0]
    for q in range(1, RING):
        du = du + deg_recv[q]
    scale_u[pl.ds(c * STREAMS, STREAMS)] = lax.rsqrt(jnp.maximum(du, 1.0))
    col_send(1, lambda cc: shard(scale_u, c), shard(scale_u, c))
    for s in range(4, 7):
        for j in ORDER:
            ag_step(0, j, s, last=s == 6)
    row_wait(0, lambda rr: ei_all.at[0, r], lambda rr: ei_all.at[0, rr])
    col_wait(1, lambda cc: shard(scale_u, c), lambda cc: shard(scale_u, cc))

    def build(b):
        sv = scale_v[...]
        for t in range(4):
            su = scale_u[b, :, t * 128:(t + 1) * 128]
            suc = jnp.transpose(jnp.broadcast_to(su, (128, 128)))
            val = (jnp.concatenate([suc] * 4, axis=1) * sv).astype(BF16)
            adj[b, t * 128:(t + 1) * 128, :] = adj[b, t * 128:(t + 1) * 128, :] * val

    def block(j, off):
        return col_of(pos - sign(j) * off) * STREAMS + j

    def user_part(k, b):
        ei = jnp.concatenate([ei_all[k, q] for q in range(ROWS)], axis=1)
        return dot_t(ei, adj[b])

    def item_part(k, j, off):
        q = col_of(pos - sign(j) * off)
        item_acc[...] += dot_n(panels[k][q, j], adj[q * STREAMS + j])

    def item_start(k):
        for q in range(ROWS):
            item_send[k, q] = item_acc[:, q * 128:(q + 1) * 128]
        row_send(2 + 2 * k, lambda rr: item_send.at[k, rr], item_recv.at[k, r])
        item_recv[k, r] = item_send[k, r]
        item_acc[...] = jnp.zeros_like(item_acc)

    def item_sum(k):
        row_wait(2 + 2 * k, lambda rr: item_send.at[k, rr], lambda rr: item_recv.at[k, rr])
        tot = item_recv[k, 0] + item_recv[k, 1] + item_recv[k, 2] + item_recv[k, 3]
        return tot.astype(BF16)

    def item_share(k, val):
        ei_all[k + 1, r] = val
        row_send(3 + 2 * k, lambda rr: ei_all.at[k + 1, r], ei_all.at[k + 1, r])

    def item_end(k):
        row_wait(3 + 2 * k, lambda rr: ei_all.at[k + 1, r], lambda rr: ei_all.at[k + 1, rr])

    def rs_begin(k, make):
        for j in ORDER:
            b = block(j, 1)
            if make:
                build(b)
            first[k, j] = user_part(k, b)
            rs_copy(k, j, 0, first.at[k, j]).start()

    def rs_loop(k, lo, hi, make):
        def step(s, carry):
            for j in ORDER:
                b = block(j, s + 2)
                if make:
                    build(b)
                part = user_part(k, b)
                rs_copy(k, j, s).wait_recv()
                slots[k, j, s] = slots[k, j, s] + part
                pltpu.make_async_remote_copy(
                    src_ref=slots.at[k, j, s], dst_ref=slots.at[k, j, s + 1], send_sem=rs_ss.at[k, j, s + 1],
                    recv_sem=rs_rs.at[k, j, s + 1], device_id=ring_dev(j), device_id_type=MESH).start()
            if make:
                for j in ORDER:
                    item_part(0, j, s + 1)
            return carry
        lax.fori_loop(lo, hi, step, 0)

    def rs_end(k, make, then):
        for j in ORDER:
            b = block(j, 8)
            if make:
                build(b)
            part = user_part(k, b)
            rs_copy(k, j, 6).wait_recv()
            then(j, (slots[k, j, 6] + part).astype(BF16))

    def ag_loop(k, lo, hi):
        def step(s, carry):
            for j in ORDER:
                ag_step(k, j, s)
            for j in ORDER:
                item_part(k, j, s + 1)
            return carry
        lax.fori_loop(lo, hi, step, 0)

    def ag_begin(k):
        def then(j, val):
            panels[k][c, j] = val
            ag_copy(k, j, 0).start()
        return then

    def ag_end(k):
        for j in ORDER:
            ag_step(k, j, 6, last=True)
        for j in ORDER:
            item_part(k, j, 7)

    item_acc[...] = jnp.zeros_like(item_acc)
    rs_begin(0, True)
    rs_loop(0, 0, 6, True)
    rs_end(0, True, ag_begin(1))
    for off in (7, 8):
        for j in ORDER:
            item_part(0, j, off)
    item_start(0)
    for j in ORDER:
        item_part(1, j, 0)
    ag_loop(1, 0, 2)
    item_share(0, item_sum(0))
    ag_loop(1, 2, 6)
    ag_end(1)
    item_start(1)
    item_end(0)
    rs_begin(1, False)
    rs_loop(1, 0, 2, False)
    item_share(1, item_sum(1))
    rs_loop(1, 2, 6, False)
    rs_end(1, False, ag_begin(2))
    for j in ORDER:
        item_part(2, j, 0)
    ag_loop(2, 0, 6)
    ag_end(2)
    item_start(2)
    item_end(1)
    rs_begin(2, False)
    rs_loop(2, 0, 2, False)
    last_item = item_sum(2)
    tot = ei_all[0, r].astype(F32) + ei_all[1, r].astype(F32) + ei_all[2, r].astype(F32) + last_item.astype(F32)
    out_item = (tot / (LAYERS + 1)).astype(BF16)
    outi[...] = out_item
    item_share(2, out_item)
    rs_loop(2, 2, 3, False)
    item_end(2)
    iota_i = lax.broadcasted_iota(jnp.int32, (BLK, 128), 0) + c * BLK
    hot = jnp.concatenate([(iota_i == trip[1:2, :]).astype(BF16), (iota_i == trip[2:3, :]).astype(BF16)], axis=1)
    block_items = jnp.concatenate([ei_all[3, q] for q in range(ROWS)], axis=1)
    got = dot_n(block_items, hot).astype(BF16)
    for q in range(ROWS):
        pk[q] = got[q * 16:(q + 1) * 16, :]
    col_send(2, lambda cc: pk.at[r], pk_recv.at[c])
    pk_recv[c] = pk[r]
    rs_loop(2, 3, 5, False)
    col_wait(2, lambda cc: pk.at[r], lambda cc: pk_recv.at[cc])
    psum = pk_recv[0].astype(F32)
    for q in range(1, RING):
        psum = psum + pk_recv[q].astype(F32)
    picks[r] = psum.astype(BF16)
    row_send(8, lambda rr: picks.at[r], picks.at[r])
    base = (r * RING + c) * (STREAMS * BLK)
    ids_a = trip[0:1, :] - base
    for j in range(STREAMS):
        iota_u = lax.broadcasted_iota(jnp.int32, (BLK, 128), 0) + j * BLK
        onehot_a[j] = (iota_u == ids_a).astype(BF16)
    rs_loop(2, 5, 6, False)
    row_wait(8, lambda rr: picks.at[r], lambda rr: picks.at[rr])
    user_vec = []

    def finish(j, val):
        tot = (panel0[c, j].astype(F32) + panel1[c, j].astype(F32) + panel2[c, j].astype(F32) + val.astype(F32))
        out = (tot / (LAYERS + 1)).astype(BF16)
        outu[:, j * BLK:(j + 1) * BLK] = out
        user_vec.append(dot_n(out, onehot_a[j]))

    rs_end(2, False, finish)
    ea = user_vec[0] + user_vec[1] + user_vec[2] + user_vec[3]
    both = jnp.concatenate([picks[q] for q in range(ROWS)], axis=0).astype(F32)
    margin = (jnp.sum(ea * both[:, 0:128], axis=0, keepdims=True)
              - jnp.sum(ea * both[:, 128:256], axis=0, keepdims=True))
    term = jnp.maximum(-margin, 0.0) + jnp.log1p(jnp.exp(-jnp.abs(margin)))
    mine = jnp.logical_and(ids_a >= 0, ids_a < STREAMS * BLK)
    terms[r] = jnp.where(mine, term, 0.0)
    row_send(9, lambda rr: terms.at[r], terms.at[r])
    row_wait(9, lambda rr: terms.at[r], lambda rr: terms.at[rr])
    terms2[c] = terms[0] + terms[1] + terms[2] + terms[3]
    col_send(3, lambda cc: terms2.at[c], terms2.at[c])
    col_wait(3, lambda cc: terms2.at[c], lambda cc: terms2.at[cc])
    tsum = terms2[0]
    for q in range(1, RING):
        tsum = tsum + terms2[q]
    loss[...] = jnp.broadcast_to(jnp.sum(tsum, axis=1, keepdims=True) / tsum.shape[1], loss.shape)

    def drain(s, carry):
        for k in range(LAYERS):
            for j in range(STREAMS):
                ag_copy(k, j, s).wait_send()
                rs_copy(k, j, s).wait_send()
        return carry
    lax.fori_loop(0, RING - 1, drain, 0)


def solution(mesh):
    def local_prog(mask_blk, user_shard, item_shard, triples):
        vmem = pl.BlockSpec(memory_space=pltpu.VMEM)
        dma = pltpu.SemaphoreType.DMA
        outu, outi, loss = pl.pallas_call(
            kernel,
            out_shape=(jax.ShapeDtypeStruct((DIM, STREAMS * BLK), BF16),
                       jax.ShapeDtypeStruct((DIM, 128), BF16),
                       jax.ShapeDtypeStruct((8, 128), F32)),
            in_specs=[pl.BlockSpec(memory_space=pl.ANY), vmem, vmem, vmem],
            out_specs=(vmem, vmem, vmem),
            scratch_shapes=[
                pltpu.VMEM((RING * STREAMS, BLK, BLK), BF16),
                pltpu.VMEM((MASK_BUFS, BLK, BLK), jnp.int32),
                dma((MASK_BUFS,)),
                pltpu.VMEM((RING, STREAMS, DIM, BLK), BF16),
                pltpu.VMEM((RING, STREAMS, DIM, BLK), BF16),
                pltpu.VMEM((RING, STREAMS, DIM, BLK), BF16),
                pltpu.VMEM((LAYERS + 1, ROWS, DIM, 128), BF16),
                pltpu.VMEM((DIM, BLK), F32),
                pltpu.VMEM((LAYERS, ROWS, DIM, 128), F32),
                pltpu.VMEM((LAYERS, ROWS, DIM, 128), F32),
                pltpu.VMEM((LAYERS, STREAMS, RING - 1, DIM, BLK), F32),
                pltpu.VMEM((LAYERS, STREAMS, DIM, BLK), F32),
                pltpu.VMEM((8, BLK), F32),
                pltpu.VMEM((RING * STREAMS, 1, BLK), F32),
                pltpu.VMEM((RING, STREAMS, 1, BLK), F32),
                pltpu.VMEM((RING * STREAMS, 1, BLK), F32),
                pltpu.VMEM((1, BLK), F32),
                pltpu.VMEM((ROWS, 1, BLK), F32),
                pltpu.VMEM((1, BLK), F32),
                pltpu.VMEM((STREAMS, BLK, 128), BF16),
                pltpu.VMEM((ROWS, 16, 256), BF16),
                pltpu.VMEM((RING, 16, 256), BF16),
                pltpu.VMEM((ROWS, 16, 256), BF16),
                pltpu.VMEM((ROWS, 1, 128), F32),
                pltpu.VMEM((RING, 1, 128), F32),
                dma((LAYERS, STREAMS, RING - 1)), dma((LAYERS, STREAMS, RING - 1)),
                dma((LAYERS, STREAMS, RING - 1)), dma((LAYERS, STREAMS, RING - 1)),
                dma((10, ROWS)), dma((10, ROWS)),
                dma((4, RING)), dma((4, RING)),
            ],
            compiler_params=pltpu.CompilerParams(
                collective_id=0, has_side_effects=True, vmem_limit_bytes=60 * 1024 * 1024),
            name="propagate",
        )(mask_blk, user_shard.T, item_shard.T, triples.T)
        return outu.T, outi.T, loss[0, 0]

    return jax.shard_map(local_prog, mesh=mesh,
                         in_specs=(P("row", "col"), P(("row", "col"), None), P(("col", "row"), None), P(None, None)),
                         out_specs=(P(("row", "col"), None), P(("col", "row"), None), P()), check_vma=False)
```

```python
import jax
import jax.numpy as jnp
from jax import lax
from jax.experimental import pallas as pl
from jax.experimental.pallas import tpu as pltpu
from jax.sharding import PartitionSpec as P

LAYERS = 3
RING = 8
ROWS = 4
DEPTH = 4
ROUNDS = 16
AHEAD = 3
DELAY = 8
SUBS = 4
DIM = 64
BLK = 512
MASK_BUFS = 8
MESH = pl.DeviceIdType.MESH
BF16 = jnp.bfloat16
F32 = jnp.float32


def dot_t(lhs, rhs):
    return lax.dot_general(lhs, rhs, (((1,), (1,)), ((), ())), preferred_element_type=F32)


def dot_n(lhs, rhs):
    return lax.dot_general(lhs, rhs, (((1,), (0,)), ((), ())), preferred_element_type=F32)


def kernel(mask_hbm, euT, eiT, trip, outu, outi, loss,
           adj, mbuf, msem,
           panel0, panel1, panel2, ei_all, item_acc, item_send, item_recv,
           ysend, yrecv, zin,
           colsum, deg_part, deg_recv, scale_u, itemdeg, itemdeg_recv, scale_v,
           onehot_a, pk, pk_recv, picks, user_vec, terms, terms2,
           y_ss, y_rs, z_ss, z_rs, ag_sy, ag_s1, ag_s2, ag_rs,
           row_ss, row_rs, col_ss, col_rs):
    c = lax.axis_index("col")
    r = lax.axis_index("row")
    z, y = lax.div(c, 2), lax.rem(c, 2)
    mate = 2 * z + 1 - y
    is_up, is_down = z < DEPTH - 1, z > 0
    is_mid = jnp.logical_and(is_up, is_down)
    row_peers = [lax.rem(r + d, ROWS) for d in range(1, ROWS)]
    col_peers = [lax.rem(c + d, RING) for d in range(1, RING)]
    panels = (panel0, panel1, panel2)

    def mask_copy(i):
        slot = lax.rem(i, MASK_BUFS)
        return pltpu.make_async_copy(mask_hbm.at[pl.ds(i * BLK, BLK), :], mbuf.at[slot], msem.at[slot])

    for i in range(MASK_BUFS):
        mask_copy(i).start()

    barrier = pltpu.get_barrier_semaphore()
    for rr in row_peers:
        pl.semaphore_signal(barrier, inc=1, device_id=(c, rr), device_id_type=MESH)
    for cc in col_peers:
        pl.semaphore_signal(barrier, inc=1, device_id=(cc, r), device_id_type=MESH)

    def remote(src, dst, ss, rs, col):
        return pltpu.make_async_remote_copy(src_ref=src, dst_ref=dst, send_sem=ss, recv_sem=rs,
                                            device_id=(col, r), device_id_type=MESH)

    def ag_y(k, q, col):
        ref = panels[k].at[col, q]
        return remote(ref, ref, ag_sy.at[k, q], ag_rs.at[k, col, q], mate)

    def ag_up(k, col, q):
        ref = panels[k].at[col, q]
        return remote(ref, ref, ag_s1.at[k, col, q], ag_rs.at[k, col, q], c + 2)

    def ag_down(k, col, q):
        ref = panels[k].at[col, q]
        return remote(ref, ref, ag_s1.at[k, col, q], ag_rs.at[k, col, q], c - 2)

    def ag_down2(k, col, q):
        ref = panels[k].at[col, q]
        return remote(ref, ref, ag_s2.at[k, lax.rem(col, 2), q], ag_rs.at[k, col, q], c - 2)

    def ag_both(k, col, q):
        @pl.when(is_up)
        def _():
            ag_up(k, col, q).start()

        @pl.when(is_down)
        def _():
            ag_down2(k, col, q).start()

    def ag_own(k, q):
        ag_y(k, q, c).start()
        ag_both(k, c, q)

    def ag_mate(k, q):
        with jax.named_scope("ag%d_mate" % k):
            ag_y(k, q, mate).wait_recv()
        ag_both(k, mate, q)

    def ag_event(k, e, then):
        d, rest = lax.div(e, 2 * SUBS) + 1, lax.rem(e, 2 * SUBS)
        yy = y + lax.div(rest, SUBS) * (1 - 2 * y)
        q = lax.rem(rest, SUBS)

        @pl.when(z + d < DEPTH)
        def _():
            col = 2 * (z + d) + yy
            with jax.named_scope("ag%d_above" % k):
                ag_down(k, col, q).wait_recv()

            @pl.when(is_down)
            def _():
                ag_down(k, col, q).start()
            then(col, q)

        @pl.when(z - d >= 0)
        def _():
            col = 2 * (z - d) + yy
            with jax.named_scope("ag%d_below" % k):
                ag_up(k, col, q).wait_recv()

            @pl.when(is_up)
            def _():
                ag_up(k, col, q).start()
            then(col, q)

    def row_send(u, src, dst):
        for rr in row_peers:
            pltpu.make_async_remote_copy(src_ref=src(rr), dst_ref=dst, send_sem=row_ss.at[u, rr],
                                         recv_sem=row_rs.at[u, r], device_id=(c, rr), device_id_type=MESH).start()

    def row_wait(u, src, dst):
        with jax.named_scope("row_wait_%d" % u):
            for rr in row_peers:
                cp = pltpu.make_async_remote_copy(src_ref=src(rr), dst_ref=dst(rr), send_sem=row_ss.at[u, rr],
                                                  recv_sem=row_rs.at[u, rr], device_id=(c, rr), device_id_type=MESH)
                cp.wait_recv()
                cp.wait_send()

    def col_send(u, src, dst):
        for cc in col_peers:
            remote(src(cc), dst, col_ss.at[u, cc], col_rs.at[u, c], cc).start()

    def col_wait(u, src, dst):
        with jax.named_scope("col_wait_%d" % u):
            for cc in col_peers:
                cp = remote(src(cc), dst(cc), col_ss.at[u, cc], col_rs.at[u, cc], cc)
                cp.wait_recv()
                cp.wait_send()

    ones = jnp.ones((16, BLK), BF16)
    colsum[...] = jnp.zeros_like(colsum)

    def mask_block(i, carry):
        slot = lax.rem(i, MASK_BUFS)
        mask_copy(i).wait()
        acc = jnp.zeros((8, BLK), F32)
        for t in range(4):
            m = mbuf[slot, t * 128:(t + 1) * 128, :].astype(F32)
            acc = acc + jnp.sum(m.reshape(16, 8, BLK), axis=0)
            adj[i, t * 128:(t + 1) * 128, :] = m.astype(BF16)
        colsum[...] += acc
        deg_part[i] = dot_t(ones, adj[i])[0:1, :]

        @pl.when(i + MASK_BUFS < SUBS * RING)
        def _():
            mask_copy(i + MASK_BUFS).start()
        return carry

    with jax.named_scope("mask0"):
        lax.fori_loop(0, 8, mask_block, 0)
    for q in range(SUBS):
        panel0[c, q] = euT[:, q * BLK:(q + 1) * BLK]
    ei_all[0, r] = eiT[...]
    with jax.named_scope("entry"):
        pl.semaphore_wait(barrier, (ROWS - 1) + (RING - 1))
    for q in range(SUBS):
        ag_own(0, q)
    row_send(0, lambda rr: ei_all.at[0, r], ei_all.at[0, r])
    with jax.named_scope("mask1"):
        lax.fori_loop(8, SUBS * RING, mask_block, 0)

    nothing = lambda col, q: None
    shard = lambda ref, cc: ref.at[pl.ds(cc * SUBS, SUBS)]
    itemdeg[...] = jnp.sum(colsum[...], axis=0, keepdims=True)
    col_send(0, lambda cc: shard(deg_part, cc), deg_recv.at[c])
    row_send(1, lambda rr: itemdeg, itemdeg_recv.at[r])
    itemdeg_recv[r] = itemdeg[...]
    deg_recv[c] = deg_part[pl.ds(c * SUBS, SUBS)]
    for q in range(SUBS):
        ag_mate(0, q)
    row_wait(1, lambda rr: itemdeg, lambda rr: itemdeg_recv.at[rr])
    dv = itemdeg_recv[0] + itemdeg_recv[1] + itemdeg_recv[2] + itemdeg_recv[3]
    scale_v[...] = lax.rsqrt(jnp.maximum(dv, 1.0))
    col_wait(0, lambda cc: shard(deg_part, cc), lambda cc: deg_recv.at[cc])
    du = deg_recv[0]
    for q in range(1, RING):
        du = du + deg_recv[q]
    scale_u[pl.ds(c * SUBS, SUBS)] = lax.rsqrt(jnp.maximum(du, 1.0))
    col_send(1, lambda cc: shard(scale_u, c), shard(scale_u, c))

    def early(e, carry):
        ag_event(0, e, nothing)
        return carry
    lax.fori_loop(0, DELAY, early, 0)
    row_wait(0, lambda rr: ei_all.at[0, r], lambda rr: ei_all.at[0, rr])
    col_wait(1, lambda cc: shard(scale_u, c), lambda cc: shard(scale_u, cc))

    def build(b):
        sv = scale_v[...]
        for t in range(4):
            su = scale_u[b, :, t * 128:(t + 1) * 128]
            suc = jnp.transpose(jnp.broadcast_to(su, (128, 128)))
            val = (jnp.concatenate([suc] * 4, axis=1) * sv).astype(BF16)
            adj[b, t * 128:(t + 1) * 128, :] = adj[b, t * 128:(t + 1) * 128, :] * val

    def user_part(k, b):
        ei = jnp.concatenate([ei_all[k, q] for q in range(ROWS)], axis=1)
        return dot_t(ei, adj[b])

    def item_part(k, col, q):
        item_acc[...] += dot_n(panels[k][col, q], adj[col * SUBS + q])

    def item_start(k):
        for q in range(ROWS):
            item_send[k, q] = item_acc[:, q * 128:(q + 1) * 128]
        row_send(2 + 2 * k, lambda rr: item_send.at[k, rr], item_recv.at[k, r])
        item_recv[k, r] = item_send[k, r]
        item_acc[...] = jnp.zeros_like(item_acc)

    def item_sum(k):
        row_wait(2 + 2 * k, lambda rr: item_send.at[k, rr], lambda rr: item_recv.at[k, rr])
        tot = item_recv[k, 0] + item_recv[k, 1] + item_recv[k, 2] + item_recv[k, 3]
        return tot.astype(BF16)

    def item_share(k, val):
        ei_all[k + 1, r] = val
        row_send(3 + 2 * k, lambda rr: ei_all.at[k + 1, r], ei_all.at[k + 1, r])

    def item_end(k):
        row_wait(3 + 2 * k, lambda rr: ei_all.at[k + 1, r], lambda rr: ei_all.at[k + 1, rr])

    def round_z(i):
        g = lax.div(i, SUBS)
        pw = 1 + 3 * g + 9 * lax.div(g * (g - 1), 2) + 27 * lax.div(g * (g - 1) * (g - 2), 6)
        return lax.rem(lax.div(27 + 48 * z + 57 * lax.div(z, 2), pw), 4)

    def y_copy(k, i):
        t, q = round_z(i), lax.rem(i, SUBS)
        return remote(ysend.at[k, t, q], yrecv.at[k, t, q], y_ss.at[k, t, q], y_rs.at[k, t, q], mate)

    def y_begin(k, i):
        t, q = round_z(i), lax.rem(i, SUBS)
        ysend[k, t, q] = user_part(k, (2 * t + 1 - y) * SUBS + q)
        y_copy(k, i).start()

    def z_up(k, t, q):
        return remote(yrecv.at[k, t, q], zin.at[k, t, q], z_ss.at[k, t, q], z_rs.at[k, t, q], c + 2)

    def z_down(k, t, q):
        to = t + lax.div(2 - (z - 1 - t), 2) * (DEPTH - t)
        return remote(yrecv.at[k, t, q], zin.at[k, to, q], z_ss.at[k, t, q], z_rs.at[k, to, q], c - 2)

    def z_add(k, t, at, q):
        with jax.named_scope("rs%d_z" % k):
            remote(yrecv.at[k, t, q], zin.at[k, at, q], z_ss.at[k, t, q], z_rs.at[k, at, q], mate).wait_recv()
        yrecv[k, t, q] = yrecv[k, t, q] + zin[k, at, q]

    def rs_round(k, i, then):
        t, q = round_z(i), lax.rem(i, SUBS)
        part = user_part(k, (2 * t + y) * SUBS + q)
        with jax.named_scope("rs%d_y" % k):
            y_copy(k, i).wait_recv()
        yrecv[k, t, q] = yrecv[k, t, q] + part

        @pl.when(i < 3 * SUBS)
        def _():
            @pl.when(is_mid)
            def _():
                z_add(k, t, t, q)

            @pl.when(t > z)
            def _():
                z_up(k, t, q).start()

            @pl.when(t < z)
            def _():
                z_down(k, t, q).start()

        @pl.when(i >= 3 * SUBS)
        def _():
            @pl.when(is_down)
            def _():
                z_add(k, z, z, q)

            @pl.when(is_up)
            def _():
                z_add(k, z, DEPTH, q)
            then(q, yrecv[k, z, q].astype(BF16))

    def table_end(k):
        def then(q, val):
            panels[k + 1][c, q] = val
            ag_own(k + 1, q)
        return then

    def build_round(i):
        t, q = round_z(i), lax.rem(i, SUBS)
        build((2 * t + 1 - y) * SUBS + q)
        build((2 * t + y) * SUBS + q)

    item_acc[...] = jnp.zeros_like(item_acc)

    for i in range(2):
        build_round(i)
        y_begin(0, i)
    for i in range(2, AHEAD + 1):
        build_round(i)
        if i < AHEAD:
            y_begin(0, i)

    def round_1(i, carry):
        @pl.when(i + AHEAD < ROUNDS)
        def _():
            y_begin(0, i + AHEAD)
        rs_round(0, i, table_end(0))

        @pl.when(i < 6)
        def _():
            build_round(2 * i + AHEAD + 1)
            build_round(2 * i + AHEAD + 2)

        @pl.when(i < (6 * SUBS - DELAY) // 2)
        def _():
            ag_event(0, DELAY + 2 * i, nothing)
            ag_event(0, DELAY + 2 * i + 1, nothing)

        @pl.when(jnp.logical_and(i >= 8, i < 12))
        def _():
            for a in range(2):
                for q in range(SUBS):
                    item_part(0, 2 * (i - 8) + a, q)

        @pl.when(i == 11)
        def _():
            item_start(0)

        @pl.when(i == 12)
        def _():
            item_share(0, item_sum(0))

        @pl.when(i == 13)
        def _():
            item_end(0)

        @pl.when(i >= 13)
        def _():
            y_begin(1, i - 13)
        return carry
    lax.fori_loop(0, ROUNDS, round_1, 0)

    def gather_round(k, i):
        @pl.when(i < SUBS)
        def _():
            ag_mate(k, i)
            item_part(k, c, i)
            item_part(k, mate, i)

        @pl.when(jnp.logical_and(i >= 1, i < 13))
        def _():
            ag_event(k, 2 * i - 2, lambda col, q: item_part(k, col, q))
            ag_event(k, 2 * i - 1, lambda col, q: item_part(k, col, q))

        @pl.when(i == 12)
        def _():
            item_start(k)

    def round_2(i, carry):
        @pl.when(i + AHEAD < ROUNDS)
        def _():
            y_begin(1, i + AHEAD)
        rs_round(1, i, table_end(1))
        gather_round(1, i)

        @pl.when(i == 13)
        def _():
            item_share(1, item_sum(1))

        @pl.when(i == 14)
        def _():
            item_end(1)

        @pl.when(i >= 14)
        def _():
            y_begin(2, i - 14)
        return carry
    lax.fori_loop(0, ROUNDS, round_2, 0)
    for i in range(2, AHEAD):
        y_begin(2, i)

    base = (r * RING + c) * (SUBS * BLK)
    ids_a = trip[0:1, :] - base
    user_vec[...] = jnp.zeros_like(user_vec)

    def finish(q, val):
        tot = (panel0[c, q].astype(F32) + panel1[c, q].astype(F32) + panel2[c, q].astype(F32) + val.astype(F32))
        out = (tot / (LAYERS + 1)).astype(BF16)
        outu[q] = out
        user_vec[...] += dot_n(out, onehot_a[q])

    def round_3(i, carry):
        @pl.when(i + AHEAD < ROUNDS)
        def _():
            y_begin(2, i + AHEAD)

        @pl.when(i < SUBS)
        def _():
            iota_u = lax.broadcasted_iota(jnp.int32, (BLK, 128), 0) + i * BLK
            onehot_a[i] = (iota_u == ids_a).astype(BF16)
        rs_round(2, i, finish)
        gather_round(2, i)

        @pl.when(i == 13)
        def _():
            last_item = item_sum(2)
            tot = (ei_all[0, r].astype(F32) + ei_all[1, r].astype(F32) + ei_all[2, r].astype(F32)
                   + last_item.astype(F32))
            out_item = (tot / (LAYERS + 1)).astype(BF16)
            outi[...] = out_item
            item_share(2, out_item)

        @pl.when(i == 14)
        def _():
            item_end(2)
            iota_i = lax.broadcasted_iota(jnp.int32, (BLK, 128), 0) + c * BLK
            hot = jnp.concatenate([(iota_i == trip[1:2, :]).astype(BF16), (iota_i == trip[2:3, :]).astype(BF16)],
                                  axis=1)
            got = dot_n(jnp.concatenate([ei_all[3, q] for q in range(ROWS)], axis=1), hot).astype(BF16)
            for q in range(ROWS):
                pk[q] = got[q * 16:(q + 1) * 16, :]
            col_send(2, lambda cc: pk.at[r], pk_recv.at[c])
            pk_recv[c] = pk[r]
        return carry
    lax.fori_loop(0, ROUNDS, round_3, 0)

    col_wait(2, lambda cc: pk.at[r], lambda cc: pk_recv.at[cc])
    psum = pk_recv[0].astype(F32)
    for q in range(1, RING):
        psum = psum + pk_recv[q].astype(F32)
    picks[r] = psum.astype(BF16)
    row_send(8, lambda rr: picks.at[r], picks.at[r])
    row_wait(8, lambda rr: picks.at[r], lambda rr: picks.at[rr])
    ea = user_vec[...]
    both = jnp.concatenate([picks[q] for q in range(ROWS)], axis=0).astype(F32)
    margin = (jnp.sum(ea * both[:, 0:128], axis=0, keepdims=True)
              - jnp.sum(ea * both[:, 128:256], axis=0, keepdims=True))
    term = jnp.maximum(-margin, 0.0) + jnp.log1p(jnp.exp(-jnp.abs(margin)))
    mine = jnp.logical_and(ids_a >= 0, ids_a < SUBS * BLK)
    terms[r] = jnp.where(mine, term, 0.0)
    row_send(9, lambda rr: terms.at[r], terms.at[r])
    row_wait(9, lambda rr: terms.at[r], lambda rr: terms.at[rr])
    terms2[c] = terms[0] + terms[1] + terms[2] + terms[3]
    col_send(3, lambda cc: terms2.at[c], terms2.at[c])

    def drain(i, carry):
        for k in range(LAYERS):
            t, q = round_z(i), lax.rem(i, SUBS)
            y_copy(k, i).wait_send()

            @pl.when(i < 3 * SUBS)
            def _():
                z_up(k, t, q).wait_send()

            @pl.when(i < SUBS)
            def _():
                ag_y(k, i, c).wait_send()
                for col in (c, mate):
                    @pl.when(is_up)
                    def _():
                        ag_up(k, col, i).wait_send()

                    @pl.when(is_down)
                    def _():
                        ag_down2(k, col, i).wait_send()
        return carry
    lax.fori_loop(0, ROUNDS, drain, 0)

    def drain_lines(e, carry):
        d, rest = lax.div(e, 2 * SUBS) + 1, lax.rem(e, 2 * SUBS)
        yy, q = lax.div(rest, SUBS), lax.rem(rest, SUBS)
        for k in range(LAYERS):
            @pl.when(jnp.logical_and(z + d < DEPTH, is_down))
            def _():
                ag_down(k, 2 * (z + d) + yy, q).wait_send()

            @pl.when(jnp.logical_and(z - d >= 0, is_up))
            def _():
                ag_up(k, 2 * (z - d) + yy, q).wait_send()
        return carry
    lax.fori_loop(0, 6 * SUBS, drain_lines, 0)

    col_wait(3, lambda cc: terms2.at[c], lambda cc: terms2.at[cc])
    tsum = terms2[0]
    for q in range(1, RING):
        tsum = tsum + terms2[q]
    loss[...] = jnp.broadcast_to(jnp.sum(tsum, axis=1, keepdims=True) / tsum.shape[1], loss.shape)


def solution(mesh):
    def local_prog(mask_blk, user_shard, item_shard, triples):
        vmem = pl.BlockSpec(memory_space=pltpu.VMEM)
        dma = pltpu.SemaphoreType.DMA
        outu, outi, loss = pl.pallas_call(
            kernel,
            out_shape=(jax.ShapeDtypeStruct((SUBS, DIM, BLK), BF16),
                       jax.ShapeDtypeStruct((DIM, 128), BF16),
                       jax.ShapeDtypeStruct((8, 128), F32)),
            in_specs=[pl.BlockSpec(memory_space=pl.ANY), vmem, vmem, vmem],
            out_specs=(vmem, vmem, vmem),
            scratch_shapes=[
                pltpu.VMEM((RING * SUBS, BLK, BLK), BF16),
                pltpu.VMEM((MASK_BUFS, BLK, BLK), jnp.int32),
                dma((MASK_BUFS,)),
                pltpu.VMEM((RING, SUBS, DIM, BLK), BF16),
                pltpu.VMEM((RING, SUBS, DIM, BLK), BF16),
                pltpu.VMEM((RING, SUBS, DIM, BLK), BF16),
                pltpu.VMEM((LAYERS + 1, ROWS, DIM, 128), BF16),
                pltpu.VMEM((DIM, BLK), F32),
                pltpu.VMEM((LAYERS, ROWS, DIM, 128), F32),
                pltpu.VMEM((LAYERS, ROWS, DIM, 128), F32),
                pltpu.VMEM((LAYERS, DEPTH, SUBS, DIM, BLK), F32),
                pltpu.VMEM((LAYERS, DEPTH, SUBS, DIM, BLK), F32),
                pltpu.VMEM((LAYERS, DEPTH + 1, SUBS, DIM, BLK), F32),
                pltpu.VMEM((8, BLK), F32),
                pltpu.VMEM((RING * SUBS, 1, BLK), F32),
                pltpu.VMEM((RING, SUBS, 1, BLK), F32),
                pltpu.VMEM((RING * SUBS, 1, BLK), F32),
                pltpu.VMEM((1, BLK), F32),
                pltpu.VMEM((ROWS, 1, BLK), F32),
                pltpu.VMEM((1, BLK), F32),
                pltpu.VMEM((SUBS, BLK, 128), BF16),
                pltpu.VMEM((ROWS, 16, 256), BF16),
                pltpu.VMEM((RING, 16, 256), BF16),
                pltpu.VMEM((ROWS, 16, 256), BF16),
                pltpu.VMEM((DIM, 128), F32),
                pltpu.VMEM((ROWS, 1, 128), F32),
                pltpu.VMEM((RING, 1, 128), F32),
                dma((LAYERS, DEPTH, SUBS)), dma((LAYERS, DEPTH, SUBS)),
                dma((LAYERS, DEPTH, SUBS)), dma((LAYERS, DEPTH + 1, SUBS)),
                dma((LAYERS, SUBS)), dma((LAYERS, RING, SUBS)), dma((LAYERS, 2, SUBS)), dma((LAYERS, RING, SUBS)),
                dma((10, ROWS)), dma((10, ROWS)),
                dma((4, RING)), dma((4, RING)),
            ],
            compiler_params=pltpu.CompilerParams(
                collective_id=0, has_side_effects=True, vmem_limit_bytes=61 * 1024 * 1024),
            name="propagate",
        )(mask_blk, user_shard.T, item_shard.T, triples.T)
        out_user = jnp.concatenate([outu[q] for q in range(SUBS)], axis=1).T
        return out_user, outi.T, loss[0, 0]

    return jax.shard_map(local_prog, mesh=mesh,
                         in_specs=(P("row", "col"), P(("row", "col"), None), P(("col", "row"), None), P(None, None)),
                         out_specs=(P(("row", "col"), None), P(("col", "row"), None), P()), check_vma=False)
```

```python
import jax
import jax.numpy as jnp
from jax import lax
from jax.experimental import pallas as pl
from jax.experimental.pallas import tpu as pltpu
from jax.sharding import PartitionSpec as P

LAYERS = 3
RING = 8
ROWS = 4
DEPTH = 4
ROUNDS = 16
AHEAD = 2
SUBS = 4
DIM = 64
BLK = 512
MASK_BUFS = 8
MESH = pl.DeviceIdType.MESH
BF16 = jnp.bfloat16
F32 = jnp.float32


def dot_t(lhs, rhs):
    return lax.dot_general(lhs, rhs, (((1,), (1,)), ((), ())), preferred_element_type=F32)


def dot_n(lhs, rhs):
    return lax.dot_general(lhs, rhs, (((1,), (0,)), ((), ())), preferred_element_type=F32)


def kernel(mask_hbm, euT, eiT, trip, outu, outi, loss,
           adj, mbuf, msem,
           panels, ei_all, item_acc, item_send, item_recv,
           ysend, yrecv, zin,
           colsum, deg_part, deg_recv, scale_u, itemdeg, itemdeg_recv, scale_v,
           onehot_a, pk, pk_recv, picks, user_vec, terms, terms2,
           y_ss, y_rs, z_ss, z_rs, ag_sy, ag_s1, ag_s2, ag_rs,
           row_ss, row_rs, col_ss, col_rs):
    c = lax.axis_index("col")
    r = lax.axis_index("row")
    z, y = lax.div(c, 2), lax.rem(c, 2)
    mate = 2 * z + 1 - y
    is_up, is_down = z < DEPTH - 1, z > 0
    is_mid = jnp.logical_and(is_up, is_down)
    row_peers = [lax.rem(r + d, ROWS) for d in range(1, ROWS)]
    col_peers = [lax.rem(c + d, RING) for d in range(1, RING)]

    def mask_at(i):
        return lax.rem(i, RING) * SUBS + lax.div(i, RING)

    def mask_copy(i):
        slot = lax.rem(i, MASK_BUFS)
        return pltpu.make_async_copy(mask_hbm.at[pl.ds(mask_at(i) * BLK, BLK), :], mbuf.at[slot], msem.at[slot])

    for i in range(MASK_BUFS):
        mask_copy(jnp.int32(i)).start()

    barrier = pltpu.get_barrier_semaphore()
    for rr in row_peers:
        pl.semaphore_signal(barrier, inc=1, device_id=(c, rr), device_id_type=MESH)
    for cc in col_peers:
        pl.semaphore_signal(barrier, inc=1, device_id=(cc, r), device_id_type=MESH)

    def remote(src, dst, ss, rs, col):
        return pltpu.make_async_remote_copy(src_ref=src, dst_ref=dst, send_sem=ss, recv_sem=rs,
                                            device_id=(col, r), device_id_type=MESH)

    def ag_y(k, q, col):
        ref = panels.at[k, col, q]
        return remote(ref, ref, ag_sy.at[k, q], ag_rs.at[k, col, q], mate)

    def ag_up(k, col, q):
        ref = panels.at[k, col, q]
        return remote(ref, ref, ag_s1.at[k, col, q], ag_rs.at[k, col, q], c + 2)

    def ag_down(k, col, q):
        ref = panels.at[k, col, q]
        return remote(ref, ref, ag_s1.at[k, col, q], ag_rs.at[k, col, q], c - 2)

    def ag_down2(k, col, q):
        ref = panels.at[k, col, q]
        return remote(ref, ref, ag_s2.at[k, lax.rem(col, 2), q], ag_rs.at[k, col, q], c - 2)

    def ag_both(k, col, q):
        @pl.when(is_up)
        def _():
            ag_up(k, col, q).start()

        @pl.when(is_down)
        def _():
            ag_down2(k, col, q).start()

    def ag_own(k, q):
        ag_y(k, q, c).start()
        ag_both(k, c, q)

    def ag_mate(k, q):
        with jax.named_scope("ag_mate"):
            ag_y(k, q, mate).wait_recv()
        ag_both(k, mate, q)

    def line_event(k, s, yy, q, above, then):
        col = 2 * s + yy
        if above:
            with jax.named_scope("ag_above"):
                ag_down(k, col, q).wait_recv()

            @pl.when(is_down)
            def _():
                ag_down(k, col, q).start()
        else:
            with jax.named_scope("ag_below"):
                ag_up(k, col, q).wait_recv()

            @pl.when(is_up)
            def _():
                ag_up(k, col, q).start()
        then(col, q)

    def first_event(e, event):
        d, rest = lax.div(e, 2 * SUBS) + 1, lax.rem(e, 2 * SUBS)
        yy = y + lax.div(rest, SUBS) * (1 - 2 * y)
        q = lax.rem(rest, SUBS)

        @pl.when(z + d < DEPTH)
        def _():
            event(z + d, yy, q, True)

        @pl.when(z - d >= 0)
        def _():
            event(z - d, yy, q, False)

    def row_send(u, src, dst):
        for rr in row_peers:
            pltpu.make_async_remote_copy(src_ref=src(rr), dst_ref=dst, send_sem=row_ss.at[u, rr],
                                         recv_sem=row_rs.at[u, r], device_id=(c, rr), device_id_type=MESH).start()

    def row_wait(u, src, dst):
        with jax.named_scope("row_wait_%d" % u):
            for rr in row_peers:
                cp = pltpu.make_async_remote_copy(src_ref=src(rr), dst_ref=dst(rr), send_sem=row_ss.at[u, rr],
                                                  recv_sem=row_rs.at[u, rr], device_id=(c, rr), device_id_type=MESH)
                cp.wait_recv()
                cp.wait_send()

    def col_send(u, src, dst):
        for cc in col_peers:
            remote(src(cc), dst, col_ss.at[u, cc], col_rs.at[u, c], cc).start()

    def col_wait(u, src, dst):
        with jax.named_scope("col_wait_%d" % u):
            for cc in col_peers:
                cp = remote(src(cc), dst(cc), col_ss.at[u, cc], col_rs.at[u, cc], cc)
                cp.wait_recv()
                cp.wait_send()

    ones = jnp.ones((16, BLK), BF16)
    colsum[...] = jnp.zeros_like(colsum)

    def mask_block(i, carry):
        slot, b = lax.rem(i, MASK_BUFS), mask_at(i)
        mask_copy(i).wait()
        acc = jnp.zeros((8, BLK), F32)
        for t in range(4):
            m = mbuf[slot, t * 128:(t + 1) * 128, :].astype(F32)
            acc = acc + jnp.sum(m.reshape(16, 8, BLK), axis=0)
            adj[b, t * 128:(t + 1) * 128, :] = m.astype(BF16)
        colsum[...] += acc
        deg_part[b] = dot_t(ones, adj[b])[0:1, :]

        @pl.when(i + MASK_BUFS < SUBS * RING)
        def _():
            mask_copy(i + MASK_BUFS).start()
        return carry

    def deg_send(q):
        col_send(q, lambda cc: deg_part.at[cc * SUBS + q], deg_recv.at[c, q])
        deg_recv[c, q] = deg_part[c * SUBS + q]

    def deg_sum(q):
        col_wait(q, lambda cc: deg_part.at[cc * SUBS + q], lambda cc: deg_recv.at[cc, q])
        du = deg_recv[0, q]
        for cc in range(1, RING):
            du = du + deg_recv[cc, q]
        scale_u[c * SUBS + q] = lax.rsqrt(jnp.maximum(du, 1.0))
        col_send(SUBS + q, lambda cc: scale_u.at[c * SUBS + q], scale_u.at[c * SUBS + q])

    def deg_end(q):
        col_wait(SUBS + q, lambda cc: scale_u.at[c * SUBS + q], lambda cc: scale_u.at[cc * SUBS + q])

    def mask_quarter(q):
        with jax.named_scope("mask"):
            lax.fori_loop(RING * q, RING * (q + 1), mask_block, 0)

    mask_quarter(0)
    for q in range(SUBS):
        panels[0, c, q] = euT[:, q * BLK:(q + 1) * BLK]
    ei_all[0, r] = eiT[...]
    with jax.named_scope("entry"):
        pl.semaphore_wait(barrier, (ROWS - 1) + (RING - 1))
    deg_send(0)
    for q in range(SUBS):
        ag_own(0, q)
    row_send(0, lambda rr: ei_all.at[0, r], ei_all.at[0, r])
    mask_quarter(1)
    deg_send(1)
    mask_quarter(2)
    deg_send(2)
    deg_sum(0)
    mask_quarter(3)
    itemdeg[...] = jnp.sum(colsum[...], axis=0, keepdims=True)
    row_send(1, lambda rr: itemdeg, itemdeg_recv.at[r])
    deg_send(3)
    itemdeg_recv[r] = itemdeg[...]
    nothing = lambda col, q: None
    deg_sum(1)
    for q in range(SUBS):
        ag_mate(0, q)
    deg_sum(2)
    row_wait(1, lambda rr: itemdeg, lambda rr: itemdeg_recv.at[rr])
    dv = itemdeg_recv[0] + itemdeg_recv[1] + itemdeg_recv[2] + itemdeg_recv[3]
    scale_v[...] = lax.rsqrt(jnp.maximum(dv, 1.0))
    row_wait(0, lambda rr: ei_all.at[0, r], lambda rr: ei_all.at[0, rr])
    deg_end(0)

    def build(b):
        sv = scale_v[...]
        for t in range(4):
            su = scale_u[b, :, t * 128:(t + 1) * 128]
            suc = jnp.transpose(jnp.broadcast_to(su, (128, 128)))
            val = (jnp.concatenate([suc] * 4, axis=1) * sv).astype(BF16)
            adj[b, t * 128:(t + 1) * 128, :] = adj[b, t * 128:(t + 1) * 128, :] * val

    def user_part(k, b):
        ei = jnp.concatenate([ei_all[k, q] for q in range(ROWS)], axis=1)
        return dot_t(ei, adj[b])

    def item_part(k, col, q):
        item_acc[k] += dot_n(panels[k, col, q], adj[col * SUBS + q])

    def item_start(k):
        for q in range(ROWS):
            item_send[k, q] = item_acc[k, :, q * 128:(q + 1) * 128]
        row_send(2 + 2 * k, lambda rr: item_send.at[k, rr], item_recv.at[k, r])
        item_recv[k, r] = item_send[k, r]

    def item_sum(k):
        row_wait(2 + 2 * k, lambda rr: item_send.at[k, rr], lambda rr: item_recv.at[k, rr])
        tot = item_recv[k, 0] + item_recv[k, 1] + item_recv[k, 2] + item_recv[k, 3]
        return tot.astype(BF16)

    def item_share(k, val):
        ei_all[k + 1, r] = val
        row_send(3 + 2 * k, lambda rr: ei_all.at[k + 1, r], ei_all.at[k + 1, r])

    def item_end(k):
        row_wait(3 + 2 * k, lambda rr: ei_all.at[k + 1, r], lambda rr: ei_all.at[k + 1, rr])

    def place(n):
        k, q, g = lax.div(n, ROUNDS), lax.rem(lax.div(n, DEPTH), SUBS), lax.rem(n, DEPTH)
        pw = 1 + 3 * g + 9 * lax.div(g * (g - 1), 2) + 27 * lax.div(g * (g - 1) * (g - 2), 6)
        return k, lax.rem(lax.div(27 + 48 * z + 57 * lax.div(z, 2), pw), DEPTH), q

    def y_copy(n):
        k, t, q = place(n)
        return remote(ysend.at[k, t, q], yrecv.at[k, t, q], y_ss.at[k, t, q], y_rs.at[k, t, q], mate)

    def y_begin(n):
        k, t, q = place(n)
        ysend[k, t, q] = user_part(k, (2 * t + 1 - y) * SUBS + q)
        y_copy(n).start()

    def z_up(k, t, q):
        return remote(yrecv.at[k, t, q], zin.at[k, t, q], z_ss.at[k, t, q], z_rs.at[k, t, q], c + 2)

    def z_down(k, t, q):
        to = t + lax.div(2 - (z - 1 - t), 2) * (DEPTH - t)
        return remote(yrecv.at[k, t, q], zin.at[k, to, q], z_ss.at[k, t, q], z_rs.at[k, to, q], c - 2)

    def z_add(k, t, at, q):
        with jax.named_scope("rs_z"):
            remote(yrecv.at[k, t, q], zin.at[k, at, q], z_ss.at[k, t, q], z_rs.at[k, at, q], mate).wait_recv()
        yrecv[k, t, q] = yrecv[k, t, q] + zin[k, at, q]

    def z_send(k, t, q):
        @pl.when(t > z)
        def _():
            z_up(k, t, q).start()

        @pl.when(t < z)
        def _():
            z_down(k, t, q).start()

    def y_stage(n):
        k, t, q = place(n)
        part = user_part(k, (2 * t + y) * SUBS + q)
        with jax.named_scope("rs_y"):
            y_copy(n).wait_recv()
        yrecv[k, t, q] = yrecv[k, t, q] + part

        @pl.when(jnp.logical_and(jnp.logical_not(is_mid), t != z))
        def _():
            z_send(k, t, q)

    def mid_stage(n):
        k, t, q = place(n)

        @pl.when(t != z)
        def _():
            z_add(k, t, t, q)
            z_send(k, t, q)

    def own_stage(n):
        k, _, q = place(n)

        @pl.when(is_down)
        def _():
            z_add(k, z, z, q)

        @pl.when(is_up)
        def _():
            z_add(k, z, DEPTH, q)
        val = yrecv[k, z, q].astype(BF16)

        @pl.when(k < LAYERS - 1)
        def _():
            panels[k + 1, c, q] = val
            ag_own(k + 1, q)
            item_part(k + 1, c, q)

        @pl.when(k == LAYERS - 1)
        def _():
            tot = (panels[0, c, q].astype(F32) + panels[1, c, q].astype(F32) + panels[2, c, q].astype(F32)
                   + val.astype(F32))
            out = (tot / (LAYERS + 1)).astype(BF16)
            outu[q] = out
            user_vec[...] += dot_n(out, onehot_a[q])

    def build_round(i):
        _, t, q = place(i)
        build((2 * t + 1 - y) * SUBS + q)
        build((2 * t + y) * SUBS + q)

    base = (r * RING + c) * (SUBS * BLK)
    ids_a = trip[0:1, :] - base
    item_acc[...] = jnp.zeros_like(item_acc)
    user_vec[...] = jnp.zeros_like(user_vec)

    def is_middle(s):
        return lax.div(s * (DEPTH - 1 - s), 2)

    own_lag = 7 - 2 * is_middle(z)
    sets = SUBS * (LAYERS - 1)

    def gather_events(n):
        odd = lax.rem(n, 2)
        f = 1 - odd
        yy = y + f * (1 - 2 * y)

        lag = n - (own_lag + 3)
        @pl.when(jnp.logical_and(lax.rem(lag + 32, 4) == 0, jnp.logical_and(lag >= 0, lag < 4 * sets)))
        def _():
            m = lax.div(lag, 4)
            k, q = lax.div(m, SUBS) + 1, lax.rem(m, SUBS)
            ag_mate(k, q)
            item_part(k, mate, q)

        for d in range(1, DEPTH):
            for above in (True, False):
                s = z + d if above else z - d
                late = n - (7 - 2 * is_middle(s) + 3 * f + 2 * d)
                ok = jnp.logical_and(s < DEPTH, s >= 0)
                ok = jnp.logical_and(ok, jnp.logical_and(late >= 0, late < 4 * sets))

                @pl.when(jnp.logical_and(ok, lax.rem(late + 64, 4) == 0))
                def _():
                    m = lax.div(late, 4)
                    k, q = lax.div(m, SUBS) + 1, lax.rem(m, SUBS)
                    line_event(k, s, yy, q, above, lambda col, q: item_part(k, col, q))

    for i in range(AHEAD):
        build_round(jnp.int32(i))
        y_begin(jnp.int32(i))
    for i in range(AHEAD, 4):
        build_round(jnp.int32(i))
    deg_sum(3)

    def when_at(n, i):
        return pl.when(n == i)

    def one_round(n, carry):
        @when_at(n, 0)
        def _():
            deg_end(1)

        @when_at(n, 2)
        def _():
            deg_end(2)

        @when_at(n, 4)
        def _():
            deg_end(3)

        @when_at(n, 13)
        def _():
            item_share(0, item_sum(0))

        @when_at(n, 14)
        def _():
            item_end(0)

        @when_at(n, 29)
        def _():
            item_share(1, item_sum(1))

        @when_at(n, 30)
        def _():
            item_end(1)

        @when_at(n, 45)
        def _():
            last_item = item_sum(2)
            tot = (ei_all[0, r].astype(F32) + ei_all[1, r].astype(F32) + ei_all[2, r].astype(F32)
                   + last_item.astype(F32))
            out_item = (tot / (LAYERS + 1)).astype(BF16)
            outi[...] = out_item
            item_share(2, out_item)

        @when_at(n, 46)
        def _():
            item_end(2)
            iota_i = lax.broadcasted_iota(jnp.int32, (BLK, 128), 0) + c * BLK
            hot = jnp.concatenate([(iota_i == trip[1:2, :]).astype(BF16), (iota_i == trip[2:3, :]).astype(BF16)],
                                  axis=1)
            got = dot_n(jnp.concatenate([ei_all[3, q] for q in range(ROWS)], axis=1), hot).astype(BF16)
            for q in range(ROWS):
                pk[q] = got[q * 16:(q + 1) * 16, :]
            col_send(2 * SUBS, lambda cc: pk.at[r], pk_recv.at[c])
            pk_recv[c] = pk[r]

        @when_at(n, 48)
        def _():
            col_wait(2 * SUBS, lambda cc: pk.at[r], lambda cc: pk_recv.at[cc])
            psum = pk_recv[0].astype(F32)
            for q in range(1, RING):
                psum = psum + pk_recv[q].astype(F32)
            picks[r] = psum.astype(BF16)
            row_send(8, lambda rr: picks.at[r], picks.at[r])

        @pl.when(n + AHEAD < LAYERS * ROUNDS)
        def _():
            y_begin(n + AHEAD)

        @pl.when(n < LAYERS * ROUNDS)
        def _():
            y_stage(n)

        @pl.when(jnp.logical_and(is_mid, jnp.logical_and(n >= 2, n < LAYERS * ROUNDS + 2)))
        def _():
            mid_stage(n - 2)
        own = n - own_lag + 3

        @pl.when(jnp.logical_and(lax.rem(own + 4, 4) == 3, jnp.logical_and(own >= 0, own < LAYERS * ROUNDS)))
        def _():
            own_stage(own)
        gather_events(n)

        @pl.when(n < 6)
        def _():
            build_round(2 * n + 4)
            build_round(2 * n + 5)

            @pl.loop(2 * n, 2 * n + 2)
            def _(e):
                first_event(e, lambda s, yy, q, above: line_event(0, s, yy, q, above, nothing))

        @pl.when(jnp.logical_and(n >= 6, n < 12))
        def _():
            @pl.loop(2 * n, 2 * n + 2)
            def _(e):
                first_event(e, lambda s, yy, q, above: line_event(
                    0, s, yy, q, above, lambda col, q: item_part(0, col, q)))

            @pl.loop(2 * n - 12, 2 * n - 10)
            def _(e):
                first_event(e, lambda s, yy, q, above: item_part(0, 2 * s + yy, q))

        @pl.when(jnp.logical_and(n >= 6, n < 10))
        def _():
            item_part(0, c, n - 6)
            item_part(0, mate, n - 6)

        @when_at(n, 12)
        def _():
            item_start(0)

        @when_at(n, 28)
        def _():
            item_start(1)

        @pl.when(jnp.logical_and(n >= 32, n < 32 + SUBS))
        def _():
            iota_u = lax.broadcasted_iota(jnp.int32, (BLK, 128), 0) + (n - 32) * BLK
            onehot_a[n - 32] = (iota_u == ids_a).astype(BF16)

        @when_at(n, 44)
        def _():
            item_start(2)
        return carry
    lax.fori_loop(0, LAYERS * ROUNDS + 4, one_round, 0)

    row_wait(8, lambda rr: picks.at[r], lambda rr: picks.at[rr])
    ea = user_vec[...]
    both = jnp.concatenate([picks[q] for q in range(ROWS)], axis=0).astype(F32)
    margin = (jnp.sum(ea * both[:, 0:128], axis=0, keepdims=True)
              - jnp.sum(ea * both[:, 128:256], axis=0, keepdims=True))
    term = jnp.maximum(-margin, 0.0) + jnp.log1p(jnp.exp(-jnp.abs(margin)))
    mine = jnp.logical_and(ids_a >= 0, ids_a < SUBS * BLK)
    terms[r] = jnp.where(mine, term, 0.0)
    row_send(9, lambda rr: terms.at[r], terms.at[r])
    row_wait(9, lambda rr: terms.at[r], lambda rr: terms.at[rr])
    terms2[c] = terms[0] + terms[1] + terms[2] + terms[3]
    col_send(2 * SUBS + 1, lambda cc: terms2.at[c], terms2.at[c])

    def drain(n, carry):
        k, t, q = place(n)
        y_copy(n).wait_send()

        @pl.when(t != z)
        def _():
            z_up(k, t, q).wait_send()
        return carry
    lax.fori_loop(0, LAYERS * ROUNDS, drain, 0)

    def drain_own(q, carry):
        for k in range(LAYERS):
            ag_y(k, q, c).wait_send()
            for col in (c, mate):
                @pl.when(is_up)
                def _():
                    ag_up(k, col, q).wait_send()

                @pl.when(is_down)
                def _():
                    ag_down2(k, col, q).wait_send()
        return carry
    lax.fori_loop(0, SUBS, drain_own, 0)

    def drain_lines(e, carry):
        d, rest = lax.div(e, 2 * SUBS) + 1, lax.rem(e, 2 * SUBS)
        yy, q = lax.div(rest, SUBS), lax.rem(rest, SUBS)
        for k in range(LAYERS):
            @pl.when(jnp.logical_and(z + d < DEPTH, is_down))
            def _():
                ag_down(k, 2 * (z + d) + yy, q).wait_send()

            @pl.when(jnp.logical_and(z - d >= 0, is_up))
            def _():
                ag_up(k, 2 * (z - d) + yy, q).wait_send()
        return carry
    lax.fori_loop(0, 6 * SUBS, drain_lines, 0)

    col_wait(2 * SUBS + 1, lambda cc: terms2.at[c], lambda cc: terms2.at[cc])
    tsum = terms2[0]
    for q in range(1, RING):
        tsum = tsum + terms2[q]
    loss[...] = jnp.broadcast_to(jnp.sum(tsum, axis=1, keepdims=True) / tsum.shape[1], loss.shape)


def solution(mesh):
    def local_prog(mask_blk, user_shard, item_shard, triples):
        vmem = pl.BlockSpec(memory_space=pltpu.VMEM)
        dma = pltpu.SemaphoreType.DMA
        outu, outi, loss = pl.pallas_call(
            kernel,
            out_shape=(jax.ShapeDtypeStruct((SUBS, DIM, BLK), BF16),
                       jax.ShapeDtypeStruct((DIM, 128), BF16),
                       jax.ShapeDtypeStruct((8, 128), F32)),
            in_specs=[pl.BlockSpec(memory_space=pl.ANY), vmem, vmem, vmem],
            out_specs=(vmem, vmem, vmem),
            scratch_shapes=[
                pltpu.VMEM((RING * SUBS, BLK, BLK), BF16),
                pltpu.VMEM((MASK_BUFS, BLK, BLK), jnp.int32),
                dma((MASK_BUFS,)),
                pltpu.VMEM((LAYERS, RING, SUBS, DIM, BLK), BF16),
                pltpu.VMEM((LAYERS + 1, ROWS, DIM, 128), BF16),
                pltpu.VMEM((LAYERS, DIM, BLK), F32),
                pltpu.VMEM((LAYERS, ROWS, DIM, 128), F32),
                pltpu.VMEM((LAYERS, ROWS, DIM, 128), F32),
                pltpu.VMEM((LAYERS, DEPTH, SUBS, DIM, BLK), F32),
                pltpu.VMEM((LAYERS, DEPTH, SUBS, DIM, BLK), F32),
                pltpu.VMEM((LAYERS, DEPTH + 1, SUBS, DIM, BLK), F32),
                pltpu.VMEM((8, BLK), F32),
                pltpu.VMEM((RING * SUBS, 1, BLK), F32),
                pltpu.VMEM((RING, SUBS, 1, BLK), F32),
                pltpu.VMEM((RING * SUBS, 1, BLK), F32),
                pltpu.VMEM((1, BLK), F32),
                pltpu.VMEM((ROWS, 1, BLK), F32),
                pltpu.VMEM((1, BLK), F32),
                pltpu.VMEM((SUBS, BLK, 128), BF16),
                pltpu.VMEM((ROWS, 16, 256), BF16),
                pltpu.VMEM((RING, 16, 256), BF16),
                pltpu.VMEM((ROWS, 16, 256), BF16),
                pltpu.VMEM((DIM, 128), F32),
                pltpu.VMEM((ROWS, 1, 128), F32),
                pltpu.VMEM((RING, 1, 128), F32),
                dma((LAYERS, DEPTH, SUBS)), dma((LAYERS, DEPTH, SUBS)),
                dma((LAYERS, DEPTH, SUBS)), dma((LAYERS, DEPTH + 1, SUBS)),
                dma((LAYERS, SUBS)), dma((LAYERS, RING, SUBS)), dma((LAYERS, 2, SUBS)), dma((LAYERS, RING, SUBS)),
                dma((10, ROWS)), dma((10, ROWS)),
                dma((2 * SUBS + 2, RING)), dma((2 * SUBS + 2, RING)),
            ],
            compiler_params=pltpu.CompilerParams(
                collective_id=0, has_side_effects=True, vmem_limit_bytes=61 * 1024 * 1024),
            name="propagate",
        )(mask_blk, user_shard.T, item_shard.T, triples.T)
        out_user = jnp.concatenate([outu[q] for q in range(SUBS)], axis=1).T
        return out_user, outi.T, loss[0, 0]

    return jax.shard_map(local_prog, mesh=mesh,
                         in_specs=(P("row", "col"), P(("row", "col"), None), P(("col", "row"), None), P(None, None)),
                         out_specs=(P(("row", "col"), None), P(("col", "row"), None), P()), check_vma=False)
```

```python
import jax
import jax.numpy as jnp
from jax import lax
from jax.experimental import pallas as pl
from jax.experimental.pallas import tpu as pltpu
from jax.sharding import PartitionSpec as P

LAYERS = 3
RING = 8
ROWS = 4
DEPTH = 4
ROUNDS = 16
AHEAD = 2
Y_SEMS = 8
SUBS = 4
DIM = 64
BLK = 512
MASK_BUFS = 8
MESH = pl.DeviceIdType.MESH
BF16 = jnp.bfloat16
F32 = jnp.float32


def dot_t(lhs, rhs):
    return lax.dot_general(lhs, rhs, (((1,), (1,)), ((), ())), preferred_element_type=F32)


def dot_n(lhs, rhs):
    return lax.dot_general(lhs, rhs, (((1,), (0,)), ((), ())), preferred_element_type=F32)


def kernel(mask_hbm, euT, eiT, trip, outu, outi, loss,
           adj, mbuf, msem,
           panels, ei_all, item_acc, item_send, item_recv,
           ysend, yrecv, zin,
           colsum, deg_part, deg_recv, scale_u, itemdeg, itemdeg_recv, scale_v,
           onehot_a, pk, pk_recv, picks, user_vec, terms, terms2,
           y_ss, y_rs, z_ss, z_rs, ag_sy, ag_su, ag_sd, ag_rs,
           row_ss, row_rs, col_ss, col_rs):
    c = lax.axis_index("col")
    r = lax.axis_index("row")
    z, y = lax.div(c, 2), lax.rem(c, 2)
    mate = 2 * z + 1 - y
    is_up, is_down = z < DEPTH - 1, z > 0
    is_mid = jnp.logical_and(is_up, is_down)
    row_peers = [lax.rem(r + d, ROWS) for d in range(1, ROWS)]
    col_peers = [lax.rem(c + d, RING) for d in range(1, RING)]

    def mask_at(i):
        return lax.rem(i, RING) * SUBS + lax.div(i, RING)

    def mask_copy(i):
        slot = lax.rem(i, MASK_BUFS)
        return pltpu.make_async_copy(mask_hbm.at[pl.ds(mask_at(i) * BLK, BLK), :], mbuf.at[slot], msem.at[slot])

    for i in range(MASK_BUFS):
        mask_copy(jnp.int32(i)).start()

    barrier = pltpu.get_barrier_semaphore()
    for rr in row_peers:
        pl.semaphore_signal(barrier, inc=1, device_id=(c, rr), device_id_type=MESH)
    for cc in col_peers:
        pl.semaphore_signal(barrier, inc=1, device_id=(cc, r), device_id_type=MESH)

    def remote(src, dst, ss, rs, col):
        return pltpu.make_async_remote_copy(src_ref=src, dst_ref=dst, send_sem=ss, recv_sem=rs,
                                            device_id=(col, r), device_id_type=MESH)

    def ag_rs_of(k, col, q):
        return ag_rs.at[lax.div(k + 1, 2), col, q]

    def ag_y(k, q, col):
        ref = panels.at[k, col, q]
        return remote(ref, ref, ag_sy, ag_rs_of(k, col, q), mate)

    def ag_up(k, col, q):
        ref = panels.at[k, col, q]
        return remote(ref, ref, ag_su, ag_rs_of(k, col, q), c + 2)

    def ag_down(k, col, q):
        ref = panels.at[k, col, q]
        return remote(ref, ref, ag_sd, ag_rs_of(k, col, q), c - 2)

    def ag_both(k, col, q):
        @pl.when(is_up)
        def _():
            ag_up(k, col, q).start()

        @pl.when(is_down)
        def _():
            ag_down(k, col, q).start()

    def ag_own(k, q):
        ag_y(k, q, c).start()
        ag_both(k, c, q)

    def ag_mate(k, q):
        with jax.named_scope("ag_mate"):
            ag_y(k, q, mate).wait_recv()
        ag_both(k, mate, q)

    def line_event(k, s, yy, q, above, then):
        col = 2 * s + yy
        if above:
            with jax.named_scope("ag_above"):
                ag_down(k, col, q).wait_recv()

            @pl.when(is_down)
            def _():
                ag_down(k, col, q).start()
        else:
            with jax.named_scope("ag_below"):
                ag_up(k, col, q).wait_recv()

            @pl.when(is_up)
            def _():
                ag_up(k, col, q).start()
        then(col, q)

    def first_event(e, event):
        d, rest = lax.div(e, 2 * SUBS) + 1, lax.rem(e, 2 * SUBS)
        yy = y + lax.div(rest, SUBS) * (1 - 2 * y)
        q = lax.rem(rest, SUBS)

        @pl.when(z + d < DEPTH)
        def _():
            event(z + d, yy, q, True)

        @pl.when(z - d >= 0)
        def _():
            event(z - d, yy, q, False)

    def row_send(u, src, dst):
        for rr in row_peers:
            pltpu.make_async_remote_copy(src_ref=src(rr), dst_ref=dst, send_sem=row_ss.at[u], recv_sem=row_rs.at[u],
                                         device_id=(c, rr), device_id_type=MESH).start()

    def row_wait(u, ref):
        with jax.named_scope("row_wait_%d" % u):
            cp = pltpu.make_async_remote_copy(src_ref=ref, dst_ref=ref, send_sem=row_ss.at[u], recv_sem=row_rs.at[u],
                                              device_id=(c, row_peers[0]), device_id_type=MESH)
            cp.wait_recv()
            cp.wait_send()

    def col_send(u, src, dst):
        for cc in col_peers:
            remote(src(cc), dst, col_ss.at[u], col_rs.at[u], cc).start()

    def col_wait(u, ref):
        with jax.named_scope("col_wait_%d" % u):
            cp = remote(ref, ref, col_ss.at[u], col_rs.at[u], mate)
            cp.wait_recv()
            cp.wait_send()

    ones = jnp.ones((16, BLK), BF16)
    colsum[...] = jnp.zeros_like(colsum)

    def mask_block(i, carry):
        slot, b = lax.rem(i, MASK_BUFS), mask_at(i)
        mask_copy(i).wait()
        acc = jnp.zeros((8, BLK), F32)
        for t in range(4):
            m = mbuf[slot, t * 128:(t + 1) * 128, :].astype(F32)
            acc = acc + jnp.sum(m.reshape(16, 8, BLK), axis=0)
            adj[b, t * 128:(t + 1) * 128, :] = m.astype(BF16)
        colsum[...] += acc
        deg_part[b] = dot_t(ones, adj[b])[0:1, :]

        @pl.when(i + MASK_BUFS < SUBS * RING)
        def _():
            mask_copy(i + MASK_BUFS).start()
        return carry

    def deg_send(q):
        col_send(q, lambda cc: deg_part.at[cc * SUBS + q], deg_recv.at[c, q])
        deg_recv[c, q] = deg_part[c * SUBS + q]

    def deg_sum(q):
        col_wait(q, deg_part.at[pl.ds(0, RING - 1)])
        du = deg_recv[0, q]
        for cc in range(1, RING):
            du = du + deg_recv[cc, q]
        scale_u[c * SUBS + q] = lax.rsqrt(jnp.maximum(du, 1.0))
        col_send(SUBS + q, lambda cc: scale_u.at[c * SUBS + q], scale_u.at[c * SUBS + q])

    def deg_end(q):
        col_wait(SUBS + q, deg_part.at[pl.ds(0, RING - 1)])

    def mask_quarter(q):
        with jax.named_scope("mask"):
            lax.fori_loop(RING * q, RING * (q + 1), mask_block, 0)

    def early_event(e):
        first_event(jnp.int32(e), lambda s, yy, q, above: line_event(0, s, yy, q, above, lambda col, q: None))

    mask_quarter(0)
    for q in range(SUBS):
        panels[0, c, q] = euT[:, q * BLK:(q + 1) * BLK]
    ei_all[0, r] = eiT[...]
    with jax.named_scope("entry"):
        pl.semaphore_wait(barrier, (ROWS - 1) + (RING - 1))
    deg_send(0)
    ag_own(0, 0)
    ag_own(0, 1)
    row_send(0, lambda rr: ei_all.at[0, r], ei_all.at[0, r])
    mask_quarter(1)
    deg_send(1)
    ag_own(0, 2)
    mask_quarter(2)
    deg_send(2)
    ag_own(0, 3)
    deg_sum(0)
    for q in range(2):
        ag_mate(0, q)
        early_event(q)
    mask_quarter(3)
    itemdeg[...] = jnp.sum(colsum[...], axis=0, keepdims=True)
    row_send(1, lambda rr: itemdeg, itemdeg_recv.at[r])
    deg_send(3)
    itemdeg_recv[r] = itemdeg[...]
    deg_sum(1)
    row_wait(1, itemdeg_recv.at[pl.ds(0, ROWS - 1)])
    dv = itemdeg_recv[0] + itemdeg_recv[1] + itemdeg_recv[2] + itemdeg_recv[3]
    scale_v[...] = lax.rsqrt(jnp.maximum(dv, 1.0))
    row_wait(0, ei_all.at[0, pl.ds(0, ROWS - 1)])
    deg_end(0)

    def build(b):
        sv = scale_v[...]
        for t in range(4):
            su = scale_u[b, :, t * 128:(t + 1) * 128]
            suc = jnp.transpose(jnp.broadcast_to(su, (128, 128)))
            val = (jnp.concatenate([suc] * 4, axis=1) * sv).astype(BF16)
            adj[b, t * 128:(t + 1) * 128, :] = adj[b, t * 128:(t + 1) * 128, :] * val

    def user_part(k, b):
        ei = jnp.concatenate([ei_all[k, q] for q in range(ROWS)], axis=1)
        return dot_t(ei, adj[b])

    def item_part(k, col, q):
        item_acc[k] += dot_n(panels[k, col, q], adj[col * SUBS + q])

    def item_start(k):
        for q in range(ROWS):
            item_send[k, q] = item_acc[k, :, q * 128:(q + 1) * 128]
        row_send(2 + 2 * k, lambda rr: item_send.at[k, rr], item_recv.at[k, r])
        item_recv[k, r] = item_send[k, r]

    def item_sum(k):
        row_wait(2 + 2 * k, item_send.at[k, pl.ds(0, ROWS - 1)])
        tot = item_recv[k, 0] + item_recv[k, 1] + item_recv[k, 2] + item_recv[k, 3]
        return tot.astype(BF16)

    def item_share(k, val):
        ei_all[k + 1, r] = val
        row_send(3 + 2 * k, lambda rr: ei_all.at[k + 1, r], ei_all.at[k + 1, r])

    def item_end(k):
        row_wait(3 + 2 * k, ei_all.at[k + 1, pl.ds(0, ROWS - 1)])

    def place(n):
        k, i = lax.div(n, ROUNDS), lax.rem(n, ROUNDS)
        last, own = lax.div(k, LAYERS - 1), lax.div(i, 12)
        q, g = lax.div(i, 4), lax.rem(i, 4)
        q_last = (1 - own) * lax.div(i, 3) + own * (i - 12)
        g_last = (1 - own) * lax.rem(i, 3) + own * 3
        q, g = q + last * (q_last - q), g + last * (g_last - g)
        pw = 1 + 3 * g + 9 * lax.div(g * (g - 1), 2) + 27 * lax.div(g * (g - 1) * (g - 2), 6)
        return k, lax.rem(lax.div(27 + 48 * z + 57 * lax.div(z, 2), pw), DEPTH), q

    def y_copy(n):
        k, t, q = place(n)
        return remote(ysend.at[k, t, q], yrecv.at[k, t, q], y_ss, y_rs.at[lax.rem(n, Y_SEMS)], mate)

    def y_begin(n):
        k, t, q = place(n)
        ysend[k, t, q] = user_part(k, (2 * t + 1 - y) * SUBS + q)
        y_copy(n).start()

    def z_up(k, t, q):
        return remote(yrecv.at[k, t, q], zin.at[k, t, q], z_ss, z_rs.at[t, q], c + 2)

    def z_down(k, t, q):
        to = t + lax.div(2 - (z - 1 - t), 2) * (DEPTH - t)
        return remote(yrecv.at[k, t, q], zin.at[k, to, q], z_ss, z_rs.at[to, q], c - 2)

    def z_add(k, t, at, q):
        with jax.named_scope("rs_z"):
            remote(yrecv.at[k, t, q], zin.at[k, at, q], z_ss, z_rs.at[at, q], mate).wait_recv()
        yrecv[k, t, q] = yrecv[k, t, q] + zin[k, at, q]

    def z_send(k, t, q):
        @pl.when(t > z)
        def _():
            z_up(k, t, q).start()

        @pl.when(t < z)
        def _():
            z_down(k, t, q).start()

    def y_stage(n):
        k, t, q = place(n)
        part = user_part(k, (2 * t + y) * SUBS + q)
        with jax.named_scope("rs_y"):
            y_copy(n).wait_recv()
        yrecv[k, t, q] = yrecv[k, t, q] + part

        @pl.when(jnp.logical_and(jnp.logical_not(is_mid), t != z))
        def _():
            z_send(k, t, q)

    def mid_stage(n):
        k, t, q = place(n)

        @pl.when(t != z)
        def _():
            z_add(k, t, t, q)
            z_send(k, t, q)

    def own_stage(n):
        k, _, q = place(n)

        @pl.when(is_down)
        def _():
            z_add(k, z, z, q)

        @pl.when(is_up)
        def _():
            z_add(k, z, DEPTH, q)
        val = yrecv[k, z, q].astype(BF16)

        @pl.when(k < LAYERS - 1)
        def _():
            panels[k + 1, c, q] = val
            ag_own(k + 1, q)
            item_part(k + 1, c, q)

        @pl.when(k == LAYERS - 1)
        def _():
            tot = (panels[0, c, q].astype(F32) + panels[1, c, q].astype(F32) + panels[2, c, q].astype(F32)
                   + val.astype(F32))
            out = (tot / (LAYERS + 1)).astype(BF16)
            outu[q] = out
            user_vec[...] += dot_n(out, onehot_a[q])

    def build_round(i):
        _, t, q = place(i)
        build((2 * t + 1 - y) * SUBS + q)
        build((2 * t + y) * SUBS + q)

    base = (r * RING + c) * (SUBS * BLK)
    ids_a = trip[0:1, :] - base
    item_acc[...] = jnp.zeros_like(item_acc)
    user_vec[...] = jnp.zeros_like(user_vec)

    def is_middle(s):
        return lax.div(s * (DEPTH - 1 - s), 2)

    own_lag = 7 - 2 * is_middle(z)
    sets = SUBS * (LAYERS - 1)

    def gather_events(n):
        odd = lax.rem(n, 2)
        f = 1 - odd
        yy = y + f * (1 - 2 * y)

        lag = n - (own_lag + 3)
        @pl.when(jnp.logical_and(lax.rem(lag + 32, 4) == 0, jnp.logical_and(lag >= 0, lag < 4 * sets)))
        def _():
            m = lax.div(lag, 4)
            k, q = lax.div(m, SUBS) + 1, lax.rem(m, SUBS)
            ag_mate(k, q)
            item_part(k, mate, q)

        for d in range(1, DEPTH):
            for above in (True, False):
                s = z + d if above else z - d
                late = n - (7 - 2 * is_middle(s) + 3 * f + 2 * d)
                ok = jnp.logical_and(s < DEPTH, s >= 0)
                ok = jnp.logical_and(ok, jnp.logical_and(late >= 0, late < 4 * sets))

                @pl.when(jnp.logical_and(ok, lax.rem(late + 64, 4) == 0))
                def _():
                    m = lax.div(late, 4)
                    k, q = lax.div(m, SUBS) + 1, lax.rem(m, SUBS)
                    line_event(k, s, yy, q, above, lambda col, q: item_part(k, col, q))

    for i in range(AHEAD):
        build_round(jnp.int32(i))
        y_begin(jnp.int32(i))
    for i in range(AHEAD, 4):
        build_round(jnp.int32(i))
    deg_sum(2)
    for q in range(2, SUBS):
        ag_mate(0, q)
        early_event(q)

    def when_at(n, i):
        return pl.when(n == i)

    def one_round(n, carry):
        @when_at(n, 1)
        def _():
            deg_end(1)
            deg_sum(3)

        @when_at(n, 3)
        def _():
            deg_end(2)

        @when_at(n, 5)
        def _():
            deg_end(3)

        @when_at(n, 13)
        def _():
            item_end(0)

        @when_at(n, 29)
        def _():
            item_share(1, item_sum(1))

        @when_at(n, 30)
        def _():
            item_end(1)

        @pl.when(n + AHEAD < LAYERS * ROUNDS)
        def _():
            y_begin(n + AHEAD)

        y_stage(n)

        @pl.when(jnp.logical_and(is_mid, n >= 2))
        def _():
            mid_stage(n - 2)
        own = n - own_lag + 3

        @pl.when(jnp.logical_and(lax.rem(own + 4, 4) == 3, jnp.logical_and(own >= 0, own < 2 * ROUNDS)))
        def _():
            own_stage(own)
        gather_events(n)

        @when_at(n, 47)
        def _():
            col_wait(2 * SUBS, pk_recv.at[pl.ds(0, RING - 1)])
            psum = pk_recv[0].astype(F32)
            for q in range(1, RING):
                psum = psum + pk_recv[q].astype(F32)
            picks[r] = psum.astype(BF16)
            row_send(8, lambda rr: picks.at[r], picks.at[r])

        @pl.when(n >= LAYERS * ROUNDS - SUBS)
        def _():
            own_stage(n)

        @pl.when(jnp.logical_and(n >= 1, n < 7))
        def _():
            build_round(2 * n + 2)
            build_round(2 * n + 3)

        @pl.when(n < 6)
        def _():
            early_event(2 * n + 4)
            early_event(2 * n + 5)

        def late_event(e):
            first_event(e, lambda s, yy, q, above: line_event(
                0, s, yy, q, above, lambda col, q: item_part(0, col, q)))

        def old_event(e):
            first_event(e, lambda s, yy, q, above: item_part(0, 2 * s + yy, q))

        @pl.when(jnp.logical_and(n >= 6, n < 11))
        def _():
            e = 16 + (n - 6) + lax.div(n - 6, 3) + lax.div(n - 6, 4)
            late_event(e)

            @pl.when(n >= 8)
            def _():
                late_event(e + 1)

        @pl.when(jnp.logical_and(n >= 1, n < 9))
        def _():
            q, side = lax.div(n - 1, 2), lax.rem(n - 1, 2)
            item_part(0, c + side * (mate - c), q)
            old_event(q + 4 * side)

        @pl.when(jnp.logical_and(n >= 4, n < 11))
        def _():
            old_event(n + 4 + lax.div(n, 9))

            @pl.when(n == 8)
            def _():
                old_event(n + 5)

        @when_at(n, 10)
        def _():
            item_start(0)

        @when_at(n, 11)
        def _():
            item_share(0, item_sum(0))

        @when_at(n, 28)
        def _():
            item_start(1)

        @pl.when(jnp.logical_and(n >= 32, n < 32 + SUBS))
        def _():
            iota_u = lax.broadcasted_iota(jnp.int32, (BLK, 128), 0) + (n - 32) * BLK
            onehot_a[n - 32] = (iota_u == ids_a).astype(BF16)

        @when_at(n, 45)
        def _():
            last_item = item_sum(2)
            tot = (ei_all[0, r].astype(F32) + ei_all[1, r].astype(F32) + ei_all[2, r].astype(F32)
                   + last_item.astype(F32))
            out_item = (tot / (LAYERS + 1)).astype(BF16)
            outi[...] = out_item
            item_share(2, out_item)

        @when_at(n, 46)
        def _():
            item_end(2)
            iota_i = lax.broadcasted_iota(jnp.int32, (BLK, 128), 0) + c * BLK
            hot = jnp.concatenate([(iota_i == trip[1:2, :]).astype(BF16), (iota_i == trip[2:3, :]).astype(BF16)],
                                  axis=1)
            got = dot_n(jnp.concatenate([ei_all[3, q] for q in range(ROWS)], axis=1), hot).astype(BF16)
            for q in range(ROWS):
                pk[q] = got[q * 16:(q + 1) * 16, :]
            col_send(2 * SUBS, lambda cc: pk.at[r], pk_recv.at[c])
            pk_recv[c] = pk[r]

        @when_at(n, 44)
        def _():
            item_start(2)
        return carry
    lax.fori_loop(0, LAYERS * ROUNDS, one_round, 0)

    row_wait(8, picks.at[pl.ds(0, ROWS - 1)])
    ea = user_vec[...]
    both = jnp.concatenate([picks[q] for q in range(ROWS)], axis=0).astype(F32)
    margin = (jnp.sum(ea * both[:, 0:128], axis=0, keepdims=True)
              - jnp.sum(ea * both[:, 128:256], axis=0, keepdims=True))
    term = jnp.maximum(-margin, 0.0) + jnp.log1p(jnp.exp(-jnp.abs(margin)))
    mine = jnp.logical_and(ids_a >= 0, ids_a < SUBS * BLK)
    terms[r] = jnp.where(mine, term, 0.0)
    row_send(9, lambda rr: terms.at[r], terms.at[r])
    row_wait(9, terms.at[pl.ds(0, ROWS - 1)])
    terms2[c] = terms[0] + terms[1] + terms[2] + terms[3]
    col_send(2 * SUBS + 1, lambda cc: terms2.at[c], terms2.at[c])

    def drain(ref, sem):
        remote(ref, ref, sem, y_rs.at[0], mate).wait_send()

    drain(ysend, y_ss)
    drain(yrecv.at[:, pl.ds(0, DEPTH - 1)], z_ss)
    drain(panels.at[:, pl.ds(0, 1)], ag_sy)
    for at in range(DEPTH):
        @pl.when(z == at)
        def _():
            if at < DEPTH - 1:
                drain(panels.at[:, pl.ds(0, 2 * (at + 1))], ag_su)
            if at > 0:
                drain(panels.at[:, pl.ds(0, 2 * (DEPTH - at))], ag_sd)

    col_wait(2 * SUBS + 1, terms2.at[pl.ds(0, RING - 1)])
    tsum = terms2[0]
    for q in range(1, RING):
        tsum = tsum + terms2[q]
    loss[...] = jnp.broadcast_to(jnp.sum(tsum, axis=1, keepdims=True) / tsum.shape[1], loss.shape)


def deliver(outu, outi, loss, to_user, to_item, to_loss):
    for q in range(SUBS):
        to_user[:, q * BLK:(q + 1) * BLK] = outu[q]
    to_item[...] = outi[...]
    to_loss[...] = loss[0:1, 0:1]


def solution(mesh):
    def local_prog(mask_blk, user_shard, item_shard, triples):
        vmem = pl.BlockSpec(memory_space=pltpu.VMEM)
        dma = pltpu.SemaphoreType.DMA
        outu, outi, loss = pl.pallas_call(
            kernel,
            out_shape=(jax.ShapeDtypeStruct((SUBS, DIM, BLK), BF16),
                       jax.ShapeDtypeStruct((DIM, 128), BF16),
                       jax.ShapeDtypeStruct((8, 128), F32)),
            in_specs=[pl.BlockSpec(memory_space=pl.ANY), vmem, vmem, vmem],
            out_specs=(vmem, vmem, vmem),
            scratch_shapes=[
                pltpu.VMEM((RING * SUBS, BLK, BLK), BF16),
                pltpu.VMEM((MASK_BUFS, BLK, BLK), jnp.int32),
                dma((MASK_BUFS,)),
                pltpu.VMEM((LAYERS, RING, SUBS, DIM, BLK), BF16),
                pltpu.VMEM((LAYERS + 1, ROWS, DIM, 128), BF16),
                pltpu.VMEM((LAYERS, DIM, BLK), F32),
                pltpu.VMEM((LAYERS, ROWS, DIM, 128), F32),
                pltpu.VMEM((LAYERS, ROWS, DIM, 128), F32),
                pltpu.VMEM((LAYERS, DEPTH, SUBS, DIM, BLK), F32),
                pltpu.VMEM((LAYERS, DEPTH, SUBS, DIM, BLK), F32),
                pltpu.VMEM((LAYERS, DEPTH + 1, SUBS, DIM, BLK), F32),
                pltpu.VMEM((8, BLK), F32),
                pltpu.VMEM((RING * SUBS, 1, BLK), F32),
                pltpu.VMEM((RING, SUBS, 1, BLK), F32),
                pltpu.VMEM((RING * SUBS, 1, BLK), F32),
                pltpu.VMEM((1, BLK), F32),
                pltpu.VMEM((ROWS, 1, BLK), F32),
                pltpu.VMEM((1, BLK), F32),
                pltpu.VMEM((SUBS, BLK, 128), BF16),
                pltpu.VMEM((ROWS, 16, 256), BF16),
                pltpu.VMEM((RING, 16, 256), BF16),
                pltpu.VMEM((ROWS, 16, 256), BF16),
                pltpu.VMEM((DIM, 128), F32),
                pltpu.VMEM((ROWS, 1, 128), F32),
                pltpu.VMEM((RING, 1, 128), F32),
                dma, dma((Y_SEMS,)), dma, dma((DEPTH + 1, SUBS)),
                dma, dma, dma, dma((2, RING, SUBS)),
                dma((10,)), dma((10,)), dma((2 * SUBS + 2,)), dma((2 * SUBS + 2,)),
            ],
            compiler_params=pltpu.CompilerParams(
                collective_id=0, has_side_effects=True, vmem_limit_bytes=61 * 1024 * 1024),
            name="propagate",
        )(mask_blk, user_shard.T, item_shard.T, triples.T)
        out_user, out_item, mean = pl.pallas_call(
            deliver,
            out_shape=(jax.ShapeDtypeStruct((DIM, SUBS * BLK), BF16),
                       jax.ShapeDtypeStruct((DIM, 128), BF16),
                       jax.ShapeDtypeStruct((1, 1), F32)),
            in_specs=[vmem, vmem, vmem], out_specs=(vmem, vmem, vmem), name="deliver",
        )(outu, outi, loss)
        return out_user.T, out_item.T, mean[0, 0]

    return jax.shard_map(local_prog, mesh=mesh,
                         in_specs=(P("row", "col"), P(("row", "col"), None), P(("col", "row"), None), P(None, None)),
                         out_specs=(P(("row", "col"), None), P(("col", "row"), None), P()), check_vma=False)
```

```python
import jax
import jax.numpy as jnp
from jax import lax
from jax.experimental import pallas as pl
from jax.experimental.pallas import tpu as pltpu
from jax.sharding import PartitionSpec as P

LAYERS = 3
RING = 8
ROWS = 4
DEPTH = 4
ROUNDS = 16
AHEAD = 2
Y_SEMS = 8
SUBS = 4
DIM = 64
BLK = 512
MASK_BUFS = 8
MESH = pl.DeviceIdType.MESH
BF16 = jnp.bfloat16
F32 = jnp.float32


def dot_t(lhs, rhs):
    return lax.dot_general(lhs, rhs, (((1,), (1,)), ((), ())), preferred_element_type=F32)


def dot_n(lhs, rhs):
    return lax.dot_general(lhs, rhs, (((1,), (0,)), ((), ())), preferred_element_type=F32)


def kernel(mask_hbm, euT, eiT, trip_hbm, outu_hbm, outi_hbm, loss,
           adj, mbuf, msem, io_sem, trip, outu, outi,
           panels, ei_all, item_acc, item_send, item_recv,
           ysend, yrecv, zin,
           colsum, deg_part, deg_recv, scale_u, itemdeg, itemdeg_recv, scale_v,
           onehot_a, pk, pk_recv, picks, user_vec, terms, terms2,
           y_ss, y_rs, z_ss, z_rs, ag_sy, ag_su, ag_sd, ag_rs,
           row_ss, row_rs, col_ss, col_rs):
    c = lax.axis_index("col")
    r = lax.axis_index("row")
    z, y = lax.div(c, 2), lax.rem(c, 2)
    mate = 2 * z + 1 - y
    is_up, is_down = z < DEPTH - 1, z > 0
    is_mid = jnp.logical_and(is_up, is_down)
    row_peers = [lax.rem(r + d, ROWS) for d in range(1, ROWS)]
    col_peers = [lax.rem(c + d, RING) for d in range(1, RING)]

    def mask_at(i):
        return lax.rem(i, RING) * SUBS + lax.div(i, RING)

    def mask_copy(i):
        slot = lax.rem(i, MASK_BUFS)
        return pltpu.make_async_copy(mask_hbm.at[pl.ds(mask_at(i) * BLK, BLK), :], mbuf.at[slot], msem.at[slot])

    for i in range(MASK_BUFS):
        mask_copy(jnp.int32(i)).start()

    def table_in(q):
        return pltpu.make_async_copy(euT.at[:, pl.ds(q * BLK, BLK)], panels.at[0, c, q], io_sem.at[q])

    item_in = pltpu.make_async_copy(eiT, ei_all.at[0, r], io_sem.at[SUBS])
    trip_in = pltpu.make_async_copy(trip_hbm, trip, io_sem.at[SUBS + 1])
    for q in range(SUBS):
        table_in(q).start()
    item_in.start()
    trip_in.start()

    barrier = pltpu.get_barrier_semaphore()
    for rr in row_peers:
        pl.semaphore_signal(barrier, inc=1, device_id=(c, rr), device_id_type=MESH)
    for cc in col_peers:
        pl.semaphore_signal(barrier, inc=1, device_id=(cc, r), device_id_type=MESH)

    def remote(src, dst, ss, rs, col):
        return pltpu.make_async_remote_copy(src_ref=src, dst_ref=dst, send_sem=ss, recv_sem=rs,
                                            device_id=(col, r), device_id_type=MESH)

    def ag_rs_of(k, col, q):
        return ag_rs.at[lax.div(k + 1, 2), col, q]

    def ag_y(k, q, col):
        ref = panels.at[k, col, q]
        return remote(ref, ref, ag_sy, ag_rs_of(k, col, q), mate)

    def ag_up(k, col, q):
        ref = panels.at[k, col, q]
        return remote(ref, ref, ag_su, ag_rs_of(k, col, q), c + 2)

    def ag_down(k, col, q):
        ref = panels.at[k, col, q]
        return remote(ref, ref, ag_sd, ag_rs_of(k, col, q), c - 2)

    def ag_both(k, col, q):
        @pl.when(is_up)
        def _():
            ag_up(k, col, q).start()

        @pl.when(is_down)
        def _():
            ag_down(k, col, q).start()

    def ag_own(k, q):
        ag_y(k, q, c).start()
        ag_both(k, c, q)

    def ag_mate(k, q):
        with jax.named_scope("ag_mate"):
            ag_y(k, q, mate).wait_recv()
        ag_both(k, mate, q)

    def line_event(k, s, yy, q, above, then):
        col = 2 * s + yy
        if above:
            with jax.named_scope("ag_above"):
                ag_down(k, col, q).wait_recv()

            @pl.when(is_down)
            def _():
                ag_down(k, col, q).start()
        else:
            with jax.named_scope("ag_below"):
                ag_up(k, col, q).wait_recv()

            @pl.when(is_up)
            def _():
                ag_up(k, col, q).start()
        then(col, q)

    def first_event(e, event):
        d, rest = lax.div(e, 2 * SUBS) + 1, lax.rem(e, 2 * SUBS)
        yy = y + lax.div(rest, SUBS) * (1 - 2 * y)
        q = lax.rem(rest, SUBS)

        @pl.when(z + d < DEPTH)
        def _():
            event(z + d, yy, q, True)

        @pl.when(z - d >= 0)
        def _():
            event(z - d, yy, q, False)

    def row_send(u, src, dst):
        for rr in row_peers:
            pltpu.make_async_remote_copy(src_ref=src(rr), dst_ref=dst, send_sem=row_ss.at[u], recv_sem=row_rs.at[u],
                                         device_id=(c, rr), device_id_type=MESH).start()

    def row_wait(u, ref):
        with jax.named_scope("row_wait_%d" % u):
            cp = pltpu.make_async_remote_copy(src_ref=ref, dst_ref=ref, send_sem=row_ss.at[u], recv_sem=row_rs.at[u],
                                              device_id=(c, row_peers[0]), device_id_type=MESH)
            cp.wait_recv()
            cp.wait_send()

    def col_send(u, src, dst):
        for cc in col_peers:
            remote(src(cc), dst, col_ss.at[u], col_rs.at[u], cc).start()

    def col_wait(u, ref):
        with jax.named_scope("col_wait_%d" % u):
            cp = remote(ref, ref, col_ss.at[u], col_rs.at[u], mate)
            cp.wait_recv()
            cp.wait_send()

    ones = jnp.ones((16, BLK), BF16)
    colsum[...] = jnp.zeros_like(colsum)

    def mask_block(i, carry):
        slot, b = lax.rem(i, MASK_BUFS), mask_at(i)
        mask_copy(i).wait()
        acc = jnp.zeros((8, BLK), F32)
        for t in range(4):
            m = mbuf[slot, t * 128:(t + 1) * 128, :].astype(F32)
            acc = acc + jnp.sum(m.reshape(16, 8, BLK), axis=0)
            adj[b, t * 128:(t + 1) * 128, :] = m.astype(BF16)
        colsum[...] += acc
        deg_part[b] = dot_t(ones, adj[b])[0:1, :]

        @pl.when(i + MASK_BUFS < SUBS * RING)
        def _():
            mask_copy(i + MASK_BUFS).start()
        return carry

    def deg_send(q):
        col_send(q, lambda cc: deg_part.at[cc * SUBS + q], deg_recv.at[c, q])
        deg_recv[c, q] = deg_part[c * SUBS + q]

    def deg_sum(q):
        col_wait(q, deg_part.at[pl.ds(0, RING - 1)])
        du = deg_recv[0, q]
        for cc in range(1, RING):
            du = du + deg_recv[cc, q]
        scale_u[c * SUBS + q] = lax.rsqrt(jnp.maximum(du, 1.0))
        col_send(SUBS + q, lambda cc: scale_u.at[c * SUBS + q], scale_u.at[c * SUBS + q])

    def deg_end(q):
        col_wait(SUBS + q, deg_part.at[pl.ds(0, RING - 1)])

    def mask_quarter(q):
        with jax.named_scope("mask"):
            lax.fori_loop(RING * q, RING * (q + 1), mask_block, 0)

    def early_event(e):
        first_event(jnp.int32(e), lambda s, yy, q, above: line_event(0, s, yy, q, above, lambda col, q: None))

    mask_quarter(0)
    for q in range(SUBS):
        table_in(q).wait()
    item_in.wait()
    trip_in.wait()
    with jax.named_scope("entry"):
        pl.semaphore_wait(barrier, (ROWS - 1) + (RING - 1))
    deg_send(0)
    ag_own(0, 0)
    ag_own(0, 1)
    row_send(0, lambda rr: ei_all.at[0, r], ei_all.at[0, r])
    mask_quarter(1)
    deg_send(1)
    ag_own(0, 2)
    mask_quarter(2)
    deg_send(2)
    ag_own(0, 3)
    deg_sum(0)
    for q in range(2):
        ag_mate(0, q)
        early_event(q)
    mask_quarter(3)
    itemdeg[...] = jnp.sum(colsum[...], axis=0, keepdims=True)
    row_send(1, lambda rr: itemdeg, itemdeg_recv.at[r])
    deg_send(3)
    itemdeg_recv[r] = itemdeg[...]
    deg_sum(1)
    row_wait(1, itemdeg_recv.at[pl.ds(0, ROWS - 1)])
    dv = itemdeg_recv[0] + itemdeg_recv[1] + itemdeg_recv[2] + itemdeg_recv[3]
    scale_v[...] = lax.rsqrt(jnp.maximum(dv, 1.0))
    row_wait(0, ei_all.at[0, pl.ds(0, ROWS - 1)])
    deg_end(0)

    def build(b):
        sv = scale_v[...]
        for t in range(4):
            su = scale_u[b, :, t * 128:(t + 1) * 128]
            suc = jnp.transpose(jnp.broadcast_to(su, (128, 128)))
            val = (jnp.concatenate([suc] * 4, axis=1) * sv).astype(BF16)
            adj[b, t * 128:(t + 1) * 128, :] = adj[b, t * 128:(t + 1) * 128, :] * val

    def user_part(k, b):
        ei = jnp.concatenate([ei_all[k, q] for q in range(ROWS)], axis=1)
        return dot_t(ei, adj[b])

    def item_part(k, col, q):
        item_acc[k] += dot_n(panels[k, col, q], adj[col * SUBS + q])

    def item_start(k):
        for q in range(ROWS):
            item_send[k, q] = item_acc[k, :, q * 128:(q + 1) * 128]
        row_send(2 + 2 * k, lambda rr: item_send.at[k, rr], item_recv.at[k, r])
        item_recv[k, r] = item_send[k, r]

    def item_sum(k):
        row_wait(2 + 2 * k, item_send.at[k, pl.ds(0, ROWS - 1)])
        tot = item_recv[k, 0] + item_recv[k, 1] + item_recv[k, 2] + item_recv[k, 3]
        return tot.astype(BF16)

    def item_share(k, val):
        ei_all[k + 1, r] = val
        row_send(3 + 2 * k, lambda rr: ei_all.at[k + 1, r], ei_all.at[k + 1, r])

    def item_end(k):
        row_wait(3 + 2 * k, ei_all.at[k + 1, pl.ds(0, ROWS - 1)])

    def place(n):
        k, i = lax.div(n, ROUNDS), lax.rem(n, ROUNDS)
        last, own = lax.div(k, LAYERS - 1), lax.div(i, 12)
        q, g = lax.div(i, 4), lax.rem(i, 4)
        q_last = (1 - own) * lax.div(i, 3) + own * (i - 12)
        g_last = (1 - own) * lax.rem(i, 3) + own * 3
        q, g = q + last * (q_last - q), g + last * (g_last - g)
        pw = 1 + 3 * g + 9 * lax.div(g * (g - 1), 2) + 27 * lax.div(g * (g - 1) * (g - 2), 6)
        return k, lax.rem(lax.div(27 + 48 * z + 57 * lax.div(z, 2), pw), DEPTH), q

    def y_copy(n):
        k, t, q = place(n)
        return remote(ysend.at[k, t, q], yrecv.at[k, t, q], y_ss, y_rs.at[lax.rem(n, Y_SEMS)], mate)

    def y_begin(n):
        k, t, q = place(n)
        ysend[k, t, q] = user_part(k, (2 * t + 1 - y) * SUBS + q)
        y_copy(n).start()

    def z_up(k, t, q):
        return remote(yrecv.at[k, t, q], zin.at[k, t, q], z_ss, z_rs.at[t, q], c + 2)

    def z_down(k, t, q):
        to = t + lax.div(2 - (z - 1 - t), 2) * (DEPTH - t)
        return remote(yrecv.at[k, t, q], zin.at[k, to, q], z_ss, z_rs.at[to, q], c - 2)

    def z_add(k, t, at, q):
        with jax.named_scope("rs_z"):
            remote(yrecv.at[k, t, q], zin.at[k, at, q], z_ss, z_rs.at[at, q], mate).wait_recv()
        yrecv[k, t, q] = yrecv[k, t, q] + zin[k, at, q]

    def z_send(k, t, q):
        @pl.when(t > z)
        def _():
            z_up(k, t, q).start()

        @pl.when(t < z)
        def _():
            z_down(k, t, q).start()

    def y_stage(n):
        k, t, q = place(n)
        part = user_part(k, (2 * t + y) * SUBS + q)
        with jax.named_scope("rs_y"):
            y_copy(n).wait_recv()
        yrecv[k, t, q] = yrecv[k, t, q] + part

        @pl.when(jnp.logical_and(jnp.logical_not(is_mid), t != z))
        def _():
            z_send(k, t, q)

    def mid_stage(n):
        k, t, q = place(n)

        @pl.when(t != z)
        def _():
            z_add(k, t, t, q)
            z_send(k, t, q)

    def table_out(q):
        return pltpu.make_async_copy(outu.at[q], outu_hbm.at[q], io_sem.at[q])

    item_out = pltpu.make_async_copy(outi, outi_hbm, io_sem.at[SUBS])

    def own_stage(n):
        k, _, q = place(n)

        @pl.when(is_down)
        def _():
            z_add(k, z, z, q)

        @pl.when(is_up)
        def _():
            z_add(k, z, DEPTH, q)
        val = yrecv[k, z, q].astype(BF16)

        @pl.when(k < LAYERS - 1)
        def _():
            panels[k + 1, c, q] = val
            ag_own(k + 1, q)
            item_part(k + 1, c, q)

        @pl.when(k == LAYERS - 1)
        def _():
            tot = (panels[0, c, q].astype(F32) + panels[1, c, q].astype(F32) + panels[2, c, q].astype(F32)
                   + val.astype(F32))
            out = (tot / (LAYERS + 1)).astype(BF16)
            outu[q] = out
            table_out(q).start()
            user_vec[...] += dot_n(out, onehot_a[q])

    def build_round(i):
        _, t, q = place(i)
        build((2 * t + 1 - y) * SUBS + q)
        build((2 * t + y) * SUBS + q)

    base = (r * RING + c) * (SUBS * BLK)
    ids_a = trip[0:1, :] - base
    item_acc[...] = jnp.zeros_like(item_acc)
    user_vec[...] = jnp.zeros_like(user_vec)

    def is_middle(s):
        return lax.div(s * (DEPTH - 1 - s), 2)

    own_lag = 7 - 2 * is_middle(z)
    sets = SUBS * (LAYERS - 1)

    def gather_set(late, event):
        @pl.when(jnp.logical_and(lax.rem(late + 64, 8) == 0, jnp.logical_and(late >= 0, late < 8 * sets)))
        def _():
            m = lax.div(late, 8)
            event(lax.div(m, SUBS) + 1, lax.rem(m, SUBS))

    def gather_mate(half):
        def event(k, q):
            ag_mate(k, q)
            item_part(k, mate, q)
        gather_set(half - (2 * own_lag + 6), event)

    def gather_line(half, d, f):
        for above in (True, False):
            s = z + d if above else z - d

            @pl.when(jnp.logical_and(s < DEPTH, s >= 0))
            def _():
                gather_set(half - (2 * (7 - 2 * is_middle(s)) + 3 * d + (6 if f else 1)),
                           lambda k, q: line_event(k, s, 1 - y if f else y, q, above,
                                                   lambda col, q: item_part(k, col, q)))

    for i in range(AHEAD):
        build_round(jnp.int32(i))
        y_begin(jnp.int32(i))
    for i in range(AHEAD, 4):
        build_round(jnp.int32(i))
    deg_sum(2)
    for q in range(2, SUBS):
        ag_mate(0, q)
        early_event(q)

    def when_at(n, i):
        return pl.when(n == i)

    def one_round(n, carry):
        @when_at(n, 1)
        def _():
            deg_end(1)
            deg_sum(3)

        @when_at(n, 3)
        def _():
            deg_end(2)

        @when_at(n, 5)
        def _():
            deg_end(3)

        @when_at(n, 13)
        def _():
            item_end(0)

        @pl.when(n + AHEAD < LAYERS * ROUNDS)
        def _():
            y_begin(n + AHEAD)

        gather_mate(2 * n)
        for d, f in ((1, 0), (2, 1), (3, 0)):
            gather_line(2 * n, d, f)
        y_stage(n)

        @pl.when(jnp.logical_and(is_mid, n >= 2))
        def _():
            mid_stage(n - 2)
        own = n - own_lag + 3

        @pl.when(jnp.logical_and(lax.rem(own + 4, 4) == 3, jnp.logical_and(own >= 0, own < 2 * ROUNDS)))
        def _():
            own_stage(own)
        for d, f in ((1, 1), (2, 0), (3, 1)):
            gather_line(2 * n + 1, d, f)

        @when_at(n, 46)
        def _():
            col_wait(2 * SUBS, pk_recv.at[pl.ds(0, RING - 1)])
            psum = pk_recv[0].astype(F32)
            for q in range(1, RING):
                psum = psum + pk_recv[q].astype(F32)
            picks[r] = psum.astype(BF16)
            row_send(8, lambda rr: picks.at[r], picks.at[r])

        @pl.when(n >= LAYERS * ROUNDS - SUBS)
        def _():
            own_stage(n)

        @pl.when(jnp.logical_and(n >= 1, n < 7))
        def _():
            build_round(2 * n + 2)
            build_round(2 * n + 3)

        @pl.when(n < 6)
        def _():
            early_event(2 * n + 4)
            early_event(2 * n + 5)

        def late_event(e):
            first_event(e, lambda s, yy, q, above: line_event(
                0, s, yy, q, above, lambda col, q: item_part(0, col, q)))

        def old_event(e):
            first_event(e, lambda s, yy, q, above: item_part(0, 2 * s + yy, q))

        @pl.when(jnp.logical_and(n >= 6, n < 11))
        def _():
            e = 16 + (n - 6) + lax.div(n - 6, 3) + lax.div(n - 6, 4)
            late_event(e)

            @pl.when(n >= 8)
            def _():
                late_event(e + 1)

        @pl.when(jnp.logical_and(n >= 1, n < 9))
        def _():
            q, side = lax.div(n - 1, 2), lax.rem(n - 1, 2)
            item_part(0, c + side * (mate - c), q)
            old_event(q + 4 * side)

        @pl.when(jnp.logical_and(n >= 4, n < 11))
        def _():
            old_event(n + 4 + lax.div(n, 9))

            @pl.when(n == 8)
            def _():
                old_event(n + 5)

        @when_at(n, 10)
        def _():
            item_start(0)

        @when_at(n, 11)
        def _():
            item_share(0, item_sum(0))

        @when_at(n, 26)
        def _():
            item_start(1)

        @when_at(n, 27)
        def _():
            item_share(1, item_sum(1))

        @when_at(n, 29)
        def _():
            item_end(1)

        @pl.when(jnp.logical_and(n >= 32, n < 32 + SUBS))
        def _():
            iota_u = lax.broadcasted_iota(jnp.int32, (BLK, 128), 0) + (n - 32) * BLK
            onehot_a[n - 32] = (iota_u == ids_a).astype(BF16)

        @when_at(n, 43)
        def _():
            last_item = item_sum(2)
            tot = (ei_all[0, r].astype(F32) + ei_all[1, r].astype(F32) + ei_all[2, r].astype(F32)
                   + last_item.astype(F32))
            out_item = (tot / (LAYERS + 1)).astype(BF16)
            outi[...] = out_item
            item_out.start()
            item_share(2, out_item)

        @when_at(n, 44)
        def _():
            item_end(2)
            iota_i = lax.broadcasted_iota(jnp.int32, (BLK, 128), 0) + c * BLK
            hot = jnp.concatenate([(iota_i == trip[1:2, :]).astype(BF16), (iota_i == trip[2:3, :]).astype(BF16)],
                                  axis=1)
            got = dot_n(jnp.concatenate([ei_all[3, q] for q in range(ROWS)], axis=1), hot).astype(BF16)
            for q in range(ROWS):
                pk[q] = got[q * 16:(q + 1) * 16, :]
            col_send(2 * SUBS, lambda cc: pk.at[r], pk_recv.at[c])
            pk_recv[c] = pk[r]

        @when_at(n, 42)
        def _():
            item_start(2)
        return carry
    lax.fori_loop(0, LAYERS * ROUNDS, one_round, 0)

    row_wait(8, picks.at[pl.ds(0, ROWS - 1)])
    ea = user_vec[...]
    both = jnp.concatenate([picks[q] for q in range(ROWS)], axis=0).astype(F32)
    margin = (jnp.sum(ea * both[:, 0:128], axis=0, keepdims=True)
              - jnp.sum(ea * both[:, 128:256], axis=0, keepdims=True))
    term = jnp.maximum(-margin, 0.0) + jnp.log1p(jnp.exp(-jnp.abs(margin)))
    mine = jnp.logical_and(ids_a >= 0, ids_a < SUBS * BLK)
    terms[r] = jnp.where(mine, term, 0.0)
    row_send(9, lambda rr: terms.at[r], terms.at[r])
    row_wait(9, terms.at[pl.ds(0, ROWS - 1)])
    terms2[c] = terms[0] + terms[1] + terms[2] + terms[3]
    col_send(2 * SUBS + 1, lambda cc: terms2.at[c], terms2.at[c])

    def drain(ref, sem):
        remote(ref, ref, sem, y_rs.at[0], mate).wait_send()

    drain(ysend, y_ss)
    for q in range(SUBS):
        table_out(q).wait()
    item_out.wait()
    drain(yrecv.at[:, pl.ds(0, DEPTH - 1)], z_ss)
    drain(panels.at[:, pl.ds(0, 1)], ag_sy)
    for at in range(DEPTH):
        @pl.when(z == at)
        def _():
            if at < DEPTH - 1:
                drain(panels.at[:, pl.ds(0, 2 * (at + 1))], ag_su)
            if at > 0:
                drain(panels.at[:, pl.ds(0, 2 * (DEPTH - at))], ag_sd)

    col_wait(2 * SUBS + 1, terms2.at[pl.ds(0, RING - 1)])
    tsum = terms2[0]
    for q in range(1, RING):
        tsum = tsum + terms2[q]
    loss[...] = jnp.broadcast_to(jnp.sum(tsum, axis=1, keepdims=True) / tsum.shape[1], loss.shape)


def deliver(outu, outi, loss, to_user, to_item, to_loss):
    for q in range(SUBS):
        to_user[:, q * BLK:(q + 1) * BLK] = outu[q]
    to_item[...] = outi[...]
    to_loss[...] = loss[0:1, 0:1]


def solution(mesh):
    def local_prog(mask_blk, user_shard, item_shard, triples):
        vmem = pl.BlockSpec(memory_space=pltpu.VMEM)
        hbm = pl.BlockSpec(memory_space=pl.ANY)
        dma = pltpu.SemaphoreType.DMA
        outu, outi, loss = pl.pallas_call(
            kernel,
            out_shape=(jax.ShapeDtypeStruct((SUBS, DIM, BLK), BF16),
                       jax.ShapeDtypeStruct((DIM, 128), BF16),
                       jax.ShapeDtypeStruct((8, 128), F32)),
            in_specs=[hbm] * 4,
            out_specs=(hbm, hbm, vmem),
            scratch_shapes=[
                pltpu.VMEM((RING * SUBS, BLK, BLK), BF16),
                pltpu.VMEM((MASK_BUFS, BLK, BLK), jnp.int32),
                dma((MASK_BUFS,)),
                dma((SUBS + 2,)),
                pltpu.VMEM((3, 128), jnp.int32),
                pltpu.VMEM((SUBS, DIM, BLK), BF16),
                pltpu.VMEM((DIM, 128), BF16),
                pltpu.VMEM((LAYERS, RING, SUBS, DIM, BLK), BF16),
                pltpu.VMEM((LAYERS + 1, ROWS, DIM, 128), BF16),
                pltpu.VMEM((LAYERS, DIM, BLK), F32),
                pltpu.VMEM((LAYERS, ROWS, DIM, 128), F32),
                pltpu.VMEM((LAYERS, ROWS, DIM, 128), F32),
                pltpu.VMEM((LAYERS, DEPTH, SUBS, DIM, BLK), F32),
                pltpu.VMEM((LAYERS, DEPTH, SUBS, DIM, BLK), F32),
                pltpu.VMEM((LAYERS, DEPTH + 1, SUBS, DIM, BLK), F32),
                pltpu.VMEM((8, BLK), F32),
                pltpu.VMEM((RING * SUBS, 1, BLK), F32),
                pltpu.VMEM((RING, SUBS, 1, BLK), F32),
                pltpu.VMEM((RING * SUBS, 1, BLK), F32),
                pltpu.VMEM((1, BLK), F32),
                pltpu.VMEM((ROWS, 1, BLK), F32),
                pltpu.VMEM((1, BLK), F32),
                pltpu.VMEM((SUBS, BLK, 128), BF16),
                pltpu.VMEM((ROWS, 16, 256), BF16),
                pltpu.VMEM((RING, 16, 256), BF16),
                pltpu.VMEM((ROWS, 16, 256), BF16),
                pltpu.VMEM((DIM, 128), F32),
                pltpu.VMEM((ROWS, 1, 128), F32),
                pltpu.VMEM((RING, 1, 128), F32),
                dma, dma((Y_SEMS,)), dma, dma((DEPTH + 1, SUBS)),
                dma, dma, dma, dma((2, RING, SUBS)),
                dma((10,)), dma((10,)), dma((2 * SUBS + 2,)), dma((2 * SUBS + 2,)),
            ],
            compiler_params=pltpu.CompilerParams(
                collective_id=0, has_side_effects=True, vmem_limit_bytes=61 * 1024 * 1024),
            name="propagate",
        )(mask_blk, user_shard.T, item_shard.T, triples.T)
        out_user, out_item, mean = pl.pallas_call(
            deliver,
            out_shape=(jax.ShapeDtypeStruct((DIM, SUBS * BLK), BF16),
                       jax.ShapeDtypeStruct((DIM, 128), BF16),
                       jax.ShapeDtypeStruct((1, 1), F32)),
            in_specs=[vmem, vmem, vmem], out_specs=(vmem, vmem, vmem), name="deliver",
        )(outu, outi, loss)
        return out_user.T, out_item.T, mean[0, 0]

    return jax.shard_map(local_prog, mesh=mesh,
                         in_specs=(P("row", "col"), P(("row", "col"), None), P(("col", "row"), None), P(None, None)),
                         out_specs=(P(("row", "col"), None), P(("col", "row"), None), P()), check_vma=False)
```

```python
import jax
import jax.numpy as jnp
from jax import lax
from jax.experimental import pallas as pl
from jax.experimental.pallas import tpu as pltpu
from jax.sharding import PartitionSpec as P

LAYERS = 3
RING = 8
ROWS = 4
DEPTH = 4
ROUNDS = 16
AHEAD = 2
Y_SEMS = 8
SUBS = 4
DIM = 64
BLK = 512
MASK_BUFS = 8
MESH = pl.DeviceIdType.MESH
BF16 = jnp.bfloat16
F32 = jnp.float32


def dot_t(lhs, rhs):
    return lax.dot_general(lhs, rhs, (((1,), (1,)), ((), ())), preferred_element_type=F32)


def dot_n(lhs, rhs):
    return lax.dot_general(lhs, rhs, (((1,), (0,)), ((), ())), preferred_element_type=F32)


def kernel(mask_hbm, euT, eiT, trip_hbm, outu_hbm, outi_hbm, loss,
           adj, mbuf, msem, io_sem, trip, outu, outi,
           panels, ei_all, item_acc, item_send, item_recv,
           ysend, yrecv, zin,
           colsum, deg_part, deg_recv, scale_u, itemdeg, itemdeg_recv, scale_v,
           onehot_a, pk, pk_recv, picks, user_vec, terms, term_sem,
           y_ss, y_rs, z_ss, z_rs, ag_sy, ag_su, ag_sd, ag_rs,
           row_ss, row_rs, col_ss, col_rs):
    c = lax.axis_index("col")
    r = lax.axis_index("row")
    z, y = lax.div(c, 2), lax.rem(c, 2)
    mate = 2 * z + 1 - y
    is_up, is_down = z < DEPTH - 1, z > 0
    is_mid = jnp.logical_and(is_up, is_down)
    row_peers = [lax.rem(r + d, ROWS) for d in range(1, ROWS)]
    col_peers = [lax.rem(c + d, RING) for d in range(1, RING)]

    def mask_at(i):
        return lax.rem(i, RING) * SUBS + lax.div(i, RING)

    def mask_copy(i):
        slot = lax.rem(i, MASK_BUFS)
        return pltpu.make_async_copy(mask_hbm.at[pl.ds(mask_at(i) * BLK, BLK), :], mbuf.at[slot], msem.at[slot])

    for i in range(MASK_BUFS):
        mask_copy(jnp.int32(i)).start()

    def table_in(q):
        return pltpu.make_async_copy(euT.at[:, pl.ds(q * BLK, BLK)], panels.at[0, c, q], io_sem.at[q])

    item_in = pltpu.make_async_copy(eiT, ei_all.at[0, r], io_sem.at[SUBS])
    trip_in = pltpu.make_async_copy(trip_hbm, trip, io_sem.at[SUBS + 1])
    for q in range(SUBS):
        table_in(q).start()
    item_in.start()
    trip_in.start()

    barrier = pltpu.get_barrier_semaphore()
    all_peers = [(lax.rem(c + dc, RING), lax.rem(r + dr, ROWS))
                 for dc in range(RING) for dr in range(ROWS) if dc or dr]
    for peer in all_peers:
        pl.semaphore_signal(barrier, inc=1, device_id=peer, device_id_type=MESH)

    def remote(src, dst, ss, rs, col):
        return pltpu.make_async_remote_copy(src_ref=src, dst_ref=dst, send_sem=ss, recv_sem=rs,
                                            device_id=(col, r), device_id_type=MESH)

    def ag_rs_of(k, col, q):
        return ag_rs.at[lax.div(k + 1, 2), col, q]

    def ag_y(k, q, col):
        ref = panels.at[k, col, q]
        return remote(ref, ref, ag_sy, ag_rs_of(k, col, q), mate)

    def ag_up(k, col, q):
        ref = panels.at[k, col, q]
        return remote(ref, ref, ag_su, ag_rs_of(k, col, q), c + 2)

    def ag_down(k, col, q):
        ref = panels.at[k, col, q]
        return remote(ref, ref, ag_sd, ag_rs_of(k, col, q), c - 2)

    def ag_both(k, col, q):
        @pl.when(is_up)
        def _():
            ag_up(k, col, q).start()

        @pl.when(is_down)
        def _():
            ag_down(k, col, q).start()

    def ag_own(k, q):
        ag_y(k, q, c).start()
        ag_both(k, c, q)

    def ag_mate(k, q):
        with jax.named_scope("ag_mate"):
            ag_y(k, q, mate).wait_recv()
        ag_both(k, mate, q)

    def line_event(k, s, yy, q, above, then):
        col = 2 * s + yy
        if above:
            with jax.named_scope("ag_above"):
                ag_down(k, col, q).wait_recv()

            @pl.when(is_down)
            def _():
                ag_down(k, col, q).start()
        else:
            with jax.named_scope("ag_below"):
                ag_up(k, col, q).wait_recv()

            @pl.when(is_up)
            def _():
                ag_up(k, col, q).start()
        then(col, q)

    def first_event(e, event):
        d, rest = lax.div(e, 2 * SUBS) + 1, lax.rem(e, 2 * SUBS)
        yy = y + lax.div(rest, SUBS) * (1 - 2 * y)
        q = lax.rem(rest, SUBS)

        @pl.when(z + d < DEPTH)
        def _():
            event(z + d, yy, q, True)

        @pl.when(z - d >= 0)
        def _():
            event(z - d, yy, q, False)

    def row_send(u, src, dst):
        for rr in row_peers:
            pltpu.make_async_remote_copy(src_ref=src(rr), dst_ref=dst, send_sem=row_ss.at[u], recv_sem=row_rs.at[u],
                                         device_id=(c, rr), device_id_type=MESH).start()

    def row_wait(u, ref):
        with jax.named_scope("row_wait_%d" % u):
            cp = pltpu.make_async_remote_copy(src_ref=ref, dst_ref=ref, send_sem=row_ss.at[u], recv_sem=row_rs.at[u],
                                              device_id=(c, row_peers[0]), device_id_type=MESH)
            cp.wait_recv()
            cp.wait_send()

    def col_send(u, src, dst):
        for cc in col_peers:
            remote(src(cc), dst, col_ss.at[u], col_rs.at[u], cc).start()

    def col_wait(u, ref):
        with jax.named_scope("col_wait_%d" % u):
            cp = remote(ref, ref, col_ss.at[u], col_rs.at[u], mate)
            cp.wait_recv()
            cp.wait_send()

    ones = jnp.ones((16, BLK), BF16)
    colsum[...] = jnp.zeros_like(colsum)

    def mask_block(i, carry):
        slot, b = lax.rem(i, MASK_BUFS), mask_at(i)
        mask_copy(i).wait()
        acc = jnp.zeros((8, BLK), F32)
        for t in range(4):
            m = mbuf[slot, t * 128:(t + 1) * 128, :].astype(F32)
            acc = acc + jnp.sum(m.reshape(16, 8, BLK), axis=0)
            adj[b, t * 128:(t + 1) * 128, :] = m.astype(BF16)
        colsum[...] += acc
        deg_part[b] = dot_t(ones, adj[b])[0:1, :]

        @pl.when(i + MASK_BUFS < SUBS * RING)
        def _():
            mask_copy(i + MASK_BUFS).start()
        return carry

    def deg_send(q):
        col_send(q, lambda cc: deg_part.at[cc * SUBS + q], deg_recv.at[c, q])
        deg_recv[c, q] = deg_part[c * SUBS + q]

    def deg_sum(q):
        col_wait(q, deg_part.at[pl.ds(0, RING - 1)])
        du = deg_recv[0, q]
        for cc in range(1, RING):
            du = du + deg_recv[cc, q]
        scale_u[c * SUBS + q] = lax.rsqrt(jnp.maximum(du, 1.0))
        col_send(SUBS + q, lambda cc: scale_u.at[c * SUBS + q], scale_u.at[c * SUBS + q])

    def deg_end(q):
        col_wait(SUBS + q, deg_part.at[pl.ds(0, RING - 1)])

    def mask_quarter(q):
        with jax.named_scope("mask"):
            lax.fori_loop(RING * q, RING * (q + 1), mask_block, 0)

    def early_event(e):
        first_event(jnp.int32(e), lambda s, yy, q, above: line_event(0, s, yy, q, above, lambda col, q: None))

    mask_quarter(0)
    for q in range(SUBS):
        table_in(q).wait()
    item_in.wait()
    trip_in.wait()
    with jax.named_scope("entry"):
        pl.semaphore_wait(barrier, len(all_peers))
    deg_send(0)
    ag_own(0, 0)
    ag_own(0, 1)
    row_send(0, lambda rr: ei_all.at[0, r], ei_all.at[0, r])
    mask_quarter(1)
    deg_send(1)
    ag_own(0, 2)
    mask_quarter(2)
    deg_send(2)
    ag_own(0, 3)
    deg_sum(0)
    for q in range(2):
        ag_mate(0, q)
        early_event(q)
    mask_quarter(3)
    itemdeg[...] = jnp.sum(colsum[...], axis=0, keepdims=True)
    row_send(1, lambda rr: itemdeg, itemdeg_recv.at[r])
    deg_send(3)
    itemdeg_recv[r] = itemdeg[...]
    deg_sum(1)
    row_wait(1, itemdeg_recv.at[pl.ds(0, ROWS - 1)])
    dv = itemdeg_recv[0] + itemdeg_recv[1] + itemdeg_recv[2] + itemdeg_recv[3]
    scale_v[...] = lax.rsqrt(jnp.maximum(dv, 1.0))
    row_wait(0, ei_all.at[0, pl.ds(0, ROWS - 1)])
    deg_end(0)

    def build(b):
        sv = scale_v[...]
        for t in range(4):
            su = scale_u[b, :, t * 128:(t + 1) * 128]
            suc = jnp.transpose(jnp.broadcast_to(su, (128, 128)))
            val = (jnp.concatenate([suc] * 4, axis=1) * sv).astype(BF16)
            adj[b, t * 128:(t + 1) * 128, :] = adj[b, t * 128:(t + 1) * 128, :] * val

    def user_part(k, b):
        ei = jnp.concatenate([ei_all[k, q] for q in range(ROWS)], axis=1)
        return dot_t(ei, adj[b])

    def item_part(k, col, q):
        item_acc[k] += dot_n(panels[k, col, q], adj[col * SUBS + q])

    def item_start(k):
        for q in range(ROWS):
            item_send[k, q] = item_acc[k, :, q * 128:(q + 1) * 128]
        row_send(2 + 2 * k, lambda rr: item_send.at[k, rr], item_recv.at[k, r])
        item_recv[k, r] = item_send[k, r]

    def item_sum(k):
        row_wait(2 + 2 * k, item_send.at[k, pl.ds(0, ROWS - 1)])
        tot = item_recv[k, 0] + item_recv[k, 1] + item_recv[k, 2] + item_recv[k, 3]
        return tot.astype(BF16)

    def item_share(k, val):
        ei_all[k + 1, r] = val
        row_send(3 + 2 * k, lambda rr: ei_all.at[k + 1, r], ei_all.at[k + 1, r])

    def item_end(k):
        row_wait(3 + 2 * k, ei_all.at[k + 1, pl.ds(0, ROWS - 1)])

    def place(n):
        k, i = lax.div(n, ROUNDS), lax.rem(n, ROUNDS)
        last, own = lax.div(k, LAYERS - 1), lax.div(i, 12)
        q, g = lax.div(i, 4), lax.rem(i, 4)
        q_last = (1 - own) * lax.div(i, 3) + own * (i - 12)
        g_last = (1 - own) * lax.rem(i, 3) + own * 3
        q, g = q + last * (q_last - q), g + last * (g_last - g)
        pw = 1 + 3 * g + 9 * lax.div(g * (g - 1), 2) + 27 * lax.div(g * (g - 1) * (g - 2), 6)
        return k, lax.rem(lax.div(27 + 48 * z + 57 * lax.div(z, 2), pw), DEPTH), q

    def y_copy(n):
        k, t, q = place(n)
        return remote(ysend.at[k, t, q], yrecv.at[k, t, q], y_ss, y_rs.at[lax.rem(n, Y_SEMS)], mate)

    def y_begin(n):
        k, t, q = place(n)
        ysend[k, t, q] = user_part(k, (2 * t + 1 - y) * SUBS + q)
        y_copy(n).start()

    def z_up(k, t, q):
        return remote(yrecv.at[k, t, q], zin.at[k, t, q], z_ss, z_rs.at[t, q], c + 2)

    def z_down(k, t, q):
        to = t + lax.div(2 - (z - 1 - t), 2) * (DEPTH - t)
        return remote(yrecv.at[k, t, q], zin.at[k, to, q], z_ss, z_rs.at[to, q], c - 2)

    def z_add(k, t, at, q):
        with jax.named_scope("rs_z"):
            remote(yrecv.at[k, t, q], zin.at[k, at, q], z_ss, z_rs.at[at, q], mate).wait_recv()
        yrecv[k, t, q] = yrecv[k, t, q] + zin[k, at, q]

    def z_send(k, t, q):
        @pl.when(t > z)
        def _():
            z_up(k, t, q).start()

        @pl.when(t < z)
        def _():
            z_down(k, t, q).start()

    def y_stage(n):
        k, t, q = place(n)
        part = user_part(k, (2 * t + y) * SUBS + q)
        with jax.named_scope("rs_y"):
            y_copy(n).wait_recv()
        yrecv[k, t, q] = yrecv[k, t, q] + part

        @pl.when(jnp.logical_and(jnp.logical_not(is_mid), t != z))
        def _():
            z_send(k, t, q)

    def mid_stage(n):
        k, t, q = place(n)

        @pl.when(t != z)
        def _():
            z_add(k, t, t, q)
            z_send(k, t, q)

    def table_out(q):
        return pltpu.make_async_copy(outu.at[q], outu_hbm.at[q], io_sem.at[q])

    item_out = pltpu.make_async_copy(outi, outi_hbm, io_sem.at[SUBS])

    def own_stage(n):
        k, _, q = place(n)

        @pl.when(is_down)
        def _():
            z_add(k, z, z, q)

        @pl.when(is_up)
        def _():
            z_add(k, z, DEPTH, q)
        val = yrecv[k, z, q].astype(BF16)

        @pl.when(k < LAYERS - 1)
        def _():
            panels[k + 1, c, q] = val
            ag_own(k + 1, q)
            item_part(k + 1, c, q)

        @pl.when(k == LAYERS - 1)
        def _():
            tot = (panels[0, c, q].astype(F32) + panels[1, c, q].astype(F32) + panels[2, c, q].astype(F32)
                   + val.astype(F32))
            out = (tot / (LAYERS + 1)).astype(BF16)
            outu[q] = out
            table_out(q).start()
            user_vec[...] += dot_n(out, onehot_a[q])

    def build_round(i):
        _, t, q = place(i)
        build((2 * t + 1 - y) * SUBS + q)
        build((2 * t + y) * SUBS + q)

    base = (r * RING + c) * (SUBS * BLK)
    ids_a = trip[0:1, :] - base
    item_acc[...] = jnp.zeros_like(item_acc)
    user_vec[...] = jnp.zeros_like(user_vec)

    def is_middle(s):
        return lax.div(s * (DEPTH - 1 - s), 2)

    own_lag = 7 - 2 * is_middle(z)
    sets = SUBS * (LAYERS - 1)

    def gather_set(late, event):
        @pl.when(jnp.logical_and(lax.rem(late + 64, 8) == 0, jnp.logical_and(late >= 0, late < 8 * sets)))
        def _():
            m = lax.div(late, 8)
            event(lax.div(m, SUBS) + 1, lax.rem(m, SUBS))

    def gather_mate(half):
        def event(k, q):
            ag_mate(k, q)
            item_part(k, mate, q)
        gather_set(half - (2 * own_lag + 6), event)

    def gather_line(half, d, f):
        for above in (True, False):
            s = z + d if above else z - d

            @pl.when(jnp.logical_and(s < DEPTH, s >= 0))
            def _():
                gather_set(half - (2 * (7 - 2 * is_middle(s)) + 3 * d + (6 if f else 1)),
                           lambda k, q: line_event(k, s, 1 - y if f else y, q, above,
                                                   lambda col, q: item_part(k, col, q)))

    for i in range(AHEAD):
        build_round(jnp.int32(i))
        y_begin(jnp.int32(i))
    for i in range(AHEAD, 4):
        build_round(jnp.int32(i))
    deg_sum(2)
    for q in range(2, SUBS):
        ag_mate(0, q)
        early_event(q)

    def when_at(n, i):
        return pl.when(n == i)

    def one_round(n, carry):
        @when_at(n, 1)
        def _():
            deg_end(1)
            deg_sum(3)

        @when_at(n, 3)
        def _():
            deg_end(2)

        @when_at(n, 5)
        def _():
            deg_end(3)

        @when_at(n, 13)
        def _():
            item_end(0)

        @pl.when(n + AHEAD < LAYERS * ROUNDS)
        def _():
            y_begin(n + AHEAD)

        gather_mate(2 * n)
        for d, f in ((1, 0), (2, 1), (3, 0)):
            gather_line(2 * n, d, f)
        y_stage(n)

        @pl.when(jnp.logical_and(is_mid, n >= 2))
        def _():
            mid_stage(n - 2)
        own = n - own_lag + 3

        @pl.when(jnp.logical_and(lax.rem(own + 4, 4) == 3, jnp.logical_and(own >= 0, own < 2 * ROUNDS)))
        def _():
            own_stage(own)
        for d, f in ((1, 1), (2, 0), (3, 1)):
            gather_line(2 * n + 1, d, f)

        @when_at(n, 46)
        def _():
            col_wait(2 * SUBS, pk_recv.at[pl.ds(0, RING - 1)])
            psum = pk_recv[0].astype(F32)
            for q in range(1, RING):
                psum = psum + pk_recv[q].astype(F32)
            picks[r] = psum.astype(BF16)
            row_send(8, lambda rr: picks.at[r], picks.at[r])

        @pl.when(n >= LAYERS * ROUNDS - SUBS)
        def _():
            own_stage(n)

        @pl.when(jnp.logical_and(n >= 1, n < 7))
        def _():
            build_round(2 * n + 2)
            build_round(2 * n + 3)

        @pl.when(n < 6)
        def _():
            early_event(2 * n + 4)
            early_event(2 * n + 5)

        def late_event(e):
            first_event(e, lambda s, yy, q, above: line_event(
                0, s, yy, q, above, lambda col, q: item_part(0, col, q)))

        def old_event(e):
            first_event(e, lambda s, yy, q, above: item_part(0, 2 * s + yy, q))

        @pl.when(jnp.logical_and(n >= 6, n < 11))
        def _():
            e = 16 + (n - 6) + lax.div(n - 6, 3) + lax.div(n - 6, 4)
            late_event(e)

            @pl.when(n >= 8)
            def _():
                late_event(e + 1)

        @pl.when(jnp.logical_and(n >= 1, n < 9))
        def _():
            q, side = lax.div(n - 1, 2), lax.rem(n - 1, 2)
            item_part(0, c + side * (mate - c), q)
            old_event(q + 4 * side)

        @pl.when(jnp.logical_and(n >= 4, n < 11))
        def _():
            old_event(n + 4 + lax.div(n, 9))

            @pl.when(n == 8)
            def _():
                old_event(n + 5)

        @when_at(n, 10)
        def _():
            item_start(0)

        @when_at(n, 11)
        def _():
            item_share(0, item_sum(0))

        @when_at(n, 26)
        def _():
            item_start(1)

        @when_at(n, 27)
        def _():
            item_share(1, item_sum(1))

        @when_at(n, 29)
        def _():
            item_end(1)

        @pl.when(jnp.logical_and(n >= 32, n < 32 + SUBS))
        def _():
            iota_u = lax.broadcasted_iota(jnp.int32, (BLK, 128), 0) + (n - 32) * BLK
            onehot_a[n - 32] = (iota_u == ids_a).astype(BF16)

        @when_at(n, 43)
        def _():
            last_item = item_sum(2)
            tot = (ei_all[0, r].astype(F32) + ei_all[1, r].astype(F32) + ei_all[2, r].astype(F32)
                   + last_item.astype(F32))
            out_item = (tot / (LAYERS + 1)).astype(BF16)
            outi[...] = out_item
            item_out.start()
            item_share(2, out_item)

        @when_at(n, 44)
        def _():
            item_end(2)
            iota_i = lax.broadcasted_iota(jnp.int32, (BLK, 128), 0) + c * BLK
            hot = jnp.concatenate([(iota_i == trip[1:2, :]).astype(BF16), (iota_i == trip[2:3, :]).astype(BF16)],
                                  axis=1)
            got = dot_n(jnp.concatenate([ei_all[3, q] for q in range(ROWS)], axis=1), hot).astype(BF16)
            for q in range(ROWS):
                pk[q] = got[q * 16:(q + 1) * 16, :]
            col_send(2 * SUBS, lambda cc: pk.at[r], pk_recv.at[c])
            pk_recv[c] = pk[r]

        @when_at(n, 42)
        def _():
            item_start(2)
        return carry
    lax.fori_loop(0, LAYERS * ROUNDS, one_round, 0)

    row_wait(8, picks.at[pl.ds(0, ROWS - 1)])
    ea = user_vec[...]
    both = jnp.concatenate([picks[q] for q in range(ROWS)], axis=0).astype(F32)
    margin = (jnp.sum(ea * both[:, 0:128], axis=0, keepdims=True)
              - jnp.sum(ea * both[:, 128:256], axis=0, keepdims=True))
    term = jnp.maximum(-margin, 0.0) + jnp.log1p(jnp.exp(-jnp.abs(margin)))
    mine = jnp.logical_and(ids_a >= 0, ids_a < SUBS * BLK)
    me = c * ROWS + r
    terms[me] = jnp.where(mine, term, 0.0)
    for peer in all_peers:
        pltpu.make_async_remote_copy(src_ref=terms.at[me], dst_ref=terms.at[me], send_sem=term_sem.at[0],
                                     recv_sem=term_sem.at[1], device_id=peer, device_id_type=MESH).start()

    def drain(ref, sem):
        remote(ref, ref, sem, y_rs.at[0], mate).wait_send()

    drain(ysend, y_ss)
    for q in range(SUBS):
        table_out(q).wait()
    item_out.wait()
    drain(yrecv.at[:, pl.ds(0, DEPTH - 1)], z_ss)
    drain(panels.at[:, pl.ds(0, 1)], ag_sy)
    for at in range(DEPTH):
        @pl.when(z == at)
        def _():
            if at < DEPTH - 1:
                drain(panels.at[:, pl.ds(0, 2 * (at + 1))], ag_su)
            if at > 0:
                drain(panels.at[:, pl.ds(0, 2 * (DEPTH - at))], ag_sd)

    with jax.named_scope("terms_wait"):
        rest = terms.at[pl.ds(0, len(all_peers))]
        cp = pltpu.make_async_remote_copy(src_ref=rest, dst_ref=rest, send_sem=term_sem.at[0],
                                          recv_sem=term_sem.at[1], device_id=all_peers[0], device_id_type=MESH)
        cp.wait_recv()
        cp.wait_send()
    tsum = terms[0]
    for q in range(1, RING * ROWS):
        tsum = tsum + terms[q]
    loss[...] = jnp.broadcast_to(jnp.sum(tsum, axis=1, keepdims=True) / tsum.shape[1], loss.shape)


def deliver(outu, outi, loss, to_user, to_item, to_loss):
    for q in range(SUBS):
        to_user[:, q * BLK:(q + 1) * BLK] = outu[q]
    to_item[...] = outi[...]
    to_loss[...] = loss[0:1, 0:1]


def solution(mesh):
    def local_prog(mask_blk, user_shard, item_shard, triples):
        vmem = pl.BlockSpec(memory_space=pltpu.VMEM)
        hbm = pl.BlockSpec(memory_space=pl.ANY)
        dma = pltpu.SemaphoreType.DMA
        outu, outi, loss = pl.pallas_call(
            kernel,
            out_shape=(jax.ShapeDtypeStruct((SUBS, DIM, BLK), BF16),
                       jax.ShapeDtypeStruct((DIM, 128), BF16),
                       jax.ShapeDtypeStruct((8, 128), F32)),
            in_specs=[hbm] * 4,
            out_specs=(hbm, hbm, vmem),
            scratch_shapes=[
                pltpu.VMEM((RING * SUBS, BLK, BLK), BF16),
                pltpu.VMEM((MASK_BUFS, BLK, BLK), jnp.int32),
                dma((MASK_BUFS,)),
                dma((SUBS + 2,)),
                pltpu.VMEM((3, 128), jnp.int32),
                pltpu.VMEM((SUBS, DIM, BLK), BF16),
                pltpu.VMEM((DIM, 128), BF16),
                pltpu.VMEM((LAYERS, RING, SUBS, DIM, BLK), BF16),
                pltpu.VMEM((LAYERS + 1, ROWS, DIM, 128), BF16),
                pltpu.VMEM((LAYERS, DIM, BLK), F32),
                pltpu.VMEM((LAYERS, ROWS, DIM, 128), F32),
                pltpu.VMEM((LAYERS, ROWS, DIM, 128), F32),
                pltpu.VMEM((LAYERS, DEPTH, SUBS, DIM, BLK), F32),
                pltpu.VMEM((LAYERS, DEPTH, SUBS, DIM, BLK), F32),
                pltpu.VMEM((LAYERS, DEPTH + 1, SUBS, DIM, BLK), F32),
                pltpu.VMEM((8, BLK), F32),
                pltpu.VMEM((RING * SUBS, 1, BLK), F32),
                pltpu.VMEM((RING, SUBS, 1, BLK), F32),
                pltpu.VMEM((RING * SUBS, 1, BLK), F32),
                pltpu.VMEM((1, BLK), F32),
                pltpu.VMEM((ROWS, 1, BLK), F32),
                pltpu.VMEM((1, BLK), F32),
                pltpu.VMEM((SUBS, BLK, 128), BF16),
                pltpu.VMEM((ROWS, 16, 256), BF16),
                pltpu.VMEM((RING, 16, 256), BF16),
                pltpu.VMEM((ROWS, 16, 256), BF16),
                pltpu.VMEM((DIM, 128), F32),
                pltpu.VMEM((RING * ROWS, 1, 128), F32),
                dma((2,)),
                dma, dma((Y_SEMS,)), dma, dma((DEPTH + 1, SUBS)),
                dma, dma, dma, dma((2, RING, SUBS)),
                dma((9,)), dma((9,)), dma((2 * SUBS + 1,)), dma((2 * SUBS + 1,)),
            ],
            compiler_params=pltpu.CompilerParams(
                collective_id=0, has_side_effects=True, vmem_limit_bytes=61 * 1024 * 1024),
            name="propagate",
        )(mask_blk, user_shard.T, item_shard.T, triples.T)
        out_user, out_item, mean = pl.pallas_call(
            deliver,
            out_shape=(jax.ShapeDtypeStruct((DIM, SUBS * BLK), BF16),
                       jax.ShapeDtypeStruct((DIM, 128), BF16),
                       jax.ShapeDtypeStruct((1, 1), F32)),
            in_specs=[vmem, vmem, vmem], out_specs=(vmem, vmem, vmem), name="deliver",
        )(outu, outi, loss)
        return out_user.T, out_item.T, mean[0, 0]

    return jax.shard_map(local_prog, mesh=mesh,
                         in_specs=(P("row", "col"), P(("row", "col"), None), P(("col", "row"), None), P(None, None)),
                         out_specs=(P(("row", "col"), None), P(("col", "row"), None), P()), check_vma=False)
```

```python
import jax
import jax.numpy as jnp
from jax import lax
from jax.experimental import pallas as pl
from jax.experimental.pallas import tpu as pltpu
from jax.sharding import PartitionSpec as P

LAYERS = 3
RING = 8
ROWS = 4
DEPTH = 4
ROUNDS = 16
AHEAD = 3
Y_SEMS = 8
X_LO = 2
X_HI = 3
X_LEAD = 2
SUBS = 4
DIM = 64
BLK = 512
MASK_BUFS = 8
MESH = pl.DeviceIdType.MESH
BF16 = jnp.bfloat16
F32 = jnp.float32


def dot_t(lhs, rhs):
    return lax.dot_general(lhs, rhs, (((1,), (1,)), ((), ())), preferred_element_type=F32)


def dot_n(lhs, rhs):
    return lax.dot_general(lhs, rhs, (((1,), (0,)), ((), ())), preferred_element_type=F32)


def kernel(mask_hbm, euT, eiT, trip_hbm, outu_hbm, outi_hbm, loss,
           adj, mbuf, msem, io_sem, trip, outu, outi,
           panels, ei_all, item_acc, item_send, item_recv,
           ysend, yrecv, zin, xin,
           colsum, deg_part, deg_recv, scale_u, itemdeg, itemdeg_recv, scale_v,
           onehot_a, pk, pk_recv, picks, user_vec, terms, term_sem,
           y_ss, y_rs, x_ss, x_rs, z_ss, z_rs, ag_sy, ag_su, ag_sd, ag_rs,
           row_ss, row_rs, col_ss, col_rs):
    c = lax.axis_index("col")
    r = lax.axis_index("row")
    z, y = lax.div(c, 2), lax.rem(c, 2)
    mate = 2 * z + 1 - y
    is_up, is_down = z < DEPTH - 1, z > 0
    is_mid = jnp.logical_and(is_up, is_down)
    row_peers = [lax.rem(r + d, ROWS) for d in range(1, ROWS)]
    col_peers = [lax.rem(c + d, RING) for d in range(1, RING)]

    def mask_at(i):
        return lax.rem(i, RING) * SUBS + lax.div(i, RING)

    def mask_copy(i):
        slot = lax.rem(i, MASK_BUFS)
        return pltpu.make_async_copy(mask_hbm.at[pl.ds(mask_at(i) * BLK, BLK), :], mbuf.at[slot], msem.at[slot])

    for i in range(MASK_BUFS):
        mask_copy(jnp.int32(i)).start()

    def table_in(q):
        return pltpu.make_async_copy(euT.at[:, pl.ds(q * BLK, BLK)], panels.at[0, c, q], io_sem.at[q])

    item_in = pltpu.make_async_copy(eiT, ei_all.at[0, r], io_sem.at[SUBS])
    trip_in = pltpu.make_async_copy(trip_hbm, trip, io_sem.at[SUBS + 1])
    for q in range(SUBS):
        table_in(q).start()
    item_in.start()
    trip_in.start()

    barrier = pltpu.get_barrier_semaphore()
    all_peers = [(lax.rem(c + dc, RING), lax.rem(r + dr, ROWS))
                 for dc in range(RING) for dr in range(ROWS) if dc or dr]
    for peer in all_peers:
        pl.semaphore_signal(barrier, inc=1, device_id=peer, device_id_type=MESH)

    def remote(src, dst, ss, rs, col):
        return pltpu.make_async_remote_copy(src_ref=src, dst_ref=dst, send_sem=ss, recv_sem=rs,
                                            device_id=(col, r), device_id_type=MESH)

    def ag_rs_of(k, col, q):
        return ag_rs.at[lax.div(k + 1, 2), col, q]

    def ag_y(k, q, col):
        ref = panels.at[k, col, q]
        return remote(ref, ref, ag_sy, ag_rs_of(k, col, q), mate)

    def ag_up(k, col, q):
        ref = panels.at[k, col, q]
        return remote(ref, ref, ag_su, ag_rs_of(k, col, q), c + 2)

    def ag_down(k, col, q):
        ref = panels.at[k, col, q]
        return remote(ref, ref, ag_sd, ag_rs_of(k, col, q), c - 2)

    def ag_both(k, col, q):
        @pl.when(is_up)
        def _():
            ag_up(k, col, q).start()

        @pl.when(is_down)
        def _():
            ag_down(k, col, q).start()

    def ag_own(k, q):
        ag_y(k, q, c).start()
        ag_both(k, c, q)

    def ag_mate(k, q):
        with jax.named_scope("ag_mate"):
            ag_y(k, q, mate).wait_recv()
        ag_both(k, mate, q)

    def line_event(k, s, yy, q, above, then):
        col = 2 * s + yy
        if above:
            with jax.named_scope("ag_above"):
                ag_down(k, col, q).wait_recv()

            @pl.when(is_down)
            def _():
                ag_down(k, col, q).start()
        else:
            with jax.named_scope("ag_below"):
                ag_up(k, col, q).wait_recv()

            @pl.when(is_up)
            def _():
                ag_up(k, col, q).start()
        then(col, q)

    def first_event(e, event):
        d, rest = lax.div(e, 2 * SUBS) + 1, lax.rem(e, 2 * SUBS)
        yy = y + lax.div(rest, SUBS) * (1 - 2 * y)
        q = lax.rem(rest, SUBS)

        @pl.when(z + d < DEPTH)
        def _():
            event(z + d, yy, q, True)

        @pl.when(z - d >= 0)
        def _():
            event(z - d, yy, q, False)

    def row_send(u, src, dst):
        for rr in row_peers:
            pltpu.make_async_remote_copy(src_ref=src(rr), dst_ref=dst, send_sem=row_ss.at[u], recv_sem=row_rs.at[u],
                                         device_id=(c, rr), device_id_type=MESH).start()

    def row_wait(u, ref):
        with jax.named_scope("row_wait_%d" % u):
            cp = pltpu.make_async_remote_copy(src_ref=ref, dst_ref=ref, send_sem=row_ss.at[u], recv_sem=row_rs.at[u],
                                              device_id=(c, row_peers[0]), device_id_type=MESH)
            cp.wait_recv()
            cp.wait_send()

    def col_send(u, src, dst):
        for cc in col_peers:
            remote(src(cc), dst, col_ss.at[u], col_rs.at[u], cc).start()

    def col_wait(u, ref):
        with jax.named_scope("col_wait_%d" % u):
            cp = remote(ref, ref, col_ss.at[u], col_rs.at[u], mate)
            cp.wait_recv()
            cp.wait_send()

    ones = jnp.ones((16, BLK), BF16)
    colsum[...] = jnp.zeros_like(colsum)

    def mask_block(i, carry):
        slot, b = lax.rem(i, MASK_BUFS), mask_at(i)
        mask_copy(i).wait()
        acc = jnp.zeros((8, BLK), F32)
        for t in range(4):
            m = mbuf[slot, t * 128:(t + 1) * 128, :].astype(F32)
            acc = acc + jnp.sum(m.reshape(16, 8, BLK), axis=0)
            adj[b, t * 128:(t + 1) * 128, :] = m.astype(BF16)
        colsum[...] += acc
        deg_part[b] = dot_t(ones, adj[b])[0:1, :]

        @pl.when(i + MASK_BUFS < SUBS * RING)
        def _():
            mask_copy(i + MASK_BUFS).start()
        return carry

    def deg_send(q):
        col_send(q, lambda cc: deg_part.at[cc * SUBS + q], deg_recv.at[c, q])
        deg_recv[c, q] = deg_part[c * SUBS + q]

    def deg_sum(q):
        col_wait(q, deg_part.at[pl.ds(0, RING - 1)])
        du = deg_recv[0, q]
        for cc in range(1, RING):
            du = du + deg_recv[cc, q]
        scale_u[c * SUBS + q] = lax.rsqrt(jnp.maximum(du, 1.0))
        col_send(SUBS + q, lambda cc: scale_u.at[c * SUBS + q], scale_u.at[c * SUBS + q])

    def deg_end(q):
        col_wait(SUBS + q, deg_part.at[pl.ds(0, RING - 1)])

    def mask_quarter(q):
        with jax.named_scope("mask"):
            lax.fori_loop(RING * q, RING * (q + 1), mask_block, 0)

    def early_event(e):
        first_event(jnp.int32(e), lambda s, yy, q, above: line_event(0, s, yy, q, above, lambda col, q: None))

    mask_quarter(0)
    for q in range(SUBS):
        table_in(q).wait()
    item_in.wait()
    trip_in.wait()
    with jax.named_scope("entry"):
        pl.semaphore_wait(barrier, len(all_peers))
    deg_send(0)
    ag_own(0, 0)
    ag_own(0, 1)
    row_send(0, lambda rr: ei_all.at[0, r], ei_all.at[0, r])
    mask_quarter(1)
    deg_send(1)
    ag_own(0, 2)
    mask_quarter(2)
    deg_send(2)
    ag_own(0, 3)
    deg_sum(0)
    for q in range(2):
        ag_mate(0, q)
        early_event(q)
    mask_quarter(3)
    itemdeg[...] = jnp.sum(colsum[...], axis=0, keepdims=True)
    row_send(1, lambda rr: itemdeg, itemdeg_recv.at[r])
    deg_send(3)
    itemdeg_recv[r] = itemdeg[...]
    deg_sum(1)
    row_wait(1, itemdeg_recv.at[pl.ds(0, ROWS - 1)])
    dv = itemdeg_recv[0] + itemdeg_recv[1] + itemdeg_recv[2] + itemdeg_recv[3]
    scale_v[...] = lax.rsqrt(jnp.maximum(dv, 1.0))
    row_wait(0, ei_all.at[0, pl.ds(0, ROWS - 1)])
    deg_end(0)

    def build(b):
        sv = scale_v[...]
        for t in range(4):
            su = scale_u[b, :, t * 128:(t + 1) * 128]
            suc = jnp.transpose(jnp.broadcast_to(su, (128, 128)))
            val = (jnp.concatenate([suc] * 4, axis=1) * sv).astype(BF16)
            adj[b, t * 128:(t + 1) * 128, :] = adj[b, t * 128:(t + 1) * 128, :] * val

    def user_part(k, b):
        ei = jnp.concatenate([ei_all[k, q] for q in range(ROWS)], axis=1)
        return dot_t(ei, adj[b])

    def item_part(k, col, q):
        item_acc[k] += dot_n(panels[k, col, q], adj[col * SUBS + q])

    def item_start(k):
        for q in range(ROWS):
            item_send[k, q] = item_acc[k, :, q * 128:(q + 1) * 128]
        row_send(2 + 2 * k, lambda rr: item_send.at[k, rr], item_recv.at[k, r])
        item_recv[k, r] = item_send[k, r]

    def item_sum(k):
        row_wait(2 + 2 * k, item_send.at[k, pl.ds(0, ROWS - 1)])
        tot = item_recv[k, 0] + item_recv[k, 1] + item_recv[k, 2] + item_recv[k, 3]
        return tot.astype(BF16)

    def item_share(k, val):
        ei_all[k + 1, r] = val
        row_send(3 + 2 * k, lambda rr: ei_all.at[k + 1, r], ei_all.at[k + 1, r])

    def item_end(k):
        row_wait(3 + 2 * k, ei_all.at[k + 1, pl.ds(0, ROWS - 1)])

    def place(n):
        k, i = lax.div(n, ROUNDS), lax.rem(n, ROUNDS)
        last, own = lax.div(k, LAYERS - 1), lax.div(i, 12)
        q, g = lax.div(i, 4), lax.rem(i, 4)
        q_last = (1 - own) * lax.div(i, 3) + own * (i - 12)
        g_last = (1 - own) * lax.rem(i, 3) + own * 3
        q, g = q + last * (q_last - q), g + last * (g_last - g)
        pw = 1 + 3 * g + 9 * lax.div(g * (g - 1), 2) + 27 * lax.div(g * (g - 1) * (g - 2), 6)
        return k, lax.rem(lax.div(27 + 48 * z + 57 * lax.div(z, 2), pw), DEPTH), q

    def y_set(k, q):
        later = lax.div(k + 1, 2)
        skip = lax.div(q + SUBS - X_LO, SUBS) * (1 - lax.div(q + SUBS - X_HI, SUBS))
        return later + (1 - later) * 2 * skip

    def y_copy(n):
        k, t, q = place(n)
        return remote(ysend.at[k, t, q], yrecv.at[k, t, q], y_ss.at[y_set(k, q)], y_rs.at[lax.rem(n, Y_SEMS)], mate)

    def is_middle(s):
        return lax.div(s * (DEPTH - 1 - s), 2)

    inner = 1 + lax.rem(z, 2)
    x_from = lax.div(z, 2)
    x_last = 2 - is_middle(z)

    def skips_y(n):
        return jnp.logical_and(lax.rem(n, DEPTH) == x_last, jnp.logical_and(n >= 4 * X_LO, n < 4 * X_HI))

    def x_copy(q, side):
        return remote(ysend.at[0, inner, q], xin.at[side, q], x_ss.at[q], x_rs.at[side, q], 2 * inner + y)

    def x_begin(q):
        ysend[0, inner, q] = user_part(0, (2 * inner + 1 - y) * SUBS + q)
        x_copy(q, x_from).start()

    def y_begin(n):
        k, t, q = place(n)

        @pl.when(jnp.logical_not(skips_y(n)))
        def _():
            ysend[k, t, q] = user_part(k, (2 * t + 1 - y) * SUBS + q)
            takes = jnp.logical_and(lax.rem(n, DEPTH) == DEPTH - 1, jnp.logical_and(n >= 4 * X_LO, n < 4 * X_HI))

            @pl.when(jnp.logical_and(is_mid, takes))
            def _():
                for side in range(2):
                    with jax.named_scope("rs_x"):
                        x_copy(q, side).wait_recv()
                    ysend[k, t, q] = ysend[k, t, q] + xin[side, q]
            y_copy(n).start()

    def z_up(k, t, q):
        return remote(yrecv.at[k, t, q], zin.at[k, t, q], z_ss, z_rs.at[t, q], c + 2)

    def z_down(k, t, q):
        to = t + lax.div(2 - (z - 1 - t), 2) * (DEPTH - t)
        return remote(yrecv.at[k, t, q], zin.at[k, to, q], z_ss, z_rs.at[to, q], c - 2)

    def z_add(k, t, at, q):
        with jax.named_scope("rs_z"):
            remote(yrecv.at[k, t, q], zin.at[k, at, q], z_ss, z_rs.at[at, q], mate).wait_recv()
        yrecv[k, t, q] = yrecv[k, t, q] + zin[k, at, q]

    def z_send(k, t, q):
        @pl.when(t > z)
        def _():
            z_up(k, t, q).start()

        @pl.when(t < z)
        def _():
            z_down(k, t, q).start()

    def y_stage(n):
        k, t, q = place(n)
        part = user_part(k, (2 * t + y) * SUBS + q)
        skipped = skips_y(n)

        @pl.when(skipped)
        def _():
            yrecv[k, t, q] = part

        @pl.when(jnp.logical_not(skipped))
        def _():
            with jax.named_scope("rs_y"):
                y_copy(n).wait_recv()
            yrecv[k, t, q] = yrecv[k, t, q] + part

        @pl.when(jnp.logical_and(jnp.logical_not(is_mid), t != z))
        def _():
            z_send(k, t, q)

    def mid_stage(n):
        k, t, q = place(n)

        @pl.when(t != z)
        def _():
            z_add(k, t, t, q)
            z_send(k, t, q)

    def table_out(q):
        return pltpu.make_async_copy(outu.at[q], outu_hbm.at[q], io_sem.at[q])

    item_out = pltpu.make_async_copy(outi, outi_hbm, io_sem.at[SUBS])

    def own_stage(n):
        k, _, q = place(n)

        @pl.when(is_down)
        def _():
            z_add(k, z, z, q)

        @pl.when(is_up)
        def _():
            z_add(k, z, DEPTH, q)
        val = yrecv[k, z, q].astype(BF16)

        @pl.when(k < LAYERS - 1)
        def _():
            panels[k + 1, c, q] = val
            ag_own(k + 1, q)
            item_part(k + 1, c, q)

        @pl.when(k == LAYERS - 1)
        def _():
            tot = (panels[0, c, q].astype(F32) + panels[1, c, q].astype(F32) + panels[2, c, q].astype(F32)
                   + val.astype(F32))
            out = (tot / (LAYERS + 1)).astype(BF16)
            outu[q] = out
            table_out(q).start()
            user_vec[...] += dot_n(out, onehot_a[q])

    def build_round(i):
        _, t, q = place(i)
        build((2 * t + 1 - y) * SUBS + q)
        build((2 * t + y) * SUBS + q)

    base = (r * RING + c) * (SUBS * BLK)
    ids_a = trip[0:1, :] - base
    item_acc[...] = jnp.zeros_like(item_acc)
    user_vec[...] = jnp.zeros_like(user_vec)

    own_lag = 7 - 2 * is_middle(z)
    sets = SUBS * (LAYERS - 1)

    def gather_set(late, event):
        @pl.when(jnp.logical_and(lax.rem(late + 64, 8) == 0, jnp.logical_and(late >= 0, late < 8 * sets)))
        def _():
            m = lax.div(late, 8)
            event(lax.div(m, SUBS) + 1, lax.rem(m, SUBS))

    def gather_mate(half):
        def event(k, q):
            ag_mate(k, q)
            item_part(k, mate, q)
        gather_set(half - (2 * own_lag + 6), event)

    def gather_line(half, d, f):
        for above in (True, False):
            s = z + d if above else z - d

            @pl.when(jnp.logical_and(s < DEPTH, s >= 0))
            def _():
                gather_set(half - (2 * (7 - 2 * is_middle(s)) + 3 * d + (6 if f else 1)),
                           lambda k, q: line_event(k, s, 1 - y if f else y, q, above,
                                                   lambda col, q: item_part(k, col, q)))

    for i in range(AHEAD):
        build_round(jnp.int32(i))
        y_begin(jnp.int32(i))
    for i in range(AHEAD, 4):
        build_round(jnp.int32(i))
    deg_sum(2)
    for q in range(2, SUBS):
        ag_mate(0, q)
        early_event(q)

    def when_at(n, i):
        return pl.when(n == i)

    def one_round(n, carry):
        @when_at(n, 1)
        def _():
            deg_sum(3)

        @when_at(n, 2)
        def _():
            deg_end(2)

        @when_at(n, 4)
        def _():
            deg_end(3)

        @when_at(n, 13)
        def _():
            item_end(0)

        @pl.when(n + AHEAD < LAYERS * ROUNDS)
        def _():
            y_begin(n + AHEAD)

        @pl.when(jnp.logical_and(lax.rem(n + X_LEAD, DEPTH) == 0,
                                 jnp.logical_and(n + X_LEAD >= 4 * X_LO, n + X_LEAD < 4 * X_HI)))
        def _():
            x_begin(lax.div(n + X_LEAD, DEPTH))
        gather_mate(2 * n)
        for d, f in ((1, 0), (2, 1), (3, 0)):
            gather_line(2 * n, d, f)
        y_stage(n)

        @pl.when(jnp.logical_and(is_mid, n >= 2))
        def _():
            mid_stage(n - 2)
        own = n - own_lag + 3

        @pl.when(jnp.logical_and(lax.rem(own + 4, 4) == 3, jnp.logical_and(own >= 0, own < 2 * ROUNDS)))
        def _():
            own_stage(own)
        for d, f in ((1, 1), (2, 0), (3, 1)):
            gather_line(2 * n + 1, d, f)

        @when_at(n, 46)
        def _():
            col_wait(2 * SUBS, pk_recv.at[pl.ds(0, RING - 1)])
            psum = pk_recv[0].astype(F32)
            for q in range(1, RING):
                psum = psum + pk_recv[q].astype(F32)
            picks[r] = psum.astype(BF16)
            row_send(8, lambda rr: picks.at[r], picks.at[r])

        @pl.when(n >= LAYERS * ROUNDS - SUBS)
        def _():
            own_stage(n)

        @when_at(n, 0)
        def _():
            deg_end(1)

        @pl.when(n < 6)
        def _():
            build_round(2 * n + 4)
            build_round(2 * n + 5)

        @pl.when(n < 6)
        def _():
            early_event(2 * n + 4)
            early_event(2 * n + 5)

        def late_event(e):
            first_event(e, lambda s, yy, q, above: line_event(
                0, s, yy, q, above, lambda col, q: item_part(0, col, q)))

        def old_event(e):
            first_event(e, lambda s, yy, q, above: item_part(0, 2 * s + yy, q))

        @pl.when(jnp.logical_and(n >= 6, n < 11))
        def _():
            e = 16 + (n - 6) + lax.div(n - 6, 3) + lax.div(n - 6, 4)
            late_event(e)

            @pl.when(n >= 8)
            def _():
                late_event(e + 1)

        @pl.when(jnp.logical_and(n >= 1, n < 9))
        def _():
            q, side = lax.div(n - 1, 2), lax.rem(n - 1, 2)
            item_part(0, c + side * (mate - c), q)
            old_event(q + 4 * side)

        @pl.when(jnp.logical_and(n >= 4, n < 11))
        def _():
            old_event(n + 4 + lax.div(n, 9))

            @pl.when(n == 8)
            def _():
                old_event(n + 5)

        @when_at(n, 10)
        def _():
            item_start(0)

        @when_at(n, 11)
        def _():
            item_share(0, item_sum(0))

        @when_at(n, 26)
        def _():
            item_start(1)

        @when_at(n, 27)
        def _():
            item_share(1, item_sum(1))

        @when_at(n, 28)
        def _():
            item_end(1)

        @pl.when(jnp.logical_and(n >= 32, n < 32 + SUBS))
        def _():
            iota_u = lax.broadcasted_iota(jnp.int32, (BLK, 128), 0) + (n - 32) * BLK
            onehot_a[n - 32] = (iota_u == ids_a).astype(BF16)

        @when_at(n, 43)
        def _():
            last_item = item_sum(2)
            tot = (ei_all[0, r].astype(F32) + ei_all[1, r].astype(F32) + ei_all[2, r].astype(F32)
                   + last_item.astype(F32))
            out_item = (tot / (LAYERS + 1)).astype(BF16)
            outi[...] = out_item
            item_out.start()
            item_share(2, out_item)

        @when_at(n, 44)
        def _():
            item_end(2)
            iota_i = lax.broadcasted_iota(jnp.int32, (BLK, 128), 0) + c * BLK
            hot = jnp.concatenate([(iota_i == trip[1:2, :]).astype(BF16), (iota_i == trip[2:3, :]).astype(BF16)],
                                  axis=1)
            got = dot_n(jnp.concatenate([ei_all[3, q] for q in range(ROWS)], axis=1), hot).astype(BF16)
            for q in range(ROWS):
                pk[q] = got[q * 16:(q + 1) * 16, :]
            col_send(2 * SUBS, lambda cc: pk.at[r], pk_recv.at[c])
            pk_recv[c] = pk[r]

        @when_at(n, 42)
        def _():
            item_start(2)
        return carry
    lax.fori_loop(0, LAYERS * ROUNDS, one_round, 0)

    row_wait(8, picks.at[pl.ds(0, ROWS - 1)])
    ea = user_vec[...]
    both = jnp.concatenate([picks[q] for q in range(ROWS)], axis=0).astype(F32)
    margin = (jnp.sum(ea * both[:, 0:128], axis=0, keepdims=True)
              - jnp.sum(ea * both[:, 128:256], axis=0, keepdims=True))
    term = jnp.maximum(-margin, 0.0) + jnp.log1p(jnp.exp(-jnp.abs(margin)))
    mine = jnp.logical_and(ids_a >= 0, ids_a < SUBS * BLK)
    me = c * ROWS + r
    terms[me] = jnp.where(mine, term, 0.0)
    for peer in all_peers:
        pltpu.make_async_remote_copy(src_ref=terms.at[me], dst_ref=terms.at[me], send_sem=term_sem.at[0],
                                     recv_sem=term_sem.at[1], device_id=peer, device_id_type=MESH).start()

    def drain(ref, sem):
        remote(ref, ref, sem, y_rs.at[0], mate).wait_send()

    drain(ysend.at[pl.ds(1, LAYERS - 1)], y_ss.at[1])
    drain(ysend.at[0, :, pl.ds(0, SUBS - X_HI + X_LO)], y_ss.at[0])
    drain(ysend.at[0, pl.ds(0, DEPTH - 1), pl.ds(0, X_HI - X_LO)], y_ss.at[2])
    for q in range(X_LO, X_HI):
        drain(xin.at[0, q], x_ss.at[q])
    for q in range(SUBS):
        table_out(q).wait()
    item_out.wait()
    drain(yrecv.at[:, pl.ds(0, DEPTH - 1)], z_ss)
    drain(panels.at[:, pl.ds(0, 1)], ag_sy)
    for at in range(DEPTH):
        @pl.when(z == at)
        def _():
            if at < DEPTH - 1:
                drain(panels.at[:, pl.ds(0, 2 * (at + 1))], ag_su)
            if at > 0:
                drain(panels.at[:, pl.ds(0, 2 * (DEPTH - at))], ag_sd)

    with jax.named_scope("terms_wait"):
        rest = terms.at[pl.ds(0, len(all_peers))]
        cp = pltpu.make_async_remote_copy(src_ref=rest, dst_ref=rest, send_sem=term_sem.at[0],
                                          recv_sem=term_sem.at[1], device_id=all_peers[0], device_id_type=MESH)
        cp.wait_recv()
        cp.wait_send()
    tsum = terms[0]
    for q in range(1, RING * ROWS):
        tsum = tsum + terms[q]
    loss[...] = jnp.broadcast_to(jnp.sum(tsum, axis=1, keepdims=True) / tsum.shape[1], loss.shape)


def deliver(outu, outi, loss, to_user, to_item, to_loss):
    for q in range(SUBS):
        to_user[:, q * BLK:(q + 1) * BLK] = outu[q]
    to_item[...] = outi[...]
    to_loss[...] = loss[0:1, 0:1]


def solution(mesh):
    def local_prog(mask_blk, user_shard, item_shard, triples):
        vmem = pl.BlockSpec(memory_space=pltpu.VMEM)
        hbm = pl.BlockSpec(memory_space=pl.ANY)
        dma = pltpu.SemaphoreType.DMA
        outu, outi, loss = pl.pallas_call(
            kernel,
            out_shape=(jax.ShapeDtypeStruct((SUBS, DIM, BLK), BF16),
                       jax.ShapeDtypeStruct((DIM, 128), BF16),
                       jax.ShapeDtypeStruct((8, 128), F32)),
            in_specs=[hbm] * 4,
            out_specs=(hbm, hbm, vmem),
            scratch_shapes=[
                pltpu.VMEM((RING * SUBS, BLK, BLK), BF16),
                pltpu.VMEM((MASK_BUFS, BLK, BLK), jnp.int32),
                dma((MASK_BUFS,)),
                dma((SUBS + 2,)),
                pltpu.VMEM((3, 128), jnp.int32),
                pltpu.VMEM((SUBS, DIM, BLK), BF16),
                pltpu.VMEM((DIM, 128), BF16),
                pltpu.VMEM((LAYERS, RING, SUBS, DIM, BLK), BF16),
                pltpu.VMEM((LAYERS + 1, ROWS, DIM, 128), BF16),
                pltpu.VMEM((LAYERS, DIM, BLK), F32),
                pltpu.VMEM((LAYERS, ROWS, DIM, 128), F32),
                pltpu.VMEM((LAYERS, ROWS, DIM, 128), F32),
                pltpu.VMEM((LAYERS, DEPTH, SUBS, DIM, BLK), F32),
                pltpu.VMEM((LAYERS, DEPTH, SUBS, DIM, BLK), F32),
                pltpu.VMEM((LAYERS, DEPTH + 1, SUBS, DIM, BLK), F32),
                pltpu.VMEM((2, SUBS, DIM, BLK), F32),
                pltpu.VMEM((8, BLK), F32),
                pltpu.VMEM((RING * SUBS, 1, BLK), F32),
                pltpu.VMEM((RING, SUBS, 1, BLK), F32),
                pltpu.VMEM((RING * SUBS, 1, BLK), F32),
                pltpu.VMEM((1, BLK), F32),
                pltpu.VMEM((ROWS, 1, BLK), F32),
                pltpu.VMEM((1, BLK), F32),
                pltpu.VMEM((SUBS, BLK, 128), BF16),
                pltpu.VMEM((ROWS, 16, 256), BF16),
                pltpu.VMEM((RING, 16, 256), BF16),
                pltpu.VMEM((ROWS, 16, 256), BF16),
                pltpu.VMEM((DIM, 128), F32),
                pltpu.VMEM((RING * ROWS, 1, 128), F32),
                dma((2,)),
                dma((3,)), dma((Y_SEMS,)), dma((SUBS,)), dma((2, SUBS)), dma, dma((DEPTH + 1, SUBS)),
                dma, dma, dma, dma((2, RING, SUBS)),
                dma((9,)), dma((9,)), dma((2 * SUBS + 1,)), dma((2 * SUBS + 1,)),
            ],
            compiler_params=pltpu.CompilerParams(
                collective_id=0, has_side_effects=True, vmem_limit_bytes=61 * 1024 * 1024),
            name="propagate",
        )(mask_blk, user_shard.T, item_shard.T, triples.T)
        out_user, out_item, mean = pl.pallas_call(
            deliver,
            out_shape=(jax.ShapeDtypeStruct((DIM, SUBS * BLK), BF16),
                       jax.ShapeDtypeStruct((DIM, 128), BF16),
                       jax.ShapeDtypeStruct((1, 1), F32)),
            in_specs=[vmem, vmem, vmem], out_specs=(vmem, vmem, vmem), name="deliver",
        )(outu, outi, loss)
        return out_user.T, out_item.T, mean[0, 0]

    return jax.shard_map(local_prog, mesh=mesh,
                         in_specs=(P("row", "col"), P(("row", "col"), None), P(("col", "row"), None), P(None, None)),
                         out_specs=(P(("row", "col"), None), P(("col", "row"), None), P()), check_vma=False)
```

```python
import jax
import jax.numpy as jnp
from jax import lax
from jax.experimental import pallas as pl
from jax.experimental.pallas import tpu as pltpu
from jax.sharding import PartitionSpec as P

LAYERS = 3
RING = 8
ROWS = 4
DEPTH = 4
ROUNDS = 16
AHEAD = 3
Y_SEMS = 8
ROW_SET = (0, 1, 2, 1, 2, 1, 2, 1, 2)
X_LO = 2
X_HI = 3
X_LEAD = 2
SUBS = 4
DIM = 64
BLK = 512
MASK_BUFS = 8
MESH = pl.DeviceIdType.MESH
BF16 = jnp.bfloat16
F32 = jnp.float32


def dot_t(lhs, rhs):
    return lax.dot_general(lhs, rhs, (((1,), (1,)), ((), ())), preferred_element_type=F32)


def dot_n(lhs, rhs):
    return lax.dot_general(lhs, rhs, (((1,), (0,)), ((), ())), preferred_element_type=F32)


def kernel(mask_hbm, euT, eiT, trip_hbm, outu_hbm, outi_hbm, loss,
           adj, mbuf, msem, io_sem, trip, outu, outi,
           panels, ei_all, item_acc, item_send, item_recv,
           ysend, yrecv, zin, xin,
           colsum, deg_part, deg_recv, scale_u, itemdeg, itemdeg_recv, scale_v,
           onehot_a, pk, pk_recv, picks, user_vec, terms, term_sem,
           y_ss, y_rs, x_ss, x_rs, z_ss, z_rs, ag_sy, ag_su, ag_sd, ag_rs,
           row_ss, row_rs, col_ss, col_rs):
    c = lax.axis_index("col")
    r = lax.axis_index("row")
    z, y = lax.div(c, 2), lax.rem(c, 2)
    mate = 2 * z + 1 - y
    is_up, is_down = z < DEPTH - 1, z > 0
    is_mid = jnp.logical_and(is_up, is_down)
    row_peers = [lax.rem(r + d, ROWS) for d in range(1, ROWS)]
    col_peers = [lax.rem(c + d, RING) for d in range(1, RING)]

    def mask_at(i):
        return lax.rem(i, RING) * SUBS + lax.div(i, RING)

    def mask_copy(i):
        slot = lax.rem(i, MASK_BUFS)
        return pltpu.make_async_copy(mask_hbm.at[pl.ds(mask_at(i) * BLK, BLK), :], mbuf.at[slot], msem.at[slot])

    for i in range(MASK_BUFS):
        mask_copy(jnp.int32(i)).start()

    def table_in(q):
        return pltpu.make_async_copy(euT.at[:, pl.ds(q * BLK, BLK)], panels.at[0, c, q], io_sem.at[q])

    item_in = pltpu.make_async_copy(eiT, ei_all.at[0, r], io_sem.at[SUBS])
    trip_in = pltpu.make_async_copy(trip_hbm, trip, io_sem.at[SUBS + 1])
    for q in range(SUBS):
        table_in(q).start()
    item_in.start()
    trip_in.start()

    barrier = pltpu.get_barrier_semaphore()
    all_peers = [(lax.rem(c + dc, RING), lax.rem(r + dr, ROWS))
                 for dc in range(RING) for dr in range(ROWS) if dc or dr]
    for peer in all_peers:
        pl.semaphore_signal(barrier, inc=1, device_id=peer, device_id_type=MESH)

    def remote(src, dst, ss, rs, col):
        return pltpu.make_async_remote_copy(src_ref=src, dst_ref=dst, send_sem=ss, recv_sem=rs,
                                            device_id=(col, r), device_id_type=MESH)

    def ag_rs_of(k, col, q):
        return ag_rs.at[lax.div(k + 1, 2), col, q]

    def ag_y(k, q, col):
        ref = panels.at[k, col, q]
        return remote(ref, ref, ag_sy, ag_rs_of(k, col, q), mate)

    def ag_up(k, col, q):
        ref = panels.at[k, col, q]
        return remote(ref, ref, ag_su, ag_rs_of(k, col, q), c + 2)

    def ag_down(k, col, q):
        ref = panels.at[k, col, q]
        return remote(ref, ref, ag_sd, ag_rs_of(k, col, q), c - 2)

    def ag_both(k, col, q):
        @pl.when(is_up)
        def _():
            ag_up(k, col, q).start()

        @pl.when(is_down)
        def _():
            ag_down(k, col, q).start()

    def ag_own(k, q):
        ag_y(k, q, c).start()
        ag_both(k, c, q)

    def ag_mate(k, q):
        with jax.named_scope("ag_mate"):
            ag_y(k, q, mate).wait_recv()
        ag_both(k, mate, q)

    def line_event(k, s, yy, q, above, then):
        col = 2 * s + yy
        if above:
            with jax.named_scope("ag_above"):
                ag_down(k, col, q).wait_recv()

            @pl.when(is_down)
            def _():
                ag_down(k, col, q).start()
        else:
            with jax.named_scope("ag_below"):
                ag_up(k, col, q).wait_recv()

            @pl.when(is_up)
            def _():
                ag_up(k, col, q).start()
        then(col, q)

    def first_event(e, event):
        d, rest = lax.div(e, 2 * SUBS) + 1, lax.rem(e, 2 * SUBS)
        yy = y + lax.div(rest, SUBS) * (1 - 2 * y)
        q = lax.rem(rest, SUBS)

        @pl.when(z + d < DEPTH)
        def _():
            event(z + d, yy, q, True)

        @pl.when(z - d >= 0)
        def _():
            event(z - d, yy, q, False)

    def row_send(u, src, dst):
        for rr in row_peers:
            pltpu.make_async_remote_copy(src_ref=src(rr), dst_ref=dst, send_sem=row_ss.at[ROW_SET[u]], recv_sem=row_rs.at[ROW_SET[u]],
                                         device_id=(c, rr), device_id_type=MESH).start()

    def row_wait(u, ref):
        with jax.named_scope("row_wait_%d" % u):
            cp = pltpu.make_async_remote_copy(src_ref=ref, dst_ref=ref, send_sem=row_ss.at[ROW_SET[u]], recv_sem=row_rs.at[ROW_SET[u]],
                                              device_id=(c, row_peers[0]), device_id_type=MESH)
            cp.wait_recv()
            cp.wait_send()

    def col_send(u, src, dst):
        for cc in col_peers:
            remote(src(cc), dst, col_ss.at[u], col_rs.at[u], cc).start()

    def col_wait(u, ref):
        with jax.named_scope("col_wait_%d" % u):
            cp = remote(ref, ref, col_ss.at[u], col_rs.at[u], mate)
            cp.wait_recv()
            cp.wait_send()

    ones = jnp.ones((16, BLK), BF16)
    colsum[...] = jnp.zeros_like(colsum)

    def mask_block(i, carry):
        slot, b = lax.rem(i, MASK_BUFS), mask_at(i)
        mask_copy(i).wait()
        acc = jnp.zeros((8, BLK), F32)
        for t in range(4):
            m = mbuf[slot, t * 128:(t + 1) * 128, :].astype(F32)
            acc = acc + jnp.sum(m.reshape(16, 8, BLK), axis=0)
            adj[b, t * 128:(t + 1) * 128, :] = m.astype(BF16)
        colsum[...] += acc
        deg_part[b] = dot_t(ones, adj[b])[0:1, :]

        @pl.when(i + MASK_BUFS < SUBS * RING)
        def _():
            mask_copy(i + MASK_BUFS).start()
        return carry

    def deg_send(q):
        col_send(q, lambda cc: deg_part.at[cc * SUBS + q], deg_recv.at[c, q])
        deg_recv[c, q] = deg_part[c * SUBS + q]

    def deg_sum(q):
        col_wait(q, deg_part.at[pl.ds(0, RING - 1)])
        du = deg_recv[0, q]
        for cc in range(1, RING):
            du = du + deg_recv[cc, q]
        scale_u[c * SUBS + q] = lax.rsqrt(jnp.maximum(du, 1.0))
        col_send(SUBS + q, lambda cc: scale_u.at[c * SUBS + q], scale_u.at[c * SUBS + q])

    def deg_end(q):
        col_wait(SUBS + q, deg_part.at[pl.ds(0, RING - 1)])

    def mask_quarter(q):
        with jax.named_scope("mask"):
            lax.fori_loop(RING * q, RING * (q + 1), mask_block, 0)

    def early_event(e):
        first_event(jnp.int32(e), lambda s, yy, q, above: line_event(0, s, yy, q, above, lambda col, q: None))

    mask_quarter(0)
    for q in range(SUBS):
        table_in(q).wait()
    item_in.wait()
    trip_in.wait()
    with jax.named_scope("entry"):
        pl.semaphore_wait(barrier, len(all_peers))
    deg_send(0)
    ag_own(0, 0)
    ag_own(0, 1)
    row_send(0, lambda rr: ei_all.at[0, r], ei_all.at[0, r])
    mask_quarter(1)
    deg_send(1)
    ag_own(0, 2)
    mask_quarter(2)
    deg_send(2)
    deg_sum(0)
    ag_own(0, 3)
    for q in range(2):
        ag_mate(0, q)
        early_event(q)
    mask_quarter(3)
    itemdeg[...] = jnp.sum(colsum[...], axis=0, keepdims=True)
    row_send(1, lambda rr: itemdeg, itemdeg_recv.at[r])
    deg_send(3)
    itemdeg_recv[r] = itemdeg[...]
    deg_sum(1)
    row_wait(1, itemdeg_recv.at[pl.ds(0, ROWS - 1)])
    dv = itemdeg_recv[0] + itemdeg_recv[1] + itemdeg_recv[2] + itemdeg_recv[3]
    scale_v[...] = lax.rsqrt(jnp.maximum(dv, 1.0))
    row_wait(0, ei_all.at[0, pl.ds(0, ROWS - 1)])
    deg_end(0)

    def build(b):
        sv = scale_v[...]
        for t in range(4):
            su = scale_u[b, :, t * 128:(t + 1) * 128]
            suc = jnp.transpose(jnp.broadcast_to(su, (128, 128)))
            val = (jnp.concatenate([suc] * 4, axis=1) * sv).astype(BF16)
            adj[b, t * 128:(t + 1) * 128, :] = adj[b, t * 128:(t + 1) * 128, :] * val

    def user_part(k, b):
        ei = jnp.concatenate([ei_all[k, q] for q in range(ROWS)], axis=1)
        return dot_t(ei, adj[b])

    def item_part(k, col, q):
        item_acc[k] += dot_n(panels[k, col, q], adj[col * SUBS + q])

    def item_start(k):
        for q in range(ROWS):
            item_send[k, q] = item_acc[k, :, q * 128:(q + 1) * 128]
        row_send(2 + 2 * k, lambda rr: item_send.at[k, rr], item_recv.at[k, r])
        item_recv[k, r] = item_send[k, r]

    def item_sum(k):
        row_wait(2 + 2 * k, item_send.at[k, pl.ds(0, ROWS - 1)])
        tot = item_recv[k, 0] + item_recv[k, 1] + item_recv[k, 2] + item_recv[k, 3]
        return tot.astype(BF16)

    def item_share(k, val):
        ei_all[k + 1, r] = val
        row_send(3 + 2 * k, lambda rr: ei_all.at[k + 1, r], ei_all.at[k + 1, r])

    def item_end(k):
        row_wait(3 + 2 * k, ei_all.at[k + 1, pl.ds(0, ROWS - 1)])

    def place(n):
        k, i = lax.div(n, ROUNDS), lax.rem(n, ROUNDS)
        last, own = lax.div(k, LAYERS - 1), lax.div(i, 12)
        q, g = lax.div(i, 4), lax.rem(i, 4)
        q_last = (1 - own) * lax.div(i, 3) + own * (i - 12)
        g_last = (1 - own) * lax.rem(i, 3) + own * 3
        q, g = q + last * (q_last - q), g + last * (g_last - g)
        pw = 1 + 3 * g + 9 * lax.div(g * (g - 1), 2) + 27 * lax.div(g * (g - 1) * (g - 2), 6)
        return k, lax.rem(lax.div(27 + 48 * z + 57 * lax.div(z, 2), pw), DEPTH), q

    def y_set(k, q):
        later = lax.div(k + 1, 2)
        skip = lax.div(q + SUBS - X_LO, SUBS) * (1 - lax.div(q + SUBS - X_HI, SUBS))
        return later + (1 - later) * 2 * skip

    def y_copy(n):
        k, t, q = place(n)
        return remote(ysend.at[k, t, q], yrecv.at[k, t, q], y_ss.at[y_set(k, q)], y_rs.at[lax.rem(n, Y_SEMS)], mate)

    def is_middle(s):
        return lax.div(s * (DEPTH - 1 - s), 2)

    inner = 1 + lax.rem(z, 2)
    x_from = lax.div(z, 2)
    x_last = 2 - is_middle(z)

    def skips_y(n):
        return jnp.logical_and(lax.rem(n, DEPTH) == x_last, jnp.logical_and(n >= 4 * X_LO, n < 4 * X_HI))

    def x_copy(q, side):
        return remote(ysend.at[0, inner, q], xin.at[side, q], x_ss.at[q], x_rs.at[side, q], 2 * inner + y)

    def x_begin(q):
        ysend[0, inner, q] = user_part(0, (2 * inner + 1 - y) * SUBS + q)
        x_copy(q, x_from).start()

    def y_begin(n):
        k, t, q = place(n)

        @pl.when(jnp.logical_not(skips_y(n)))
        def _():
            ysend[k, t, q] = user_part(k, (2 * t + 1 - y) * SUBS + q)
            takes = jnp.logical_and(lax.rem(n, DEPTH) == DEPTH - 1, jnp.logical_and(n >= 4 * X_LO, n < 4 * X_HI))

            @pl.when(jnp.logical_and(is_mid, takes))
            def _():
                for side in range(2):
                    with jax.named_scope("rs_x"):
                        x_copy(q, side).wait_recv()
                    ysend[k, t, q] = ysend[k, t, q] + xin[side, q]
            y_copy(n).start()

    def z_up(k, t, q):
        return remote(yrecv.at[k, t, q], zin.at[k, t, q], z_ss, z_rs.at[t, q], c + 2)

    def z_down(k, t, q):
        to = t + lax.div(2 - (z - 1 - t), 2) * (DEPTH - t)
        return remote(yrecv.at[k, t, q], zin.at[k, to, q], z_ss, z_rs.at[to, q], c - 2)

    def z_add(k, t, at, q):
        with jax.named_scope("rs_z"):
            remote(yrecv.at[k, t, q], zin.at[k, at, q], z_ss, z_rs.at[at, q], mate).wait_recv()
        yrecv[k, t, q] = yrecv[k, t, q] + zin[k, at, q]

    def z_send(k, t, q):
        @pl.when(t > z)
        def _():
            z_up(k, t, q).start()

        @pl.when(t < z)
        def _():
            z_down(k, t, q).start()

    def y_stage(n):
        k, t, q = place(n)
        part = user_part(k, (2 * t + y) * SUBS + q)
        skipped = skips_y(n)

        @pl.when(skipped)
        def _():
            yrecv[k, t, q] = part

        @pl.when(jnp.logical_not(skipped))
        def _():
            with jax.named_scope("rs_y"):
                y_copy(n).wait_recv()
            yrecv[k, t, q] = yrecv[k, t, q] + part

        @pl.when(jnp.logical_and(jnp.logical_not(is_mid), t != z))
        def _():
            z_send(k, t, q)

    def mid_stage(n):
        k, t, q = place(n)

        @pl.when(t != z)
        def _():
            z_add(k, t, t, q)
            z_send(k, t, q)

    def table_out(q):
        return pltpu.make_async_copy(outu.at[q], outu_hbm.at[q], io_sem.at[q])

    item_out = pltpu.make_async_copy(outi, outi_hbm, io_sem.at[SUBS])

    def own_stage(n):
        k, _, q = place(n)

        @pl.when(is_down)
        def _():
            z_add(k, z, z, q)

        @pl.when(is_up)
        def _():
            z_add(k, z, DEPTH, q)
        val = yrecv[k, z, q].astype(BF16)

        @pl.when(k < LAYERS - 1)
        def _():
            panels[k + 1, c, q] = val
            ag_own(k + 1, q)
            item_part(k + 1, c, q)

        @pl.when(k == LAYERS - 1)
        def _():
            tot = (panels[0, c, q].astype(F32) + panels[1, c, q].astype(F32) + panels[2, c, q].astype(F32)
                   + val.astype(F32))
            out = (tot / (LAYERS + 1)).astype(BF16)
            outu[q] = out
            table_out(q).start()
            user_vec[...] += dot_n(out, onehot_a[q])

    def build_round(i):
        _, t, q = place(i)
        build((2 * t + 1 - y) * SUBS + q)
        build((2 * t + y) * SUBS + q)

    base = (r * RING + c) * (SUBS * BLK)
    ids_a = trip[0:1, :] - base
    item_acc[...] = jnp.zeros_like(item_acc)
    user_vec[...] = jnp.zeros_like(user_vec)

    own_lag = 7 - 2 * is_middle(z)
    sets = SUBS * (LAYERS - 1)

    def gather_set(late, event):
        @pl.when(jnp.logical_and(lax.rem(late + 64, 8) == 0, jnp.logical_and(late >= 0, late < 8 * sets)))
        def _():
            m = lax.div(late, 8)
            event(lax.div(m, SUBS) + 1, lax.rem(m, SUBS))

    def gather_mate(half):
        def event(k, q):
            ag_mate(k, q)
            item_part(k, mate, q)
        gather_set(half - (2 * own_lag + 6), event)

    def gather_line(half, d, f):
        for above in (True, False):
            s = z + d if above else z - d

            @pl.when(jnp.logical_and(s < DEPTH, s >= 0))
            def _():
                gather_set(half - (2 * (7 - 2 * is_middle(s)) + 3 * d + (6 if f else 1)),
                           lambda k, q: line_event(k, s, 1 - y if f else y, q, above,
                                                   lambda col, q: item_part(k, col, q)))

    for i in range(AHEAD):
        build_round(jnp.int32(i))
        y_begin(jnp.int32(i))
    for i in range(AHEAD, 4):
        build_round(jnp.int32(i))
    deg_sum(2)
    for q in range(2, SUBS):
        ag_mate(0, q)
        early_event(q)

    def when_at(n, i):
        return pl.when(n == i)

    def one_round(n, carry):
        @when_at(n, 1)
        def _():
            deg_sum(3)

        @when_at(n, 2)
        def _():
            deg_end(2)

        @when_at(n, 4)
        def _():
            deg_end(3)

        @when_at(n, 13)
        def _():
            item_end(0)

        @pl.when(n + AHEAD < LAYERS * ROUNDS)
        def _():
            y_begin(n + AHEAD)

        @pl.when(jnp.logical_and(lax.rem(n + X_LEAD, DEPTH) == 0,
                                 jnp.logical_and(n + X_LEAD >= 4 * X_LO, n + X_LEAD < 4 * X_HI)))
        def _():
            x_begin(lax.div(n + X_LEAD, DEPTH))
        gather_mate(2 * n)
        for d, f in ((1, 0), (2, 1), (3, 0)):
            gather_line(2 * n, d, f)
        y_stage(n)

        @pl.when(jnp.logical_and(is_mid, n >= 2))
        def _():
            mid_stage(n - 2)
        own = n - own_lag + 3

        @pl.when(jnp.logical_and(lax.rem(own + 4, 4) == 3, jnp.logical_and(own >= 0, own < 2 * ROUNDS)))
        def _():
            own_stage(own)
        for d, f in ((1, 1), (2, 0), (3, 1)):
            gather_line(2 * n + 1, d, f)

        @when_at(n, 46)
        def _():
            col_wait(2 * SUBS, pk_recv.at[pl.ds(0, RING - 1)])
            psum = pk_recv[0].astype(F32)
            for q in range(1, RING):
                psum = psum + pk_recv[q].astype(F32)
            picks[r] = psum.astype(BF16)
            row_send(8, lambda rr: picks.at[r], picks.at[r])

        @pl.when(n >= LAYERS * ROUNDS - SUBS)
        def _():
            own_stage(n)

        @when_at(n, 0)
        def _():
            deg_end(1)

        @pl.when(n < 6)
        def _():
            build_round(2 * n + 4)
            build_round(2 * n + 5)

        @pl.when(n < 6)
        def _():
            early_event(2 * n + 4)
            early_event(2 * n + 5)

        def late_event(e):
            first_event(e, lambda s, yy, q, above: line_event(
                0, s, yy, q, above, lambda col, q: item_part(0, col, q)))

        def old_event(e):
            first_event(e, lambda s, yy, q, above: item_part(0, 2 * s + yy, q))

        @pl.when(jnp.logical_and(n >= 6, n < 11))
        def _():
            e = 16 + (n - 6) + lax.div(n - 6, 3) + lax.div(n - 6, 4)
            late_event(e)

            @pl.when(n >= 8)
            def _():
                late_event(e + 1)

        @pl.when(jnp.logical_and(n >= 1, n < 9))
        def _():
            q, side = lax.div(n - 1, 2), lax.rem(n - 1, 2)
            item_part(0, c + side * (mate - c), q)
            old_event(q + 4 * side)

        @pl.when(jnp.logical_and(n >= 4, n < 11))
        def _():
            old_event(n + 4 + lax.div(n, 9))

            @pl.when(n == 8)
            def _():
                old_event(n + 5)

        @when_at(n, 10)
        def _():
            item_start(0)

        @when_at(n, 11)
        def _():
            item_share(0, item_sum(0))

        @when_at(n, 26)
        def _():
            item_start(1)

        @when_at(n, 27)
        def _():
            item_share(1, item_sum(1))

        @when_at(n, 28)
        def _():
            item_end(1)

        @pl.when(jnp.logical_and(n >= 32, n < 32 + SUBS))
        def _():
            iota_u = lax.broadcasted_iota(jnp.int32, (BLK, 128), 0) + (n - 32) * BLK
            onehot_a[n - 32] = (iota_u == ids_a).astype(BF16)

        @when_at(n, 43)
        def _():
            last_item = item_sum(2)
            tot = (ei_all[0, r].astype(F32) + ei_all[1, r].astype(F32) + ei_all[2, r].astype(F32)
                   + last_item.astype(F32))
            out_item = (tot / (LAYERS + 1)).astype(BF16)
            outi[...] = out_item
            item_out.start()
            item_share(2, out_item)

        @when_at(n, 44)
        def _():
            item_end(2)
            iota_i = lax.broadcasted_iota(jnp.int32, (BLK, 128), 0) + c * BLK
            hot = jnp.concatenate([(iota_i == trip[1:2, :]).astype(BF16), (iota_i == trip[2:3, :]).astype(BF16)],
                                  axis=1)
            got = dot_n(jnp.concatenate([ei_all[3, q] for q in range(ROWS)], axis=1), hot).astype(BF16)
            for q in range(ROWS):
                pk[q] = got[q * 16:(q + 1) * 16, :]
            col_send(2 * SUBS, lambda cc: pk.at[r], pk_recv.at[c])
            pk_recv[c] = pk[r]

        @when_at(n, 42)
        def _():
            item_start(2)
        return carry
    lax.fori_loop(0, LAYERS * ROUNDS, one_round, 0)

    row_wait(8, picks.at[pl.ds(0, ROWS - 1)])
    ea = user_vec[...]
    both = jnp.concatenate([picks[q] for q in range(ROWS)], axis=0).astype(F32)
    margin = (jnp.sum(ea * both[:, 0:128], axis=0, keepdims=True)
              - jnp.sum(ea * both[:, 128:256], axis=0, keepdims=True))
    term = jnp.maximum(-margin, 0.0) + jnp.log1p(jnp.exp(-jnp.abs(margin)))
    mine = jnp.logical_and(ids_a >= 0, ids_a < SUBS * BLK)
    me = c * ROWS + r
    terms[me] = jnp.where(mine, term, 0.0)
    for peer in all_peers:
        pltpu.make_async_remote_copy(src_ref=terms.at[me], dst_ref=terms.at[me], send_sem=term_sem.at[0],
                                     recv_sem=term_sem.at[1], device_id=peer, device_id_type=MESH).start()

    def drain(ref, sem):
        remote(ref, ref, sem, y_rs.at[0], mate).wait_send()

    drain(ysend.at[pl.ds(1, LAYERS - 1)], y_ss.at[1])
    drain(ysend.at[0, :, pl.ds(0, SUBS - X_HI + X_LO)], y_ss.at[0])
    drain(ysend.at[0, pl.ds(0, DEPTH - 1), pl.ds(0, X_HI - X_LO)], y_ss.at[2])
    for q in range(X_LO, X_HI):
        drain(xin.at[0, q], x_ss.at[q])
    for q in range(SUBS):
        table_out(q).wait()
    item_out.wait()
    drain(yrecv.at[:, pl.ds(0, DEPTH - 1)], z_ss)
    drain(panels.at[:, pl.ds(0, 1)], ag_sy)
    for at in range(DEPTH):
        @pl.when(z == at)
        def _():
            if at < DEPTH - 1:
                drain(panels.at[:, pl.ds(0, 2 * (at + 1))], ag_su)
            if at > 0:
                drain(panels.at[:, pl.ds(0, 2 * (DEPTH - at))], ag_sd)

    with jax.named_scope("terms_wait"):
        rest = terms.at[pl.ds(0, len(all_peers))]
        cp = pltpu.make_async_remote_copy(src_ref=rest, dst_ref=rest, send_sem=term_sem.at[0],
                                          recv_sem=term_sem.at[1], device_id=all_peers[0], device_id_type=MESH)
        cp.wait_recv()
        cp.wait_send()
    tsum = terms[0]
    for q in range(1, RING * ROWS):
        tsum = tsum + terms[q]
    loss[...] = jnp.broadcast_to(jnp.sum(tsum, axis=1, keepdims=True) / tsum.shape[1], loss.shape)


def deliver(outu, outi, loss, to_user, to_item, to_loss):
    for q in range(SUBS):
        to_user[:, q * BLK:(q + 1) * BLK] = outu[q]
    to_item[...] = outi[...]
    to_loss[...] = loss[0:1, 0:1]


def solution(mesh):
    def local_prog(mask_blk, user_shard, item_shard, triples):
        vmem = pl.BlockSpec(memory_space=pltpu.VMEM)
        hbm = pl.BlockSpec(memory_space=pl.ANY)
        dma = pltpu.SemaphoreType.DMA
        outu, outi, loss = pl.pallas_call(
            kernel,
            out_shape=(jax.ShapeDtypeStruct((SUBS, DIM, BLK), BF16),
                       jax.ShapeDtypeStruct((DIM, 128), BF16),
                       jax.ShapeDtypeStruct((8, 128), F32)),
            in_specs=[hbm] * 4,
            out_specs=(hbm, hbm, vmem),
            scratch_shapes=[
                pltpu.VMEM((RING * SUBS, BLK, BLK), BF16),
                pltpu.VMEM((MASK_BUFS, BLK, BLK), jnp.int32),
                dma((MASK_BUFS,)),
                dma((SUBS + 2,)),
                pltpu.VMEM((3, 128), jnp.int32),
                pltpu.VMEM((SUBS, DIM, BLK), BF16),
                pltpu.VMEM((DIM, 128), BF16),
                pltpu.VMEM((LAYERS, RING, SUBS, DIM, BLK), BF16),
                pltpu.VMEM((LAYERS + 1, ROWS, DIM, 128), BF16),
                pltpu.VMEM((LAYERS, DIM, BLK), F32),
                pltpu.VMEM((LAYERS, ROWS, DIM, 128), F32),
                pltpu.VMEM((LAYERS, ROWS, DIM, 128), F32),
                pltpu.VMEM((LAYERS, DEPTH, SUBS, DIM, BLK), F32),
                pltpu.VMEM((LAYERS, DEPTH, SUBS, DIM, BLK), F32),
                pltpu.VMEM((LAYERS, DEPTH + 1, SUBS, DIM, BLK), F32),
                pltpu.VMEM((2, SUBS, DIM, BLK), F32),
                pltpu.VMEM((8, BLK), F32),
                pltpu.VMEM((RING * SUBS, 1, BLK), F32),
                pltpu.VMEM((RING, SUBS, 1, BLK), F32),
                pltpu.VMEM((RING * SUBS, 1, BLK), F32),
                pltpu.VMEM((1, BLK), F32),
                pltpu.VMEM((ROWS, 1, BLK), F32),
                pltpu.VMEM((1, BLK), F32),
                pltpu.VMEM((SUBS, BLK, 128), BF16),
                pltpu.VMEM((ROWS, 16, 256), BF16),
                pltpu.VMEM((RING, 16, 256), BF16),
                pltpu.VMEM((ROWS, 16, 256), BF16),
                pltpu.VMEM((DIM, 128), F32),
                pltpu.VMEM((RING * ROWS, 1, 128), F32),
                dma((2,)),
                dma((3,)), dma((Y_SEMS,)), dma((SUBS,)), dma((2, SUBS)), dma, dma((DEPTH + 1, SUBS)),
                dma, dma, dma, dma((2, RING, SUBS)),
                dma((3,)), dma((3,)), dma((2 * SUBS + 1,)), dma((2 * SUBS + 1,)),
            ],
            compiler_params=pltpu.CompilerParams(
                collective_id=0, has_side_effects=True, vmem_limit_bytes=61 * 1024 * 1024),
            name="propagate",
        )(mask_blk, user_shard.T, item_shard.T, triples.T)
        out_user, out_item, mean = pl.pallas_call(
            deliver,
            out_shape=(jax.ShapeDtypeStruct((DIM, SUBS * BLK), BF16),
                       jax.ShapeDtypeStruct((DIM, 128), BF16),
                       jax.ShapeDtypeStruct((1, 1), F32)),
            in_specs=[vmem, vmem, vmem], out_specs=(vmem, vmem, vmem), name="deliver",
        )(outu, outi, loss)
        return out_user.T, out_item.T, mean[0, 0]

    return jax.shard_map(local_prog, mesh=mesh,
                         in_specs=(P("row", "col"), P(("row", "col"), None), P(("col", "row"), None), P(None, None)),
                         out_specs=(P(("row", "col"), None), P(("col", "row"), None), P()), check_vma=False)
```

```python
import jax
import jax.numpy as jnp
from jax import lax
from jax.experimental import pallas as pl
from jax.experimental.pallas import tpu as pltpu
from jax.sharding import PartitionSpec as P

LAYERS = 3
RING = 8
ROWS = 4
DEPTH = 4
ROUNDS = 16
AHEAD = 3
Y_SEMS = 8
ROW_SET = (0, 1, 2, 1, 2, 1, 2, 1, 2)
X_LO = 2
X_HI = 3
X_LEAD = 2
SUBS = 4
DIM = 64
BLK = 512
MASK_BUFS = 8
MESH = pl.DeviceIdType.MESH
BF16 = jnp.bfloat16
F32 = jnp.float32


def dot_t(lhs, rhs):
    return lax.dot_general(lhs, rhs, (((1,), (1,)), ((), ())), preferred_element_type=F32)


def dot_n(lhs, rhs):
    return lax.dot_general(lhs, rhs, (((1,), (0,)), ((), ())), preferred_element_type=F32)


def kernel(mask_hbm, euT, eiT, trip_hbm, outu_hbm, outi_hbm, loss,
           adj, mbuf, msem, io_sem, trip, outu, outi,
           panels, ei_all, item_acc, item_send, item_recv,
           ysend, yrecv, zin, xin,
           colsum, deg_part, deg_recv, scale_u, itemdeg, itemdeg_recv, scale_v,
           onehot_a, pk, pk_recv, picks, user_vec, terms, term_sem,
           y_ss, y_rs, x_ss, x_rs, z_ss, z_rs, ag_sy, ag_su, ag_sd, ag_rs,
           row_ss, row_rs, col_ss, col_rs):
    c = lax.axis_index("col")
    r = lax.axis_index("row")
    z, y = lax.div(c, 2), lax.rem(c, 2)
    mate = 2 * z + 1 - y
    is_up, is_down = z < DEPTH - 1, z > 0
    is_mid = jnp.logical_and(is_up, is_down)
    row_peers = [lax.rem(r + d, ROWS) for d in range(1, ROWS)]
    col_peers = [lax.rem(c + d, RING) for d in range(1, RING)]

    def mask_at(i):
        return lax.rem(i, RING) * SUBS + lax.div(i, RING)

    def mask_copy(i):
        slot = lax.rem(i, MASK_BUFS)
        return pltpu.make_async_copy(mask_hbm.at[pl.ds(mask_at(i) * BLK, BLK), :], mbuf.at[slot], msem.at[slot])

    for i in range(MASK_BUFS):
        mask_copy(jnp.int32(i)).start()

    def table_in(q):
        return pltpu.make_async_copy(euT.at[:, pl.ds(q * BLK, BLK)], panels.at[0, c, q], io_sem.at[q])

    item_in = pltpu.make_async_copy(eiT, ei_all.at[0, r], io_sem.at[SUBS])
    trip_in = pltpu.make_async_copy(trip_hbm, trip, io_sem.at[SUBS + 1])
    for q in range(SUBS):
        table_in(q).start()
    item_in.start()
    trip_in.start()

    barrier = pltpu.get_barrier_semaphore()
    all_peers = [(lax.rem(c + dc, RING), lax.rem(r + dr, ROWS))
                 for dc in range(RING) for dr in range(ROWS) if dc or dr]
    for peer in all_peers:
        pl.semaphore_signal(barrier, inc=1, device_id=peer, device_id_type=MESH)

    def remote(src, dst, ss, rs, col):
        return pltpu.make_async_remote_copy(src_ref=src, dst_ref=dst, send_sem=ss, recv_sem=rs,
                                            device_id=(col, r), device_id_type=MESH)

    def ag_rs_of(k, col, q):
        return ag_rs.at[col, q]

    def ag_y(k, q, col):
        ref = panels.at[k, col, q]
        return remote(ref, ref, ag_sy, ag_rs_of(k, col, q), mate)

    def ag_up(k, col, q):
        ref = panels.at[k, col, q]
        return remote(ref, ref, ag_su, ag_rs_of(k, col, q), c + 2)

    def ag_down(k, col, q):
        ref = panels.at[k, col, q]
        return remote(ref, ref, ag_sd, ag_rs_of(k, col, q), c - 2)

    def ag_both(k, col, q):
        @pl.when(is_up)
        def _():
            ag_up(k, col, q).start()

        @pl.when(is_down)
        def _():
            ag_down(k, col, q).start()

    def ag_own(k, q):
        ag_y(k, q, c).start()
        ag_both(k, c, q)

    def ag_mate(k, q):
        with jax.named_scope("ag_mate"):
            ag_y(k, q, mate).wait_recv()
        ag_both(k, mate, q)

    def line_event(k, s, yy, q, above, then):
        col = 2 * s + yy
        if above:
            with jax.named_scope("ag_above"):
                ag_down(k, col, q).wait_recv()

            @pl.when(is_down)
            def _():
                ag_down(k, col, q).start()
        else:
            with jax.named_scope("ag_below"):
                ag_up(k, col, q).wait_recv()

            @pl.when(is_up)
            def _():
                ag_up(k, col, q).start()
        then(col, q)

    def first_event(e, event):
        d, rest = lax.div(e, 2 * SUBS) + 1, lax.rem(e, 2 * SUBS)
        yy = y + lax.div(rest, SUBS) * (1 - 2 * y)
        q = lax.rem(rest, SUBS)

        @pl.when(z + d < DEPTH)
        def _():
            event(z + d, yy, q, True)

        @pl.when(z - d >= 0)
        def _():
            event(z - d, yy, q, False)

    def row_send(u, src, dst):
        for rr in row_peers:
            pltpu.make_async_remote_copy(src_ref=src(rr), dst_ref=dst, send_sem=row_ss.at[ROW_SET[u]], recv_sem=row_rs.at[ROW_SET[u]],
                                         device_id=(c, rr), device_id_type=MESH).start()

    def row_wait(u, ref):
        with jax.named_scope("row_wait_%d" % u):
            cp = pltpu.make_async_remote_copy(src_ref=ref, dst_ref=ref, send_sem=row_ss.at[ROW_SET[u]], recv_sem=row_rs.at[ROW_SET[u]],
                                              device_id=(c, row_peers[0]), device_id_type=MESH)
            cp.wait_recv()
            cp.wait_send()

    def col_send(u, src, dst):
        for cc in col_peers:
            remote(src(cc), dst, col_ss.at[u], col_rs.at[u], cc).start()

    def col_wait(u, ref):
        with jax.named_scope("col_wait_%d" % u):
            cp = remote(ref, ref, col_ss.at[u], col_rs.at[u], mate)
            cp.wait_recv()
            cp.wait_send()

    ones = jnp.ones((16, BLK), BF16)
    colsum[...] = jnp.zeros_like(colsum)

    def mask_block(i, carry):
        slot, b = lax.rem(i, MASK_BUFS), mask_at(i)
        mask_copy(i).wait()
        acc = jnp.zeros((8, BLK), F32)
        for t in range(4):
            m = mbuf[slot, t * 128:(t + 1) * 128, :].astype(F32)
            acc = acc + jnp.sum(m.reshape(16, 8, BLK), axis=0)
            adj[b, t * 128:(t + 1) * 128, :] = m.astype(BF16)
        colsum[...] += acc
        deg_part[b] = dot_t(ones, adj[b])[0:1, :]

        @pl.when(i + MASK_BUFS < SUBS * RING)
        def _():
            mask_copy(i + MASK_BUFS).start()
        return carry

    def deg_send(q):
        col_send(q, lambda cc: deg_part.at[cc * SUBS + q], deg_recv.at[c, q])
        deg_recv[c, q] = deg_part[c * SUBS + q]

    def deg_sum(q):
        col_wait(q, deg_part.at[pl.ds(0, RING - 1)])
        du = deg_recv[0, q]
        for cc in range(1, RING):
            du = du + deg_recv[cc, q]
        scale_u[c * SUBS + q] = lax.rsqrt(jnp.maximum(du, 1.0))
        col_send(SUBS + q, lambda cc: scale_u.at[c * SUBS + q], scale_u.at[c * SUBS + q])

    def deg_end(q):
        col_wait(SUBS + q, deg_part.at[pl.ds(0, RING - 1)])

    def mask_quarter(q):
        with jax.named_scope("mask"):
            lax.fori_loop(RING * q, RING * (q + 1), mask_block, 0)

    def early_event(e):
        first_event(jnp.int32(e), lambda s, yy, q, above: line_event(0, s, yy, q, above, lambda col, q: None))

    mask_quarter(0)
    for q in range(SUBS):
        table_in(q).wait()
    item_in.wait()
    trip_in.wait()
    with jax.named_scope("entry"):
        pl.semaphore_wait(barrier, len(all_peers))
    deg_send(0)
    ag_own(0, 0)
    ag_own(0, 1)
    row_send(0, lambda rr: ei_all.at[0, r], ei_all.at[0, r])
    mask_quarter(1)
    deg_send(1)
    ag_own(0, 2)
    mask_quarter(2)
    deg_send(2)
    deg_sum(0)
    ag_own(0, 3)
    for q in range(2):
        ag_mate(0, q)
        early_event(q)
    mask_quarter(3)
    itemdeg[...] = jnp.sum(colsum[...], axis=0, keepdims=True)
    row_send(1, lambda rr: itemdeg, itemdeg_recv.at[r])
    deg_send(3)
    itemdeg_recv[r] = itemdeg[...]
    deg_sum(1)
    row_wait(1, itemdeg_recv.at[pl.ds(0, ROWS - 1)])
    dv = itemdeg_recv[0] + itemdeg_recv[1] + itemdeg_recv[2] + itemdeg_recv[3]
    scale_v[...] = lax.rsqrt(jnp.maximum(dv, 1.0))
    row_wait(0, ei_all.at[0, pl.ds(0, ROWS - 1)])
    deg_end(0)

    def build(b):
        sv = scale_v[...]
        for t in range(4):
            su = scale_u[b, :, t * 128:(t + 1) * 128]
            suc = jnp.transpose(jnp.broadcast_to(su, (128, 128)))
            val = (jnp.concatenate([suc] * 4, axis=1) * sv).astype(BF16)
            adj[b, t * 128:(t + 1) * 128, :] = adj[b, t * 128:(t + 1) * 128, :] * val

    def user_part(k, b):
        ei = jnp.concatenate([ei_all[k, q] for q in range(ROWS)], axis=1)
        return dot_t(ei, adj[b])

    def item_part(k, col, q):
        item_acc[k] += dot_n(panels[k, col, q], adj[col * SUBS + q])

    def item_start(k):
        for q in range(ROWS):
            item_send[k, q] = item_acc[k, :, q * 128:(q + 1) * 128]
        row_send(2 + 2 * k, lambda rr: item_send.at[k, rr], item_recv.at[k, r])
        item_recv[k, r] = item_send[k, r]

    def item_sum(k):
        row_wait(2 + 2 * k, item_send.at[k, pl.ds(0, ROWS - 1)])
        tot = item_recv[k, 0] + item_recv[k, 1] + item_recv[k, 2] + item_recv[k, 3]
        return tot.astype(BF16)

    def item_share(k, val):
        ei_all[k + 1, r] = val
        row_send(3 + 2 * k, lambda rr: ei_all.at[k + 1, r], ei_all.at[k + 1, r])

    def item_end(k):
        row_wait(3 + 2 * k, ei_all.at[k + 1, pl.ds(0, ROWS - 1)])

    def place(n):
        k, i = lax.div(n, ROUNDS), lax.rem(n, ROUNDS)
        last, own = lax.div(k, LAYERS - 1), lax.div(i, 12)
        q, g = lax.div(i, 4), lax.rem(i, 4)
        q_last = (1 - own) * lax.div(i, 3) + own * (i - 12)
        g_last = (1 - own) * lax.rem(i, 3) + own * 3
        q, g = q + last * (q_last - q), g + last * (g_last - g)
        pw = 1 + 3 * g + 9 * lax.div(g * (g - 1), 2) + 27 * lax.div(g * (g - 1) * (g - 2), 6)
        return k, lax.rem(lax.div(27 + 48 * z + 57 * lax.div(z, 2), pw), DEPTH), q

    def y_set(k, q):
        later = lax.div(k + 1, 2)
        skip = lax.div(q + SUBS - X_LO, SUBS) * (1 - lax.div(q + SUBS - X_HI, SUBS))
        return later + (1 - later) * 2 * skip

    def y_copy(n):
        k, t, q = place(n)
        return remote(ysend.at[k, t, q], yrecv.at[k, t, q], y_ss.at[y_set(k, q)], y_rs.at[lax.rem(n, Y_SEMS)], mate)

    def is_middle(s):
        return lax.div(s * (DEPTH - 1 - s), 2)

    inner = 1 + lax.rem(z, 2)
    x_from = lax.div(z, 2)
    x_last = 2 - is_middle(z)

    def skips_y(n):
        return jnp.logical_and(lax.rem(n, DEPTH) == x_last, jnp.logical_and(n >= 4 * X_LO, n < 4 * X_HI))

    def x_copy(q, side):
        return remote(ysend.at[0, inner, q], xin.at[side, q], x_ss.at[q], x_rs.at[side, q], 2 * inner + y)

    def x_begin(q):
        ysend[0, inner, q] = user_part(0, (2 * inner + 1 - y) * SUBS + q)
        x_copy(q, x_from).start()

    def y_begin(n):
        k, t, q = place(n)

        @pl.when(jnp.logical_not(skips_y(n)))
        def _():
            ysend[k, t, q] = user_part(k, (2 * t + 1 - y) * SUBS + q)
            takes = jnp.logical_and(lax.rem(n, DEPTH) == DEPTH - 1, jnp.logical_and(n >= 4 * X_LO, n < 4 * X_HI))

            @pl.when(jnp.logical_and(is_mid, takes))
            def _():
                for side in range(2):
                    with jax.named_scope("rs_x"):
                        x_copy(q, side).wait_recv()
                    ysend[k, t, q] = ysend[k, t, q] + xin[side, q]
            y_copy(n).start()

    def z_up(k, t, q):
        return remote(yrecv.at[k, t, q], zin.at[k, t, q], z_ss, z_rs.at[t, q], c + 2)

    def z_down(k, t, q):
        to = t + lax.div(2 - (z - 1 - t), 2) * (DEPTH - t)
        return remote(yrecv.at[k, t, q], zin.at[k, to, q], z_ss, z_rs.at[to, q], c - 2)

    def z_add(k, t, at, q):
        with jax.named_scope("rs_z"):
            remote(yrecv.at[k, t, q], zin.at[k, at, q], z_ss, z_rs.at[at, q], mate).wait_recv()
        yrecv[k, t, q] = yrecv[k, t, q] + zin[k, at, q]

    def z_send(k, t, q):
        @pl.when(t > z)
        def _():
            z_up(k, t, q).start()

        @pl.when(t < z)
        def _():
            z_down(k, t, q).start()

    def y_stage(n):
        k, t, q = place(n)
        part = user_part(k, (2 * t + y) * SUBS + q)
        skipped = skips_y(n)

        @pl.when(skipped)
        def _():
            yrecv[k, t, q] = part

        @pl.when(jnp.logical_not(skipped))
        def _():
            with jax.named_scope("rs_y"):
                y_copy(n).wait_recv()
            yrecv[k, t, q] = yrecv[k, t, q] + part

        @pl.when(jnp.logical_and(jnp.logical_not(is_mid), t != z))
        def _():
            z_send(k, t, q)

    def mid_stage(n):
        k, t, q = place(n)

        @pl.when(t != z)
        def _():
            z_add(k, t, t, q)
            z_send(k, t, q)

    def table_out(q):
        return pltpu.make_async_copy(outu.at[q], outu_hbm.at[q], io_sem.at[q])

    item_out = pltpu.make_async_copy(outi, outi_hbm, io_sem.at[SUBS])

    def own_stage(n):
        k, _, q = place(n)

        @pl.when(is_down)
        def _():
            z_add(k, z, z, q)

        @pl.when(is_up)
        def _():
            z_add(k, z, DEPTH, q)
        val = yrecv[k, z, q].astype(BF16)

        @pl.when(k < LAYERS - 1)
        def _():
            panels[k + 1, c, q] = val
            ag_own(k + 1, q)
            item_part(k + 1, c, q)

        @pl.when(k == LAYERS - 1)
        def _():
            tot = (panels[0, c, q].astype(F32) + panels[1, c, q].astype(F32) + panels[2, c, q].astype(F32)
                   + val.astype(F32))
            out = (tot / (LAYERS + 1)).astype(BF16)
            outu[q] = out
            table_out(q).start()
            user_vec[...] += dot_n(out, onehot_a[q])

    def build_round(i):
        _, t, q = place(i)
        build((2 * t + 1 - y) * SUBS + q)
        build((2 * t + y) * SUBS + q)

    base = (r * RING + c) * (SUBS * BLK)
    ids_a = trip[0:1, :] - base
    item_acc[...] = jnp.zeros_like(item_acc)
    user_vec[...] = jnp.zeros_like(user_vec)

    own_lag = 7 - 2 * is_middle(z)
    sets = SUBS * (LAYERS - 1)

    def gather_set(late, event):
        @pl.when(jnp.logical_and(lax.rem(late + 64, 8) == 0, jnp.logical_and(late >= 0, late < 8 * sets)))
        def _():
            m = lax.div(late, 8)
            event(lax.div(m, SUBS) + 1, lax.rem(m, SUBS))

    def gather_mate(half):
        def event(k, q):
            ag_mate(k, q)
            item_part(k, mate, q)
        gather_set(half - (2 * own_lag + 6), event)

    def gather_line(half, d, f):
        for above in (True, False):
            s = z + d if above else z - d

            @pl.when(jnp.logical_and(s < DEPTH, s >= 0))
            def _():
                gather_set(half - (2 * (7 - 2 * is_middle(s)) + 3 * d + (6 if f else 1)),
                           lambda k, q: line_event(k, s, 1 - y if f else y, q, above,
                                                   lambda col, q: item_part(k, col, q)))

    for i in range(AHEAD):
        build_round(jnp.int32(i))
        y_begin(jnp.int32(i))
    for i in range(AHEAD, 4):
        build_round(jnp.int32(i))
    deg_sum(2)
    for q in range(2, SUBS):
        ag_mate(0, q)
        early_event(q)

    def when_at(n, i):
        return pl.when(n == i)

    def one_round(n, carry):
        @when_at(n, 1)
        def _():
            deg_sum(3)

        @when_at(n, 2)
        def _():
            deg_end(2)

        @when_at(n, 4)
        def _():
            deg_end(3)

        @when_at(n, 13)
        def _():
            item_end(0)

        @pl.when(n + AHEAD < LAYERS * ROUNDS)
        def _():
            y_begin(n + AHEAD)

        @pl.when(jnp.logical_and(lax.rem(n + X_LEAD, DEPTH) == 0,
                                 jnp.logical_and(n + X_LEAD >= 4 * X_LO, n + X_LEAD < 4 * X_HI)))
        def _():
            x_begin(lax.div(n + X_LEAD, DEPTH))
        gather_mate(2 * n)
        for d, f in ((1, 0), (2, 1), (3, 0)):
            gather_line(2 * n, d, f)
        y_stage(n)

        @pl.when(jnp.logical_and(is_mid, n >= 2))
        def _():
            mid_stage(n - 2)
        own = n - own_lag + 3

        @pl.when(jnp.logical_and(lax.rem(own + 4, 4) == 3, jnp.logical_and(own >= 0, own < 2 * ROUNDS)))
        def _():
            own_stage(own)
        for d, f in ((1, 1), (2, 0), (3, 1)):
            gather_line(2 * n + 1, d, f)

        @when_at(n, 46)
        def _():
            col_wait(2 * SUBS, pk_recv.at[pl.ds(0, RING - 1)])
            psum = pk_recv[0].astype(F32)
            for q in range(1, RING):
                psum = psum + pk_recv[q].astype(F32)
            picks[r] = psum.astype(BF16)
            row_send(8, lambda rr: picks.at[r], picks.at[r])

        @pl.when(n >= LAYERS * ROUNDS - SUBS)
        def _():
            own_stage(n)

        @when_at(n, 0)
        def _():
            deg_end(1)

        @pl.when(n < 6)
        def _():
            build_round(2 * n + 4)
            build_round(2 * n + 5)

        @pl.when(n < 6)
        def _():
            early_event(2 * n + 4)
            early_event(2 * n + 5)

        def late_event(e):
            first_event(e, lambda s, yy, q, above: line_event(
                0, s, yy, q, above, lambda col, q: item_part(0, col, q)))

        def old_event(e):
            first_event(e, lambda s, yy, q, above: item_part(0, 2 * s + yy, q))

        @pl.when(jnp.logical_and(n >= 6, n < 11))
        def _():
            e = 16 + (n - 6) + lax.div(n - 6, 3) + lax.div(n - 6, 4)
            late_event(e)

            @pl.when(n >= 8)
            def _():
                late_event(e + 1)

        @pl.when(jnp.logical_and(n >= 1, n < 9))
        def _():
            q, side = lax.div(n - 1, 2), lax.rem(n - 1, 2)
            item_part(0, c + side * (mate - c), q)
            old_event(q + 4 * side)

        @pl.when(jnp.logical_and(n >= 4, n < 11))
        def _():
            old_event(n + 4 + lax.div(n, 9))

            @pl.when(n == 8)
            def _():
                old_event(n + 5)

        @when_at(n, 10)
        def _():
            item_start(0)

        @when_at(n, 11)
        def _():
            item_share(0, item_sum(0))

        @when_at(n, 26)
        def _():
            item_start(1)

        @when_at(n, 27)
        def _():
            item_share(1, item_sum(1))

        @when_at(n, 28)
        def _():
            item_end(1)

        @pl.when(jnp.logical_and(n >= 32, n < 32 + SUBS))
        def _():
            iota_u = lax.broadcasted_iota(jnp.int32, (BLK, 128), 0) + (n - 32) * BLK
            onehot_a[n - 32] = (iota_u == ids_a).astype(BF16)

        @when_at(n, 43)
        def _():
            last_item = item_sum(2)
            tot = (ei_all[0, r].astype(F32) + ei_all[1, r].astype(F32) + ei_all[2, r].astype(F32)
                   + last_item.astype(F32))
            out_item = (tot / (LAYERS + 1)).astype(BF16)
            outi[...] = out_item
            item_out.start()
            item_share(2, out_item)

        @when_at(n, 44)
        def _():
            item_end(2)
            iota_i = lax.broadcasted_iota(jnp.int32, (BLK, 128), 0) + c * BLK
            hot = jnp.concatenate([(iota_i == trip[1:2, :]).astype(BF16), (iota_i == trip[2:3, :]).astype(BF16)],
                                  axis=1)
            got = dot_n(jnp.concatenate([ei_all[3, q] for q in range(ROWS)], axis=1), hot).astype(BF16)
            for q in range(ROWS):
                pk[q] = got[q * 16:(q + 1) * 16, :]
            col_send(2 * SUBS, lambda cc: pk.at[r], pk_recv.at[c])
            pk_recv[c] = pk[r]

        @when_at(n, 42)
        def _():
            item_start(2)
        return carry
    lax.fori_loop(0, LAYERS * ROUNDS, one_round, 0)

    row_wait(8, picks.at[pl.ds(0, ROWS - 1)])
    ea = user_vec[...]
    both = jnp.concatenate([picks[q] for q in range(ROWS)], axis=0).astype(F32)
    margin = (jnp.sum(ea * both[:, 0:128], axis=0, keepdims=True)
              - jnp.sum(ea * both[:, 128:256], axis=0, keepdims=True))
    term = jnp.maximum(-margin, 0.0) + jnp.log1p(jnp.exp(-jnp.abs(margin)))
    mine = jnp.logical_and(ids_a >= 0, ids_a < SUBS * BLK)
    me = c * ROWS + r
    terms[me] = jnp.where(mine, term, 0.0)
    for peer in all_peers:
        pltpu.make_async_remote_copy(src_ref=terms.at[me], dst_ref=terms.at[me], send_sem=term_sem.at[0],
                                     recv_sem=term_sem.at[1], device_id=peer, device_id_type=MESH).start()

    def drain(ref, sem):
        remote(ref, ref, sem, y_rs.at[0], mate).wait_send()

    drain(ysend.at[pl.ds(1, LAYERS - 1)], y_ss.at[1])
    drain(ysend.at[0, :, pl.ds(0, SUBS - X_HI + X_LO)], y_ss.at[0])
    drain(ysend.at[0, pl.ds(0, DEPTH - 1), pl.ds(0, X_HI - X_LO)], y_ss.at[2])
    for q in range(X_LO, X_HI):
        drain(xin.at[0, q], x_ss.at[q])
    for q in range(SUBS):
        table_out(q).wait()
    item_out.wait()
    drain(yrecv.at[:, pl.ds(0, DEPTH - 1)], z_ss)
    drain(panels.at[:, pl.ds(0, 1)], ag_sy)
    for at in range(DEPTH):
        @pl.when(z == at)
        def _():
            if at < DEPTH - 1:
                drain(panels.at[:, pl.ds(0, 2 * (at + 1))], ag_su)
            if at > 0:
                drain(panels.at[:, pl.ds(0, 2 * (DEPTH - at))], ag_sd)

    with jax.named_scope("terms_wait"):
        rest = terms.at[pl.ds(0, len(all_peers))]
        cp = pltpu.make_async_remote_copy(src_ref=rest, dst_ref=rest, send_sem=term_sem.at[0],
                                          recv_sem=term_sem.at[1], device_id=all_peers[0], device_id_type=MESH)
        cp.wait_recv()
        cp.wait_send()
    tsum = terms[0]
    for q in range(1, RING * ROWS):
        tsum = tsum + terms[q]
    loss[...] = jnp.broadcast_to(jnp.sum(tsum, axis=1, keepdims=True) / tsum.shape[1], loss.shape)


def deliver(outu, outi, loss, to_user, to_item, to_loss):
    for q in range(SUBS):
        to_user[:, q * BLK:(q + 1) * BLK] = outu[q]
    to_item[...] = outi[...]
    to_loss[...] = loss[0:1, 0:1]


def solution(mesh):
    def local_prog(mask_blk, user_shard, item_shard, triples):
        vmem = pl.BlockSpec(memory_space=pltpu.VMEM)
        hbm = pl.BlockSpec(memory_space=pl.ANY)
        dma = pltpu.SemaphoreType.DMA
        outu, outi, loss = pl.pallas_call(
            kernel,
            out_shape=(jax.ShapeDtypeStruct((SUBS, DIM, BLK), BF16),
                       jax.ShapeDtypeStruct((DIM, 128), BF16),
                       jax.ShapeDtypeStruct((8, 128), F32)),
            in_specs=[hbm] * 4,
            out_specs=(hbm, hbm, vmem),
            scratch_shapes=[
                pltpu.VMEM((RING * SUBS, BLK, BLK), BF16),
                pltpu.VMEM((MASK_BUFS, BLK, BLK), jnp.int32),
                dma((MASK_BUFS,)),
                dma((SUBS + 2,)),
                pltpu.VMEM((3, 128), jnp.int32),
                pltpu.VMEM((SUBS, DIM, BLK), BF16),
                pltpu.VMEM((DIM, 128), BF16),
                pltpu.VMEM((LAYERS, RING, SUBS, DIM, BLK), BF16),
                pltpu.VMEM((LAYERS + 1, ROWS, DIM, 128), BF16),
                pltpu.VMEM((LAYERS, DIM, BLK), F32),
                pltpu.VMEM((LAYERS, ROWS, DIM, 128), F32),
                pltpu.VMEM((LAYERS, ROWS, DIM, 128), F32),
                pltpu.VMEM((LAYERS, DEPTH, SUBS, DIM, BLK), F32),
                pltpu.VMEM((LAYERS, DEPTH, SUBS, DIM, BLK), F32),
                pltpu.VMEM((LAYERS, DEPTH + 1, SUBS, DIM, BLK), F32),
                pltpu.VMEM((2, SUBS, DIM, BLK), F32),
                pltpu.VMEM((8, BLK), F32),
                pltpu.VMEM((RING * SUBS, 1, BLK), F32),
                pltpu.VMEM((RING, SUBS, 1, BLK), F32),
                pltpu.VMEM((RING * SUBS, 1, BLK), F32),
                pltpu.VMEM((1, BLK), F32),
                pltpu.VMEM((ROWS, 1, BLK), F32),
                pltpu.VMEM((1, BLK), F32),
                pltpu.VMEM((SUBS, BLK, 128), BF16),
                pltpu.VMEM((ROWS, 16, 256), BF16),
                pltpu.VMEM((RING, 16, 256), BF16),
                pltpu.VMEM((ROWS, 16, 256), BF16),
                pltpu.VMEM((DIM, 128), F32),
                pltpu.VMEM((RING * ROWS, 1, 128), F32),
                dma((2,)),
                dma((3,)), dma((Y_SEMS,)), dma((SUBS,)), dma((2, SUBS)), dma, dma((DEPTH + 1, SUBS)),
                dma, dma, dma, dma((RING, SUBS)),
                dma((3,)), dma((3,)), dma((2 * SUBS + 1,)), dma((2 * SUBS + 1,)),
            ],
            compiler_params=pltpu.CompilerParams(
                collective_id=0, has_side_effects=True, vmem_limit_bytes=61 * 1024 * 1024),
            name="propagate",
        )(mask_blk, user_shard.T, item_shard.T, triples.T)
        out_user, out_item, mean = pl.pallas_call(
            deliver,
            out_shape=(jax.ShapeDtypeStruct((DIM, SUBS * BLK), BF16),
                       jax.ShapeDtypeStruct((DIM, 128), BF16),
                       jax.ShapeDtypeStruct((1, 1), F32)),
            in_specs=[vmem, vmem, vmem], out_specs=(vmem, vmem, vmem), name="deliver",
        )(outu, outi, loss)
        return out_user.T, out_item.T, mean[0, 0]

    return jax.shard_map(local_prog, mesh=mesh,
                         in_specs=(P("row", "col"), P(("row", "col"), None), P(("col", "row"), None), P(None, None)),
                         out_specs=(P(("row", "col"), None), P(("col", "row"), None), P()), check_vma=False)
```
